32 devices in a mesh: groups: 2 (over y), gx: 4 (over z), gy: 4 (over x, core).
Axes of the slice: x: 2, y: 2, z: 4, core: 2. Of those that a mesh axis runs over, the one named last changes fastest.
Arguments:
- thermal_deviation: float32 [32, 256, 512], P('groups', 'gy', 'gx'), parts along dimension 0, may hold values from -6 to 6
- brine_content: float32 [32, 256, 512], P('groups', 'gy', 'gx'), parts along dimension 0, may hold values from 0.2 to 2.4
- current_components: float32 [4, 16, 256, 512], P('groups', None, 'gy', 'gx'), parts along dimension 0, may hold values from -4 to 4
- sea_indicator: int32 [256, 512], P('gy', 'gx'), may hold values from 0 to 1, as said below
- flooded_layer_number: int32 [256, 512], P('gy', 'gx'), may hold values from 1 to 16
- footprint_square_metres: float32 [256, 512], P('gy', 'gx'), may hold values from 0.5 to 5
- rainfall_input: float32 [256, 512], P('gy', 'gx'), may hold values from -2 to 3.5
- seam_partner_index: int32 [512], P('gx'), may hold values from 0 to 511, as said below
Outputs:
- temperature_next: float32 [32, 256, 512], P('groups', 'gy', 'gx'), parts along dimension 0
- salinity_next: float32 [32, 256, 512], P('groups', 'gy', 'gx'), parts along dimension 0
The draws below stay inside these ranges and needn't reach their ends.
There are 2 independent parts, one for each index of `groups`. The reference program is written for one: setup_inputs(seed, part) draws one part's arguments, and reference() takes and returns one part's arrays. A program takes and returns all parts, laid end to end along the dimension named above; an argument that names none is the same for every part. Nothing has to cross between parts.
Inputs may be any that keep to these rules, and one draw needn't show every extreme that they name: `sea_indicator`: at least one column is ocean. seam_partner_index[x] = (s - x) mod 512 for one s of each draw with s mod 128 = 127; the map is its own inverse and has no fixed point.
All inputs are finite; a program needn't handle non-finite values.
Results may differ from the reference program's by a relative error of at most 0.00002.
Values sent between devices are 32-bit elements; how exact they have to be, the bound alone decides.
A program may use at most 64 MiB of HBM per device.

```python
import math
import jax
import jax.numpy as jnp

SEA_LAYER_TOTAL = 16
CX = 128
PARALLEL_TOTAL = 256
MERIDIAN_TOTAL = 512


def draw_brine_content(key, part):
    longitude = jnp.arange(MERIDIAN_TOTAL, dtype=jnp.float32) / MERIDIAN_TOTAL
    zonal_trend = 0.5 + longitude
    factor = jax.random.uniform(key, (SEA_LAYER_TOTAL, PARALLEL_TOTAL, MERIDIAN_TOTAL), jnp.float32, 0.6, 1.4)
    return (zonal_trend * factor).astype(jnp.float32)


def draw_rainfall_input(key, part):
    second = jax.random.fold_in(jax.random.fold_in(key, 11), 1)
    longitude = jnp.arange(MERIDIAN_TOTAL, dtype=jnp.float32) / MERIDIAN_TOTAL
    zonal_trend = 0.5 + longitude
    rough_noise = jnp.clip(0.5 * jax.random.normal(second, (PARALLEL_TOTAL, MERIDIAN_TOTAL), jnp.float32), -2.0, 2.0)
    return (zonal_trend + rough_noise).astype(jnp.float32)


def draw_sea_indicator(key, part):
    first, second = jax.random.split(jax.random.fold_in(key, 23))
    ocean_draw = (jax.random.randint(first, (PARALLEL_TOTAL, MERIDIAN_TOTAL), 0, 4) < 3).astype(jnp.int32)
    chosen = jax.random.randint(second, (), 0, PARALLEL_TOTAL * MERIDIAN_TOTAL)
    flat_index = jnp.arange(PARALLEL_TOTAL * MERIDIAN_TOTAL, dtype=jnp.int32).reshape(PARALLEL_TOTAL, MERIDIAN_TOTAL)
    return jnp.where(flat_index == chosen, 1, ocean_draw).astype(jnp.int32)


def draw_seam_partner_index(key, part):
    block_choice = jax.random.randint(jax.random.fold_in(key, 37), (), 0, MERIDIAN_TOTAL // CX)
    centre = CX * block_choice + CX - 1
    return ((centre - jnp.arange(MERIDIAN_TOTAL, dtype=jnp.int32)) % MERIDIAN_TOTAL).astype(jnp.int32)


def place_ends(drawn, stream_key, low, top_value):
    place = [jax.random.randint(jax.random.fold_in(stream_key, axis), (), 0, length) for axis, length in enumerate(drawn.shape)]
    widest = drawn.shape.index(max(drawn.shape))
    beside = place[:widest] + [(place[widest] + 1) % drawn.shape[widest]] + place[widest + 1:]
    return drawn.at[tuple(place)].set(low).at[tuple(beside)].set(top_value)


def shard_levels(stream_key, shape, cuts, least, largest):
    level, own = 1.0, jax.random.fold_in(stream_key, 6)
    for position, blocks in cuts:
        draws = jnp.exp(jax.random.uniform(jax.random.fold_in(own, position), (blocks,), jnp.float32, least / len(cuts), largest / len(cuts)))
        level = level * jnp.repeat(draws, shape[position] // blocks).reshape([-1 if axis == position else 1 for axis in range(len(shape))])
    return level


def noise(rng, dims, scale, bound, pieces=(), kind=jnp.bfloat16):
    entries = scale * jax.random.normal(rng, dims, jnp.float32)
    if pieces:
        entries = entries * shard_levels(rng, dims, pieces, -0.22, 0.18)
    return jnp.clip(entries, -bound, bound).astype(kind)


def setup_inputs(seed: int = 0, part: int = 0) -> dict:
    splits = jax.random.split(jax.random.key(seed), 9)
    part_keys = jax.random.split(jax.random.fold_in(splits[8], part), 9)
    thermal_deviation = noise(part_keys[0], (SEA_LAYER_TOTAL, PARALLEL_TOTAL, MERIDIAN_TOTAL), 1.0, 6.0, ((1, 4), (2, 4)), jnp.float32)
    brine_content = draw_brine_content(jax.random.fold_in(jax.random.fold_in(splits[8], part), 71), part)
    current_components = noise(part_keys[2], (2, SEA_LAYER_TOTAL, PARALLEL_TOTAL, MERIDIAN_TOTAL), 1.0, 4.0, ((2, 4), (3, 4)), jnp.float32)
    sea_indicator = draw_sea_indicator(jax.random.fold_in(splits[8], 71), part)
    flooded_layer_number = place_ends(jax.random.randint(splits[4], (PARALLEL_TOTAL, MERIDIAN_TOTAL), 1, SEA_LAYER_TOTAL + 1), jax.random.fold_in(splits[4], 1), 1, SEA_LAYER_TOTAL).astype(jnp.int32)
    footprint_square_metres = jnp.clip(jnp.exp(math.log(5.0) - 2.3025851 * jax.random.uniform(splits[5], (PARALLEL_TOTAL, MERIDIAN_TOTAL), jnp.float32) ** shard_levels(splits[5], (PARALLEL_TOTAL, MERIDIAN_TOTAL), ((0, 4), (1, 4)), -0.2, 0.2)), 0.5, 5.0)
    rainfall_input = draw_rainfall_input(jax.random.fold_in(splits[8], 71), part)
    seam_partner_index = draw_seam_partner_index(jax.random.fold_in(splits[8], 71), part)
    return {"thermal_deviation": thermal_deviation, "brine_content": brine_content, "current_components": current_components, "sea_indicator": sea_indicator, "flooded_layer_number": flooded_layer_number, "footprint_square_metres": footprint_square_metres, "rainfall_input": rainfall_input, "seam_partner_index": seam_partner_index}


time_step = 0.25
diffusivity = 0.5
vertical_mixing = 0.3
top_thickness = 0.5


def face_flux(near_cells, far_cells, face_speed, near_wet, far_wet):
    upwind = jnp.maximum(face_speed, 0.0) * near_cells + jnp.minimum(face_speed, 0.0) * far_cells
    return near_wet * far_wet * (upwind - diffusivity * (far_cells - near_cells))


def reference(thermal_deviation, brine_content, current_components, sea_indicator, flooded_layer_number, footprint_square_metres, rainfall_input, seam_partner_index):
    layer_stack_number = thermal_deviation.shape[0]
    stacked_layer_number = (sea_indicator * flooded_layer_number).astype(jnp.float32)
    level_index = jnp.arange(layer_stack_number, dtype=jnp.float32)
    wet_cells = (level_index[:, None, None] < stacked_layer_number[None]).astype(jnp.float32)
    carried_quantity = jnp.stack([thermal_deviation, brine_content])
    east_tracer = jnp.roll(carried_quantity, -1, axis=3)
    east_wet = jnp.roll(wet_cells, -1, axis=2)
    east_flux = face_flux(carried_quantity, east_tracer, current_components[0], wet_cells, east_wet)
    west_flux = jnp.roll(east_flux, 1, axis=3)
    fold_tracer = carried_quantity[:, :, -1, :][:, :, seam_partner_index]
    fold_wet = wet_cells[:, -1, :][:, seam_partner_index]
    fold_velocity = current_components[1][:, -1, :][:, seam_partner_index]
    north_tracer = jnp.concatenate([carried_quantity[:, :, 1:], fold_tracer[:, :, None]], axis=2)
    north_wet = jnp.concatenate([wet_cells[:, 1:], fold_wet[:, None]], axis=1)
    fold_speed = 0.5 * (current_components[1][:, -1, :] - fold_velocity)
    north_speed = jnp.concatenate([current_components[1][:, :-1], fold_speed[:, None]], axis=1)
    north_flux = face_flux(carried_quantity, north_tracer, north_speed, wet_cells, north_wet)
    south_flux = jnp.concatenate([jnp.zeros_like(north_flux[:, :, :1]), north_flux[:, :, :-1]], axis=2)
    vertical = wet_cells[:-1] * wet_cells[1:] * vertical_mixing * (carried_quantity[:, :-1] - carried_quantity[:, 1:])
    zero_layer = jnp.zeros_like(vertical[:, :1])
    from_above = jnp.concatenate([zero_layer, vertical], axis=1)
    to_below = jnp.concatenate([vertical, zero_layer], axis=1)
    tendency = time_step / footprint_square_metres * (west_flux - east_flux + south_flux - north_flux) + time_step * (from_above - to_below)
    updated = carried_quantity + wet_cells * tendency
    wet_area = footprint_square_metres * sea_indicator.astype(jnp.float32)
    total_area = jnp.sum(wet_area)
    mean_fresh = jnp.sum(wet_area * rainfall_input) / total_area
    balanced = rainfall_input - mean_fresh
    surface = brine_content[0]
    total_salt = jnp.sum(wet_area * surface * balanced)
    virtual = -surface * balanced + total_salt / total_area
    surface_next = updated[1, 0] + time_step / top_thickness * virtual * wet_cells[0]
    salinity_next = jnp.concatenate([surface_next[None], updated[1, 1:]], axis=0)
    return (updated[0], salinity_next)
```

```python
import functools

import jax
import jax.numpy as jnp
from jax import lax
from jax.experimental import pallas as pl
from jax.experimental.pallas import tpu as pltpu
from jax.sharding import PartitionSpec as P

time_step = 0.25
diffusivity = 0.5
vertical_mixing = 0.3
top_thickness = 0.5

MESH = pl.DeviceIdType.MESH


def repeat(count, body):
    if count <= 16:
        for i in range(count):
            body(i)
    else:
        pl.loop(0, count)(body)


def face_weights(speed, open_face):
    near_weight = jnp.where(open_face, jnp.maximum(speed, 0.0) + diffusivity, 0.0)
    far_weight = jnp.where(open_face, jnp.minimum(speed, 0.0) - diffusivity, 0.0)
    return near_weight, far_weight


def kernel(
    nx, ny, nk, h, w,
    t_hbm, s_hbm, uv_hbm, sea_hbm, lay_hbm, area_hbm, rain_hbm, seam_hbm,
    t_out, s_out,
    t_v, s_v, uv_v, sea_v, lay_v, area_v, rain_v, s0_v, g_v, depth_v,
    pack_v, last_v, first_v, east_v, west_v, up_v, down_v, south_v, north_v, fold_v,
    part_v, parts_v, seam_smem,
    load_sems, pack_send, pack_recv, row_send, row_recv, fold_send, fold_recv,
    part_send, part_recv,
):
    mx, my = lax.axis_index("gx"), lax.axis_index("gy")
    is_top = my == ny - 1
    peers = nx * ny - 1

    def peer(r):
        r = r + 1
        return {"gx": lax.rem(mx + r // ny, nx), "gy": lax.rem(my + r % ny, ny)}

    barrier = pltpu.get_barrier_semaphore()

    def greet(r):
        pl.semaphore_signal(barrier, inc=1, device_id=peer(r), device_id_type=MESH)

    loads = [
        pltpu.make_async_copy(src, dst, load_sems.at[i])
        for i, (src, dst) in enumerate(
            [
                (area_hbm, area_v),
                (sea_hbm, sea_v),
                (rain_hbm, rain_v),
                (s_hbm.at[pl.ds(0, h)], s0_v),
                (lay_hbm, lay_v),
                (t_hbm, t_v),
                (s_hbm, s_v),
                (uv_hbm.at[pl.ds(0, nk * h)], uv_v.at[pl.ds(0, nk * h)]),
                (uv_hbm.at[pl.ds(nk * h, nk * h)], uv_v.at[pl.ds(nk * h, nk * h)]),
                (seam_hbm, seam_smem),
            ]
        )
    ]
    for load in loads[:4]:
        load.start()
    repeat(peers, greet)
    for load in loads[4:]:
        load.start()

    for load in loads[:4]:
        load.wait()
    area = area_v[...]
    sea = sea_v[...]
    wet_area = area * sea.astype(jnp.float32)
    surface = s0_v[...]
    fresh = wet_area * rain_v[...]
    row8 = lax.broadcasted_iota(jnp.int32, (8, w), 0)
    part = jnp.zeros((8, w), jnp.float32)
    for i, term in enumerate((wet_area, fresh, fresh * surface, wet_area * surface)):
        part = jnp.where(row8 == i, jnp.sum(term, axis=0, keepdims=True), part)
    part_v[...] = part
    gain = time_step / area
    g_v[...] = gain

    pl.semaphore_wait(barrier, peers)

    def part_copy(r):
        return pltpu.make_async_remote_copy(
            src_ref=part_v, dst_ref=parts_v.at[r],
            send_sem=part_send.at[r], recv_sem=part_recv.at[r],
            device_id=peer(r), device_id_type=MESH,
        )

    repeat(peers, lambda r: part_copy(r).start())

    for load in loads[4:]:
        load.wait()
    depth = (sea * lay_v[...]).astype(jnp.float32)
    depth_v[...] = depth

    lane = lax.broadcasted_iota(jnp.int32, (h, w), 1)
    pair = lane // 2
    packed = jnp.zeros((h, w), jnp.float32)
    for i, ref in enumerate((t_v, s_v, uv_v)):
        for k in range(nk):
            j = i * nk + k
            packed = jnp.where(pair == j, pltpu.roll(ref[pl.ds(k * h, h), :], 2 * j + 1, 1), packed)
    depth_at = 6 * nk
    packed = jnp.where(pair == 3 * nk, pltpu.roll(depth, depth_at + 1, 1), packed)
    pack_v[...] = packed
    half = h // 2
    even_half = lane[:half] % 2 == 0
    last_v[...] = jnp.where(even_half, packed[:half], pltpu.roll(packed[half:], 1, 1))
    first_v[...] = jnp.where(even_half, pltpu.roll(packed[half:], w - 1, 1), packed[:half])

    to_east = pltpu.make_async_remote_copy(
        src_ref=last_v, dst_ref=west_v, send_sem=pack_send.at[0], recv_sem=pack_recv.at[0],
        device_id={"gx": lax.rem(mx + 1, nx)}, device_id_type=MESH,
    )
    to_west = pltpu.make_async_remote_copy(
        src_ref=first_v, dst_ref=east_v, send_sem=pack_send.at[1], recv_sem=pack_recv.at[1],
        device_id={"gx": lax.rem(mx + nx - 1, nx)}, device_id_type=MESH,
    )
    to_east.start()
    to_west.start()

    def rows(ref, row, base=0):
        return ref[pl.ds(base + row, nk, stride=h), :]

    up_v[pl.ds(0, nk), :] = rows(t_v, h - 1)
    up_v[pl.ds(nk, nk), :] = rows(s_v, h - 1)
    up_v[pl.ds(2 * nk, nk), :] = rows(uv_v, h - 1, nk * h)
    up_v[pl.ds(3 * nk, 8), :] = jnp.broadcast_to(depth[h - 1 : h, :], (8, w))
    down_v[pl.ds(0, nk), :] = rows(t_v, 0)
    down_v[pl.ds(nk, nk), :] = rows(s_v, 0)
    down_v[pl.ds(2 * nk, 8), :] = jnp.broadcast_to(depth[0:1, :], (8, w))

    @pl.when(is_top)
    def _():
        up = up_v[...]
        flip = (w - 1) - lax.broadcasted_iota(jnp.int32, up.shape, 1)
        fold_v[mx] = jnp.take_along_axis(up, flip, axis=1)

    to_north = pltpu.make_async_remote_copy(
        src_ref=up_v, dst_ref=south_v, send_sem=row_send.at[0], recv_sem=row_recv.at[0],
        device_id={"gy": lax.rem(my + 1, ny)}, device_id_type=MESH,
    )
    to_south = pltpu.make_async_remote_copy(
        src_ref=down_v, dst_ref=north_v, send_sem=row_send.at[1], recv_sem=row_recv.at[1],
        device_id={"gy": lax.rem(my + ny - 1, ny)}, device_id_type=MESH,
    )

    def fold_copy(d):
        return pltpu.make_async_remote_copy(
            src_ref=fold_v.at[mx], dst_ref=fold_v.at[mx],
            send_sem=fold_send.at[d], recv_sem=fold_recv.at[d],
            device_id={"gx": lax.rem(mx + d + 1, nx)}, device_id_type=MESH,
        )


    @pl.when(jnp.logical_not(is_top))
    def _():
        to_north.start()

    @pl.when(my > 0)
    def _():
        to_south.start()

    @pl.when(is_top)
    def _():
        repeat(nx - 1, lambda d: fold_copy(d).start())

    row = lax.broadcasted_iota(jnp.int32, (h, w), 0)
    depth_east = jnp.where(lane == w - 1, 0.0, jnp.minimum(depth, pltpu.roll(depth, w - 1, 1)))
    depth_north = jnp.where(row == h - 1, 0.0, jnp.minimum(depth, pltpu.roll(depth, h - 1, 0)))

    def level(k, above):
        kf = k.astype(jnp.float32)
        at = pl.ds(pl.multiple_of(k * h, h), h)
        below = pl.ds(pl.multiple_of(jnp.minimum(k + 1, nk - 1) * h, h), h)
        east_near, east_far = face_weights(uv_v[at, :], depth_east > kf)
        north_near, north_far = face_weights(
            uv_v[pl.ds(pl.multiple_of((k + nk) * h, h), h), :], depth_north > kf
        )
        mix = jnp.where(depth_v[...] > kf + 1.0, time_step * vertical_mixing, 0.0)
        gain = g_v[...]
        falls = []
        for ref, out, came in ((t_v, t_out, above[0]), (s_v, s_out, above[1])):
            c = ref[at, :]
            east = east_near * c + east_far * pltpu.roll(c, w - 1, 1)
            north = north_near * c + north_far * pltpu.roll(c, h - 1, 0)
            flow = (pltpu.roll(east, 1, 1) - east) + (pltpu.roll(north, 1, 0) - north)
            fall = mix * (c - ref[below, :])
            out[at, :] = c + (gain * flow + (came - fall))
            falls.append(fall)
        return tuple(falls)

    zero = jnp.zeros((h, w), jnp.float32)
    lax.fori_loop(0, nk, level, (zero, zero))

    level_row = lax.broadcasted_iota(jnp.int32, (nk, w), 0).astype(jnp.float32)

    def north_edge(far_t, far_s, speed, far_depth):
        near_weight, far_weight = face_weights(
            speed, jnp.minimum(up_v[3 * nk : 3 * nk + 1, :], far_depth) > level_row
        )
        for near, far, out in (
            (up_v[pl.ds(0, nk), :], far_t, t_out),
            (up_v[pl.ds(nk, nk), :], far_s, s_out),
        ):
            at = pl.ds(h - 1, nk, stride=h)
            out[at, :] -= g_v[h - 1 : h, :] * (near_weight * near + far_weight * far)

    @pl.when(jnp.logical_not(is_top))
    def _():
        to_north.wait_send()
        to_south.wait_recv()
        north_edge(
            north_v[pl.ds(0, nk), :],
            north_v[pl.ds(nk, nk), :],
            up_v[pl.ds(2 * nk, nk), :],
            north_v[2 * nk : 2 * nk + 1, :],
        )

    @pl.when(my > 0)
    def _():
        to_south.wait_send()
        to_north.wait_recv()
        near_weight, far_weight = face_weights(
            south_v[pl.ds(2 * nk, nk), :],
            jnp.minimum(down_v[2 * nk : 2 * nk + 1, :], south_v[3 * nk : 3 * nk + 1, :]) > level_row,
        )
        for i, out in enumerate((t_out, s_out)):
            at = pl.ds(0, nk, stride=h)
            out[at, :] += g_v[0:1, :] * (
                near_weight * south_v[pl.ds(i * nk, nk), :]
                + far_weight * down_v[pl.ds(i * nk, nk), :]
            )

    to_east.wait()
    to_west.wait()
    mine, east_half, west_half = pack_v[...], east_v[...], west_v[...]
    east_side = jnp.concatenate([east_half, pltpu.roll(east_half, 1, 1)], axis=0)
    west_side = jnp.concatenate([west_half, pltpu.roll(west_half, w - 1, 1)], axis=0)
    even = lane % 2 == 0

    def speeds(cells):
        return jnp.where(
            pair < nk, pltpu.roll(cells, w - 4 * nk, 1), pltpu.roll(cells, w - 2 * nk, 1)
        )

    def column(cells, at):
        return jnp.broadcast_to(cells[:, at : at + 1], (h, w))

    near = jnp.where(even, mine, pltpu.roll(west_side, 1, 1))
    far = jnp.where(even, pltpu.roll(east_side, w - 1, 1), mine)
    speed = jnp.where(even, speeds(mine), pltpu.roll(speeds(west_side), 1, 1))
    shallow = jnp.where(
        even,
        jnp.minimum(column(mine, depth_at), column(east_side, depth_at + 1)),
        jnp.minimum(column(mine, depth_at + 1), column(west_side, depth_at)),
    )
    near_weight, far_weight = face_weights(speed, shallow > (pair % nk).astype(jnp.float32))
    gain = g_v[...]
    edge_gain = jnp.where(even, -column(gain, w - 1), column(gain, 0))
    edge = edge_gain * (near_weight * near + far_weight * far)
    at_edge = (lane == 0) | (lane == w - 1)
    for i, out in enumerate((t_out, s_out)):
        for k in range(nk):
            shift = (w - (2 * (i * nk + k) + 1)) % w
            out[pl.ds(k * h, h), :] += jnp.where(at_edge, pltpu.roll(edge, shift, 1), 0.0)

    @pl.when(is_top)
    def _():
        repeat(nx - 1, lambda d: fold_copy(d).wait())
        partner = fold_v[seam_smem[0] // w]
        north_edge(
            partner[:nk],
            partner[nk : 2 * nk],
            0.5 * (up_v[pl.ds(2 * nk, nk), :] - partner[2 * nk : 3 * nk]),
            partner[3 * nk : 3 * nk + 1],
        )

    repeat(peers, lambda r: part_copy(r).wait())
    totals = part_v[...] + jnp.sum(parts_v[...], axis=0)
    totals = jnp.sum(totals, axis=1, keepdims=True)
    total_area, total_fresh = totals[0:1], totals[1:2]
    salt_fresh, salt_only = totals[2:3], totals[3:4]
    mean_fresh = total_fresh / total_area
    lift = (salt_fresh - mean_fresh * salt_only) / total_area
    virtual = lift - s0_v[...] * (rain_v[...] - mean_fresh)
    s_out[pl.ds(0, h), :] += jnp.where(depth_v[...] > 0.0, time_step / top_thickness * virtual, 0.0)


store_cuts = 1


def store_kernel(t_ref, s_ref, t_out, s_out, sems):
    step = t_ref.shape[0] // store_cuts
    copies = [
        pltpu.make_async_copy(
            src.at[pl.ds(i * step, step)], dst.at[pl.ds(i * step, step)], sems.at[2 * i + n]
        )
        for i in range(store_cuts)
        for n, (src, dst) in enumerate(((t_ref, t_out), (s_ref, s_out)))
    ]
    for copy in copies:
        copy.start()
    for copy in copies:
        copy.wait()


def shards(nx, ny, t, s, uv, sea, layers, area, rain, seam):
    nk, h, w = t.shape
    assert w == 128 and h % 16 == 0 and nk % 8 == 0 and 6 * nk + 2 <= w
    f32 = jnp.float32
    peers = nx * ny - 1
    half_plane = pltpu.VMEM((h // 2, w), f32)
    any_space = pl.BlockSpec(memory_space=pl.ANY)
    dma = pltpu.SemaphoreType.DMA
    plane = pltpu.VMEM((h, w), f32)
    t_next, s_next = pl.pallas_call(
        functools.partial(kernel, nx, ny, nk, h, w),
        out_shape=[pltpu.VMEM((nk * h, w), f32)] * 2,
        in_specs=[any_space] * 8,
        out_specs=[pl.BlockSpec(memory_space=pltpu.VMEM)] * 2,
        scratch_shapes=[
            pltpu.VMEM((nk * h, w), f32),
            pltpu.VMEM((nk * h, w), f32),
            pltpu.VMEM((2 * nk * h, w), f32),
            pltpu.VMEM((h, w), jnp.int32),
            pltpu.VMEM((h, w), jnp.int32),
            plane, plane, plane, plane, plane,
            plane, half_plane, half_plane, half_plane, half_plane,
            pltpu.VMEM((3 * nk + 8, w), f32),
            pltpu.VMEM((2 * nk + 8, w), f32),
            pltpu.VMEM((3 * nk + 8, w), f32),
            pltpu.VMEM((2 * nk + 8, w), f32),
            pltpu.VMEM((nx, 3 * nk + 8, w), f32),
            pltpu.VMEM((8, w), f32),
            pltpu.VMEM((peers, 8, w), f32),
            pltpu.SMEM((w,), jnp.int32),
            dma((10,)), dma((2,)), dma((2,)), dma((2,)), dma((2,)),
            dma((nx - 1,)), dma((nx - 1,)), dma((peers,)), dma((peers,)),
        ],
        compiler_params=pltpu.CompilerParams(
            collective_id=0, has_side_effects=True, vmem_limit_bytes=65990000
        ),
        name="tracer_step",
    )(
        t.reshape(nk * h, w), s.reshape(nk * h, w), uv.reshape(2 * nk * h, w),
        sea, layers, area, rain, seam,
    )
    t_next, s_next = pl.pallas_call(
        store_kernel,
        out_shape=[jax.ShapeDtypeStruct((nk * h, w), f32)] * 2,
        in_specs=[any_space] * 2,
        out_specs=[any_space] * 2,
        scratch_shapes=[dma((2 * store_cuts,))],
        compiler_params=pltpu.CompilerParams(vmem_limit_bytes=8 << 20),
        name="store",
    )(t_next, s_next)
    return t_next.reshape(t.shape), s_next.reshape(s.shape)


def solution(mesh):
    in_specs = (
        P("groups", "gy", "gx"),
        P("groups", "gy", "gx"),
        P("groups", None, "gy", "gx"),
        P("gy", "gx"),
        P("gy", "gx"),
        P("gy", "gx"),
        P("gy", "gx"),
        P("gx"),
    )
    out_specs = (P("groups", "gy", "gx"), P("groups", "gy", "gx"))
    return jax.shard_map(
        functools.partial(shards, mesh.shape["gx"], mesh.shape["gy"]),
        mesh=mesh, in_specs=in_specs, out_specs=out_specs, check_vma=False,
    )
```

```python
import functools

import jax
import jax.numpy as jnp
from jax import lax
from jax.experimental import pallas as pl
from jax.experimental.pallas import tpu as pltpu
from jax.sharding import PartitionSpec as P

time_step = 0.25
diffusivity = 0.5
vertical_mixing = 0.3
top_thickness = 0.5

MESH = pl.DeviceIdType.MESH


def repeat(count, body):
    if count <= 16:
        for i in range(count):
            body(i)
    else:
        pl.loop(0, count)(body)


def face_weights(speed, open_face):
    near_weight = jnp.where(open_face, jnp.maximum(speed, 0.0) + diffusivity, 0.0)
    far_weight = jnp.where(open_face, jnp.minimum(speed, 0.0) - diffusivity, 0.0)
    return near_weight, far_weight


def kernel(
    nx, ny, nk, h, w,
    t_hbm, s_hbm, uv_hbm, sea_hbm, lay_hbm, area_hbm, rain_hbm, seam_hbm,
    t_out, s_out, edge_out,
    t_v, s_v, uv_v, sea_v, lay_v, area_v, rain_v, s0_v, g_v, depth_v,
    pack_v, last_v, first_v, east_v, west_v, up_v, down_v, south_v, north_v, fold_v,
    part_v, parts_v, seam_smem,
    load_sems, pack_send, pack_recv, row_send, row_recv, fold_send, fold_recv,
    part_send, part_recv,
):
    mx, my = lax.axis_index("gx"), lax.axis_index("gy")
    is_top = my == ny - 1
    peers = nx * ny - 1

    def peer(r):
        r = r + 1
        return {"gx": lax.rem(mx + r // ny, nx), "gy": lax.rem(my + r % ny, ny)}

    barrier = pltpu.get_barrier_semaphore()

    def greet(r):
        pl.semaphore_signal(barrier, inc=1, device_id=peer(r), device_id_type=MESH)

    loads = [
        pltpu.make_async_copy(src, dst, load_sems.at[i])
        for i, (src, dst) in enumerate(
            [
                (area_hbm, area_v),
                (sea_hbm, sea_v),
                (rain_hbm, rain_v),
                (s_hbm.at[pl.ds(0, h)], s0_v),
                (lay_hbm, lay_v),
                (t_hbm, t_v),
                (s_hbm, s_v),
                (uv_hbm.at[pl.ds(0, nk * h)], uv_v.at[pl.ds(0, nk * h)]),
                (uv_hbm.at[pl.ds(nk * h, nk * h)], uv_v.at[pl.ds(nk * h, nk * h)]),
                (seam_hbm, seam_smem),
            ]
        )
    ]
    for load in loads[:4]:
        load.start()
    repeat(peers, greet)
    for load in loads[4:]:
        load.start()

    for load in loads[:4]:
        load.wait()
    area = area_v[...]
    sea = sea_v[...]
    wet_area = area * sea.astype(jnp.float32)
    surface = s0_v[...]
    fresh = wet_area * rain_v[...]
    lane1 = lax.broadcasted_iota(jnp.int32, (1, w), 1)
    part = jnp.zeros((1, w), jnp.float32)
    for i, term in enumerate((wet_area, fresh, fresh * surface, wet_area * surface)):
        rows8 = jnp.sum(term.reshape(h // 8, 8, w), axis=0)
        part = jnp.where(
            lane1 == i, jnp.sum(jnp.sum(rows8, axis=1, keepdims=True), axis=0, keepdims=True), part
        )
    part_v[...] = part
    gain = time_step / area
    g_v[...] = gain

    me = mx * ny + my
    parts_v[me] = part

    def send_part(r):
        @pl.when(r != me)
        def _():
            pltpu.make_async_remote_copy(
                src_ref=part_v, dst_ref=parts_v.at[me], send_sem=part_send, recv_sem=part_recv,
                device_id={"gx": r // ny, "gy": r % ny}, device_id_type=MESH,
            ).start()

    others = parts_v.at[pl.ds(0, peers)]
    all_parts = pltpu.make_async_remote_copy(
        src_ref=others, dst_ref=others, send_sem=part_send, recv_sem=part_recv,
        device_id=peer(0), device_id_type=MESH,
    )

    def meet():
        pl.semaphore_wait(barrier, peers)
        repeat(ny, send_part)

    early = mx == 0
    pl.when(jnp.logical_not(early))(meet)

    loads[4].wait()
    depth = (sea * lay_v[...]).astype(jnp.float32)
    depth_v[...] = depth

    half = h // 2
    depth_at = 6 * nk
    lane = lax.broadcasted_iota(jnp.int32, (h, w), 1)
    row = lax.broadcasted_iota(jnp.int32, (h, w), 0)
    slot = jnp.where(row < half, lane, lane - 1)
    pair = slot >> 1
    eastern = (slot & 1) == 0
    even_half = (lane[:half] & 1) == 0

    def spread(plane, j):
        return jnp.concatenate(
            [pltpu.roll(plane[:half], 2 * j + 1, 1), pltpu.roll(plane[half:], 2 * j + 2, 1)], axis=0
        )

    packed = jnp.where(pair == 3 * nk, spread(depth, 3 * nk), 0.0)
    for i, (load, ref) in enumerate(zip(loads[5:8], (t_v, s_v, uv_v))):
        load.wait()
        for k in range(nk):
            j = i * nk + k
            packed = jnp.where(pair == j, spread(ref[pl.ds(k * h, h), :], j), packed)
    last_v[...] = jnp.where(even_half, packed[:half], packed[half:])
    first_v[...] = jnp.where(even_half, packed[half:], packed[:half])

    to_east = pltpu.make_async_remote_copy(
        src_ref=last_v, dst_ref=west_v, send_sem=pack_send.at[0], recv_sem=pack_recv.at[0],
        device_id={"gx": lax.rem(mx + 1, nx)}, device_id_type=MESH,
    )
    to_west = pltpu.make_async_remote_copy(
        src_ref=first_v, dst_ref=east_v, send_sem=pack_send.at[1], recv_sem=pack_recv.at[1],
        device_id={"gx": lax.rem(mx + nx - 1, nx)}, device_id_type=MESH,
    )
    depth_east = jnp.where(lane == w - 1, 0.0, jnp.minimum(depth, pltpu.roll(depth, w - 1, 1)))
    depth_north = jnp.where(row == h - 1, 0.0, jnp.minimum(depth, pltpu.roll(depth, h - 1, 0)))

    def level(k, above):
        kf = k.astype(jnp.float32)
        at = pl.ds(pl.multiple_of(k * h, h), h)
        below = pl.ds(pl.multiple_of(jnp.minimum(k + 1, nk - 1) * h, h), h)
        east_near, east_far = face_weights(uv_v[at, :], depth_east > kf)
        north_near, north_far = face_weights(
            uv_v[pl.ds(pl.multiple_of((k + nk) * h, h), h), :], depth_north > kf
        )
        mix = jnp.where(depth_v[...] > kf + 1.0, time_step * vertical_mixing, 0.0)
        gain = g_v[...]
        falls = []
        for ref, out, came in ((t_v, t_out, above[0]), (s_v, s_out, above[1])):
            c = ref[at, :]
            east = east_near * c + east_far * pltpu.roll(c, w - 1, 1)
            north = north_near * c + north_far * pltpu.roll(c, h - 1, 0)
            flow = (pltpu.roll(east, 1, 1) - east) + (pltpu.roll(north, 1, 0) - north)
            fall = mix * (c - ref[below, :])
            out[at, :] = c + (gain * flow + (came - fall))
            falls.append(fall)
        return tuple(falls)

    zero = jnp.zeros((h, w), jnp.float32)
    pack_v[...] = packed
    split = jnp.where(early, nk, 0)

    @pl.when(early)
    def _():
        for load in loads[8:]:
            load.wait()

    falls = lax.fori_loop(0, split, level, (zero, zero))
    pl.when(early)(meet)
    to_east.start()
    to_west.start()
    repeat(peers - ny + 1, lambda r: send_part(r + ny))

    @pl.when(jnp.logical_not(early))
    def _():
        for load in loads[8:]:
            load.wait()


    def rows(ref, row, base=0):
        return ref[pl.ds(base + row, nk, stride=h), :]

    up_v[pl.ds(0, nk), :] = rows(t_v, h - 1)
    up_v[pl.ds(nk, nk), :] = rows(s_v, h - 1)
    up_v[pl.ds(2 * nk, nk), :] = rows(uv_v, h - 1, nk * h)
    up_v[pl.ds(3 * nk, 8), :] = jnp.broadcast_to(depth[h - 1 : h, :], (8, w))
    down_v[pl.ds(0, nk), :] = rows(t_v, 0)
    down_v[pl.ds(nk, nk), :] = rows(s_v, 0)
    down_v[pl.ds(2 * nk, 8), :] = jnp.broadcast_to(depth[0:1, :], (8, w))

    @pl.when(is_top)
    def _():
        up = up_v[...]
        flip = (w - 1) - lax.broadcasted_iota(jnp.int32, up.shape, 1)
        fold_v[mx] = jnp.take_along_axis(up, flip, axis=1)

    to_north = pltpu.make_async_remote_copy(
        src_ref=up_v, dst_ref=south_v, send_sem=row_send.at[0], recv_sem=row_recv.at[0],
        device_id={"gy": lax.rem(my + 1, ny)}, device_id_type=MESH,
    )
    to_south = pltpu.make_async_remote_copy(
        src_ref=down_v, dst_ref=north_v, send_sem=row_send.at[1], recv_sem=row_recv.at[1],
        device_id={"gy": lax.rem(my + ny - 1, ny)}, device_id_type=MESH,
    )

    def fold_copy(d):
        return pltpu.make_async_remote_copy(
            src_ref=fold_v.at[mx], dst_ref=fold_v.at[mx],
            send_sem=fold_send.at[d], recv_sem=fold_recv.at[d],
            device_id={"gx": lax.rem(mx + d + 1, nx)}, device_id_type=MESH,
        )


    @pl.when(jnp.logical_not(is_top))
    def _():
        to_north.start()

    @pl.when(my > 0)
    def _():
        to_south.start()

    @pl.when(is_top)
    def _():
        repeat(nx - 1, lambda d: fold_copy(d).start())

    lax.fori_loop(split, nk, level, falls)

    level_row = lax.broadcasted_iota(jnp.int32, (nk, w), 0).astype(jnp.float32)

    def north_edge(far_t, far_s, speed, far_depth):
        near_weight, far_weight = face_weights(
            speed, jnp.minimum(up_v[3 * nk : 3 * nk + 1, :], far_depth) > level_row
        )
        for near, far, out in (
            (up_v[pl.ds(0, nk), :], far_t, t_out),
            (up_v[pl.ds(nk, nk), :], far_s, s_out),
        ):
            at = pl.ds(h - 1, nk, stride=h)
            out[at, :] -= g_v[h - 1 : h, :] * (near_weight * near + far_weight * far)

    @pl.when(jnp.logical_not(is_top))
    def _():
        to_north.wait_send()
        to_south.wait_recv()
        north_edge(
            north_v[pl.ds(0, nk), :],
            north_v[pl.ds(nk, nk), :],
            up_v[pl.ds(2 * nk, nk), :],
            north_v[2 * nk : 2 * nk + 1, :],
        )

    @pl.when(my > 0)
    def _():
        to_south.wait_send()
        to_north.wait_recv()
        near_weight, far_weight = face_weights(
            south_v[pl.ds(2 * nk, nk), :],
            jnp.minimum(down_v[2 * nk : 2 * nk + 1, :], south_v[3 * nk : 3 * nk + 1, :]) > level_row,
        )
        for i, out in enumerate((t_out, s_out)):
            at = pl.ds(0, nk, stride=h)
            out[at, :] += g_v[0:1, :] * (
                near_weight * south_v[pl.ds(i * nk, nk), :]
                + far_weight * down_v[pl.ds(i * nk, nk), :]
            )

    @pl.when(is_top)
    def _():
        repeat(nx - 1, lambda d: fold_copy(d).wait())
        partner = fold_v[seam_smem[0] // w]
        north_edge(
            partner[:nk],
            partner[nk : 2 * nk],
            0.5 * (up_v[pl.ds(2 * nk, nk), :] - partner[2 * nk : 3 * nk]),
            partner[3 * nk : 3 * nk + 1],
        )

    all_parts.wait()
    totals = jnp.sum(parts_v[...], axis=0)
    total_area, total_fresh, salt_fresh, salt_only = (
        jnp.broadcast_to(totals[:, i : i + 1], (1, w)) for i in range(4)
    )
    mean_fresh = total_fresh / total_area
    lift = (salt_fresh - mean_fresh * salt_only) / total_area
    virtual = lift - s0_v[...] * (rain_v[...] - mean_fresh)
    s_out[pl.ds(0, h), :] += jnp.where(depth_v[...] > 0.0, time_step / top_thickness * virtual, 0.0)

    def column(cells, upper, lower):
        return jnp.concatenate(
            [
                jnp.broadcast_to(cells[:half, upper : upper + 1], (half, w)),
                jnp.broadcast_to(cells[-half:, lower : lower + 1], (half, w)),
            ],
            axis=0,
        )

    def both(cells):
        return jnp.concatenate([cells, cells], axis=0)

    def speeds(cells, shift):
        return (
            pltpu.roll(cells, (shift + w - 4 * nk) % w, 1),
            pltpu.roll(cells, (shift + w - 2 * nk) % w, 1),
        )

    mine = pack_v[...]
    own_t, own_s = speeds(mine, 0)
    depth = depth_v[...]
    own_depth = jnp.where(eastern, column(depth, w - 1, w - 1), column(depth, 0, 0))
    gain = g_v[...]
    edge_gain = jnp.where(eastern, -column(gain, w - 1, w - 1), column(gain, 0, 0))
    edge_gain = jnp.where(own_depth > (pair & (nk - 1)).astype(jnp.float32), edge_gain, 0.0)

    to_east.wait()
    to_west.wait()
    west, east = west_v[...], east_v[...]
    west_t, west_s = speeds(west, 1)
    near = jnp.where(eastern, mine, both(pltpu.roll(west, 1, 1)))
    far = jnp.where(eastern, both(pltpu.roll(east, w - 1, 1)), mine)
    speed = jnp.where(
        eastern,
        jnp.where(pair < nk, own_t, own_s),
        jnp.where(pair < nk, both(west_t), both(west_s)),
    )
    far_depth = jnp.where(
        eastern,
        column(east, depth_at + 1, depth_at + 2),
        column(west, depth_at, depth_at + 1),
    )
    near_weight, far_weight = face_weights(
        speed, far_depth > (pair & (nk - 1)).astype(jnp.float32)
    )
    edge_out[...] = edge_gain * (near_weight * near + far_weight * far)


store_cuts = 4


def store_kernel(nk, h, w, t_ref, s_ref, edge_ref, t_hbm, s_hbm, t_v, s_v, sems):
    half = h // 2
    lane = lax.broadcasted_iota(jnp.int32, (half, w), 1)
    at_edge = (lane == 0) | (lane == w - 1)
    step = nk // store_cuts
    copies = []
    for i, (ref, out, hbm) in enumerate(((t_ref, t_v, t_hbm), (s_ref, s_v, s_hbm))):
        for cut in range(store_cuts):
            for k in range(cut * step, (cut + 1) * step):
                j = i * nk + k
                for part, shift in ((0, w - 1 - 2 * j), (1, w - 2 - 2 * j)):
                    moved = pltpu.roll(edge_ref[pl.ds(part * half, half), :], shift % w, 1)
                    at = pl.ds(k * h + part * half, half)
                    out[at, :] = ref[at, :] + jnp.where(at_edge, moved, 0.0)
            at = pl.ds(cut * step * h, step * h)
            copy = pltpu.make_async_copy(out.at[at], hbm.at[at], sems.at[len(copies)])
            copy.start()
            copies.append(copy)
    for copy in copies:
        copy.wait()


def shards(nx, ny, t, s, uv, sea, layers, area, rain, seam):
    nk, h, w = t.shape
    assert w == 128 and h % 16 == 0 and nk & (nk - 1) == 0 and nk % 8 == 0 and 6 * nk + 3 <= w
    f32 = jnp.float32
    peers = nx * ny - 1
    half_plane = pltpu.VMEM((h // 2, w), f32)
    any_space = pl.BlockSpec(memory_space=pl.ANY)
    dma = pltpu.SemaphoreType.DMA
    plane = pltpu.VMEM((h, w), f32)
    t_next, s_next, edge = pl.pallas_call(
        functools.partial(kernel, nx, ny, nk, h, w),
        out_shape=[pltpu.VMEM((nk * h, w), f32)] * 2 + [pltpu.VMEM((h, w), f32)],
        in_specs=[any_space] * 8,
        out_specs=[pl.BlockSpec(memory_space=pltpu.VMEM)] * 3,
        scratch_shapes=[
            pltpu.VMEM((nk * h, w), f32),
            pltpu.VMEM((nk * h, w), f32),
            pltpu.VMEM((2 * nk * h, w), f32),
            pltpu.VMEM((h, w), jnp.int32),
            pltpu.VMEM((h, w), jnp.int32),
            plane, plane, plane, plane, plane,
            plane, half_plane, half_plane, half_plane, half_plane,
            pltpu.VMEM((3 * nk + 8, w), f32),
            pltpu.VMEM((2 * nk + 8, w), f32),
            pltpu.VMEM((3 * nk + 8, w), f32),
            pltpu.VMEM((2 * nk + 8, w), f32),
            pltpu.VMEM((nx, 3 * nk + 8, w), f32),
            pltpu.VMEM((1, w), f32),
            pltpu.VMEM((nx * ny, 1, w), f32),
            pltpu.SMEM((w,), jnp.int32),
            dma((10,)), dma((2,)), dma((2,)), dma((2,)), dma((2,)),
            dma((nx - 1,)), dma((nx - 1,)), dma, dma,
        ],
        compiler_params=pltpu.CompilerParams(
            collective_id=0, has_side_effects=True, vmem_limit_bytes=65961984
        ),
        name="tracer_step",
    )(
        t.reshape(nk * h, w), s.reshape(nk * h, w), uv.reshape(2 * nk * h, w),
        sea, layers, area, rain, seam,
    )
    t_next, s_next = pl.pallas_call(
        functools.partial(store_kernel, nk, h, w),
        out_shape=[jax.ShapeDtypeStruct((nk * h, w), f32)] * 2,
        in_specs=[pl.BlockSpec(memory_space=pltpu.VMEM)] * 3,
        out_specs=[any_space] * 2,
        scratch_shapes=[pltpu.VMEM((nk * h, w), f32)] * 2 + [dma((2 * store_cuts,))],
        compiler_params=pltpu.CompilerParams(vmem_limit_bytes=8 << 20),
        name="store",
    )(t_next, s_next, edge)
    return t_next.reshape(t.shape), s_next.reshape(s.shape)


def solution(mesh):
    in_specs = (
        P("groups", "gy", "gx"),
        P("groups", "gy", "gx"),
        P("groups", None, "gy", "gx"),
        P("gy", "gx"),
        P("gy", "gx"),
        P("gy", "gx"),
        P("gy", "gx"),
        P("gx"),
    )
    out_specs = (P("groups", "gy", "gx"), P("groups", "gy", "gx"))
    return jax.shard_map(
        functools.partial(shards, mesh.shape["gx"], mesh.shape["gy"]),
        mesh=mesh, in_specs=in_specs, out_specs=out_specs, check_vma=False,
    )
```

```python
import functools

import jax
import jax.numpy as jnp
from jax import lax
from jax.experimental import pallas as pl
from jax.experimental.pallas import tpu as pltpu
from jax.sharding import PartitionSpec as P

time_step = 0.25
diffusivity = 0.5
vertical_mixing = 0.3
top_thickness = 0.5

block_rows = 16
hubs = 2

MESH = pl.DeviceIdType.MESH


def repeat(count, body):
    if count <= 16:
        for i in range(count):
            body(i)
    else:
        pl.loop(0, count)(body)


def face_weights(speed, open_face):
    near_weight = jnp.maximum(speed, 0.0) + diffusivity
    far_weight = speed - near_weight
    return jnp.where(open_face, near_weight, 0.0), jnp.where(open_face, far_weight, 0.0)


def kernel(
    nx, ny, nk, h, w,
    t_hbm, s_hbm, uv_hbm, sea_hbm, lay_hbm, area_hbm, rain_hbm, seam_hbm,
    t_out, s_out, side_out,
    t_v, s_v, uv_v, sea_v, lay_v, area_v, rain_v, s0_v, g_v, depth_v,
    pack_v, last_v, first_v, east_v, west_v, up_v, down_v, south_v, north_v, fold_v,
    part_v, parts_v, total_v, seam_smem, depth_east_v, depth_north_v, flux_v,
    load_sems, pack_send, pack_recv, row_send, row_recv, fold_send, fold_recv,
    part_send, part_recv, total_send, total_recv,
):
    mx, my = lax.axis_index("gx"), lax.axis_index("gy")
    is_top = my == ny - 1
    peers = nx * ny - 1

    barrier = pltpu.get_barrier_semaphore()

    east, west = lax.rem(mx + 1, nx), lax.rem(mx + nx - 1, nx)
    is_hub = mx < hubs
    outside = jnp.logical_not(is_hub)

    def count(flag):
        return jnp.where(flag, 1, 0)

    far_sides = count(east >= hubs) + count(west >= hubs)
    partners = (
        hubs * ny - count(is_hub) + far_sides
        + jnp.where(outside, count(my > 0) + count(my < ny - 1), 0)
        + jnp.where(is_top, nx - hubs - count(outside) - far_sides, 0)
    )

    def signal(gx, gy):
        pl.semaphore_signal(
            barrier, inc=1, device_id={"gx": gx, "gy": gy}, device_id_type=MESH
        )

    def greet():
        @pl.when(is_hub)
        def _():
            def one(r):
                r = r + 1
                signal(lax.rem(mx + r // ny, nx), lax.rem(my + r % ny, ny))

            repeat(peers, one)

        @pl.when(outside)
        def _():
            signal(west, my)
            signal(east, my)
            pl.when(my > 0)(lambda: signal(mx, my - 1))
            pl.when(my < ny - 1)(lambda: signal(mx, my + 1))

        @pl.when(outside & is_top)
        def _():
            repeat(nx - 3, lambda d: signal(lax.rem(mx + 2 + d, nx), my))

    loads = [
        pltpu.make_async_copy(src, dst, load_sems.at[i])
        for i, (src, dst) in enumerate(
            [
                (area_hbm, area_v),
                (sea_hbm, sea_v),
                (rain_hbm, rain_v),
                (s_hbm.at[pl.ds(0, h)], s0_v),
                (lay_hbm, lay_v),
                (t_hbm, t_v.at[pl.ds(0, nk * h)]),
                (s_hbm, s_v.at[pl.ds(0, nk * h)]),
                (uv_hbm.at[pl.ds(0, nk * h)], uv_v.at[pl.ds(0, nk * h)]),
                (uv_hbm.at[pl.ds(nk * h, nk * h)], uv_v.at[pl.ds(nk * h, nk * h)]),
                (seam_hbm, seam_smem),
            ]
        )
    ]
    for load in loads[:8]:
        load.start()
    greet()
    for load in loads[8:]:
        load.start()
    zeros = jnp.zeros((8, w), jnp.float32)
    for ref in (t_v, s_v):
        ref[pl.ds(nk * h, 8), :] = zeros
    for i in range(2 * nk):
        flux_v[pl.ds(i * (h + 8), 8), :] = zeros

    for load in loads[:4]:
        load.wait()
    area = area_v[...]
    sea = sea_v[...]
    wet_area = area * sea.astype(jnp.float32)
    surface = s0_v[...]
    fresh = wet_area * rain_v[...]
    lane1 = lax.broadcasted_iota(jnp.int32, (1, w), 1)
    part = jnp.zeros((1, w), jnp.float32)
    for i, term in enumerate((wet_area, fresh, fresh * surface, wet_area * surface)):
        rows8 = jnp.sum(term.reshape(h // 8, 8, w), axis=0)
        part = jnp.where(
            lane1 == i, jnp.sum(jnp.sum(rows8, axis=1, keepdims=True), axis=0, keepdims=True), part
        )
    part_v[...] = part
    gain = time_step / area
    g_v[...] = gain

    me = mx * ny + my
    parts_v[me] = part

    def send_part(r):
        @pl.when(r != me)
        def _():
            pltpu.make_async_remote_copy(
                src_ref=part_v, dst_ref=parts_v.at[me], send_sem=part_send, recv_sem=part_recv,
                device_id={"gx": r // ny, "gy": r % ny}, device_id_type=MESH,
            ).start()

    def several(ref, n, sends, arrivals):
        block = ref.at[pl.ds(0, n)]
        return pltpu.make_async_remote_copy(
            src_ref=block, dst_ref=block, send_sem=sends, recv_sem=arrivals,
            device_id={"gx": east}, device_id_type=MESH,
        )

    def hand_on(d):
        return pltpu.make_async_remote_copy(
            src_ref=total_v, dst_ref=total_v, send_sem=total_send, recv_sem=total_recv,
            device_id={"gx": hubs + d}, device_id_type=MESH,
        )

    def meet():
        pl.semaphore_wait(barrier, partners)
        repeat(hubs * ny, send_part)

    early = mx == 0
    pl.when(jnp.logical_not(early))(meet)

    loads[4].wait()
    depth = (sea * lay_v[...]).astype(jnp.float32)
    depth_v[...] = depth

    half = h // 2
    depth_at = 6 * nk
    lane = lax.broadcasted_iota(jnp.int32, (h, w), 1)
    row = lax.broadcasted_iota(jnp.int32, (h, w), 0)
    slot = jnp.where(row < half, lane, lane - 1)
    pair = slot >> 1
    eastern = (slot & 1) == 0
    even_half = (lane[:half] & 1) == 0

    quarter = h // 4

    def cells(ref, k, b):
        return [
            ref[pl.ds(k * h + side * half + b * quarter, quarter), :] for side in (0, 1)
        ]

    def pack(packed, b, ref, first, count):
        for k in range(count):
            j = first + k
            packed = [
                jnp.where(
                    pair[side * half : side * half + quarter] == j,
                    pltpu.roll(plane, 2 * j + 1 + side, 1),
                    old,
                )
                for side, (plane, old) in enumerate(zip(cells(ref, k, b), packed))
            ]
        return packed

    empty = [jnp.zeros((quarter, w), jnp.float32)] * 2
    packed = [pack(empty, b, depth_v, 3 * nk, 1) for b in (0, 1)]
    for i, ref in enumerate((t_v, s_v)):
        loads[5 + i].wait()
        packed = [pack(packed[b], b, ref, i * nk, nk) for b in (0, 1)]
    loads[7].wait()

    def finish(b):
        upper, lower = pack(packed[b], b, uv_v, 2 * nk, nk)
        pack_v[pl.ds(b * quarter, quarter), :] = upper
        pack_v[pl.ds(half + b * quarter, quarter), :] = lower
        at = pl.ds(b * quarter, quarter)
        last_v[at, :] = jnp.where(even_half[:quarter], upper, lower)
        first_v[at, :] = jnp.where(even_half[:quarter], lower, upper)

    def strip(b, src, dst, n, step):
        at = pl.ds(b * quarter, quarter)
        return pltpu.make_async_remote_copy(
            src_ref=src.at[at], dst_ref=dst.at[at],
            send_sem=pack_send.at[2 * b + n], recv_sem=pack_recv.at[2 * b + n],
            device_id={"gx": lax.rem(mx + step, nx)}, device_id_type=MESH,
        )

    to_east = [strip(b, last_v, west_v, 0, 1) for b in (0, 1)]
    to_west = [strip(b, first_v, east_v, 1, nx - 1) for b in (0, 1)]

    for b in (0, 1):
        finish(b)
        pl.when(jnp.logical_not(early))(to_east[b].start)

    depth_east_v[...] = jnp.where(
        lane == w - 1, 0.0, jnp.minimum(depth, pltpu.roll(depth, w - 1, 1))
    )
    depth_north_v[...] = jnp.where(
        row == h - 1, 0.0, jnp.minimum(depth, pltpu.roll(depth, h - 1, 0))
    )

    def interior(block, carry):
        start = pl.multiple_of(block * block_rows, block_rows)
        here = pl.ds(start, block_rows)
        deep_east, deep_north = depth_east_v[here, :], depth_north_v[here, :]
        deep, gain = depth_v[here, :], g_v[here, :]
        came = [0.0, 0.0]
        for k in range(nk):
            at = pl.ds(start + k * h, block_rows)
            east_near, east_far = face_weights(uv_v[at, :], deep_east > k)
            north_near, north_far = face_weights(
                uv_v[pl.ds(start + (nk + k) * h, block_rows), :], deep_north > k
            )
            mix = jnp.where(deep > k + 1, time_step * vertical_mixing, 0.0)
            for n, (ref, out) in enumerate(((t_v, t_out), (s_v, s_out))):
                c = ref[at, :]
                east = east_near * c + east_far * pltpu.roll(c, w - 1, 1)
                north = north_near * c + north_far * ref[pl.ds(start + k * h + 1, block_rows), :]
                strip_at = (n * nk + k) * (h + 8) + 8
                flux_v[pl.ds(start + strip_at, block_rows), :] = north
                south = flux_v[pl.ds(start + strip_at - 1, block_rows), :]
                flow = (pltpu.roll(east, 1, 1) - east) + (south - north)
                fall = 0.0
                if k < nk - 1:
                    fall = mix * (c - ref[pl.ds(start + (k + 1) * h, block_rows), :])
                out[at, :] = c + (gain * flow + (came[n] - fall))
                came[n] = fall
        return carry

    split = jnp.where(early, h // block_rows, 0)

    @pl.when(early)
    def _():
        for load in loads[8:]:
            load.wait()

    lax.fori_loop(0, split, interior, 0)
    pl.when(early)(meet)

    @pl.when(early)
    def _():
        for b in (0, 1):
            to_east[b].start()

    for b in (0, 1):
        to_west[b].start()
    @pl.when(jnp.logical_not(early))
    def _():
        for load in loads[8:]:
            load.wait()


    def rows(ref, row, base=0):
        return ref[pl.ds(base + row, nk, stride=h), :]

    up_v[pl.ds(0, nk), :] = rows(t_v, h - 1)
    up_v[pl.ds(nk, nk), :] = rows(s_v, h - 1)
    up_v[pl.ds(2 * nk, nk), :] = rows(uv_v, h - 1, nk * h)
    up_v[pl.ds(3 * nk, 8), :] = jnp.broadcast_to(depth[h - 1 : h, :], (8, w))
    down_v[pl.ds(0, nk), :] = rows(t_v, 0)
    down_v[pl.ds(nk, nk), :] = rows(s_v, 0)
    down_v[pl.ds(2 * nk, 8), :] = jnp.broadcast_to(depth[0:1, :], (8, w))

    @pl.when(is_top)
    def _():
        up = up_v[...]
        flip = (w - 1) - lax.broadcasted_iota(jnp.int32, up.shape, 1)
        fold_v[mx] = jnp.take_along_axis(up, flip, axis=1)

    to_north = pltpu.make_async_remote_copy(
        src_ref=up_v, dst_ref=south_v, send_sem=row_send.at[0], recv_sem=row_recv.at[0],
        device_id={"gy": lax.rem(my + 1, ny)}, device_id_type=MESH,
    )
    to_south = pltpu.make_async_remote_copy(
        src_ref=down_v, dst_ref=north_v, send_sem=row_send.at[1], recv_sem=row_recv.at[1],
        device_id={"gy": lax.rem(my + ny - 1, ny)}, device_id_type=MESH,
    )

    def fold_copy(d):
        return pltpu.make_async_remote_copy(
            src_ref=fold_v.at[mx], dst_ref=fold_v.at[mx],
            send_sem=fold_send.at[d], recv_sem=fold_recv.at[d],
            device_id={"gx": lax.rem(mx + d + 1, nx)}, device_id_type=MESH,
        )


    @pl.when(jnp.logical_not(is_top))
    def _():
        to_north.start()

    @pl.when(my > 0)
    def _():
        to_south.start()

    @pl.when(is_top)
    def _():
        repeat(nx - 1, lambda d: fold_copy(d).start())

    lax.fori_loop(split, h // block_rows, interior, 0)

    level_row = lax.broadcasted_iota(jnp.int32, (nk, w), 0).astype(jnp.float32)

    def north_edge(far_t, far_s, speed, far_depth):
        near_weight, far_weight = face_weights(
            speed, jnp.minimum(up_v[3 * nk : 3 * nk + 1, :], far_depth) > level_row
        )
        for near, far, out in (
            (up_v[pl.ds(0, nk), :], far_t, t_out),
            (up_v[pl.ds(nk, nk), :], far_s, s_out),
        ):
            at = pl.ds(h - 1, nk, stride=h)
            out[at, :] -= g_v[h - 1 : h, :] * (near_weight * near + far_weight * far)

    @pl.when(jnp.logical_not(is_top))
    def _():
        to_north.wait_send()
        to_south.wait_recv()
        north_edge(
            north_v[pl.ds(0, nk), :],
            north_v[pl.ds(nk, nk), :],
            up_v[pl.ds(2 * nk, nk), :],
            north_v[2 * nk : 2 * nk + 1, :],
        )

    @pl.when(my > 0)
    def _():
        to_south.wait_send()
        to_north.wait_recv()
        near_weight, far_weight = face_weights(
            south_v[pl.ds(2 * nk, nk), :],
            jnp.minimum(down_v[2 * nk : 2 * nk + 1, :], south_v[3 * nk : 3 * nk + 1, :]) > level_row,
        )
        for i, out in enumerate((t_out, s_out)):
            at = pl.ds(0, nk, stride=h)
            out[at, :] += g_v[0:1, :] * (
                near_weight * south_v[pl.ds(i * nk, nk), :]
                + far_weight * down_v[pl.ds(i * nk, nk), :]
            )

    @pl.when(is_hub)
    def _():
        several(parts_v, peers, part_send, part_recv).wait_recv()
        total_v[...] = jnp.sum(parts_v[...], axis=0)

    @pl.when(mx == hubs - 1)
    def _():
        repeat(nx - hubs, lambda d: hand_on(d).start())

    @pl.when(is_top)
    def _():
        repeat(nx - 1, lambda d: fold_copy(d).wait())
        partner = fold_v[seam_smem[0] // w]
        north_edge(
            partner[:nk],
            partner[nk : 2 * nk],
            0.5 * (up_v[pl.ds(2 * nk, nk), :] - partner[2 * nk : 3 * nk]),
            partner[3 * nk : 3 * nk + 1],
        )

    def column(plane, at):
        return jnp.broadcast_to(plane[:, at : at + 1], (h, w))

    mine = pack_v[...]
    depth = depth_v[...]
    gain = g_v[...]
    level_of = (pair & (nk - 1)).astype(jnp.float32)
    open_cell = jnp.where(eastern, column(depth, w - 1), column(depth, 0)) > level_of
    edge_gain = jnp.where(eastern, -column(gain, w - 1), column(gain, 0))
    surface_wet = jnp.where(depth > 0.0, time_step / top_thickness, 0.0)
    surface = s0_v[...]
    s_out[pl.ds(0, h), :] -= surface_wet * surface * rain_v[...]
    for i, plane in enumerate(
        (
            mine,
            jnp.where(pair < nk, pltpu.roll(mine, w - 4 * nk, 1), pltpu.roll(mine, w - 2 * nk, 1)),
            jnp.where(open_cell, edge_gain, 0.0),
            surface_wet * surface,
            surface_wet,
        )
    ):
        side_out[pl.ds(i * h, h), :] = plane

    @pl.when(is_hub)
    def _():
        several(parts_v, hubs * ny - 1, part_send, part_recv).wait_send()

    @pl.when(outside)
    def _():
        several(parts_v, hubs * ny, part_send, part_recv).wait_send()
        hand_on(0).wait_recv()

    @pl.when(mx == hubs - 1)
    def _():
        several(parts_v, nx - hubs, total_send, total_recv).wait_send()

    side_out[pl.ds(6 * h, 8), :] = jnp.broadcast_to(total_v[...], (8, w))
    for b in (0, 1):
        to_east[b].wait()
        to_west[b].wait()
    side_out[pl.ds(5 * h, half), :] = west_v[...]
    side_out[pl.ds(5 * h + half, half), :] = east_v[...]


store_cuts = 4


def store_kernel(nk, h, w, t_ref, s_ref, side_ref, t_hbm, s_hbm, t_v, s_v, sems):
    half = h // 2
    mine, own_speed, edge_gain, surface, surface_wet = (
        side_ref[pl.ds(i * h, h), :] for i in range(5)
    )
    west = side_ref[pl.ds(5 * h, half), :]
    east = side_ref[pl.ds(5 * h + half, half), :]
    totals = side_ref[pl.ds(6 * h, 1), :]

    lane = lax.broadcasted_iota(jnp.int32, (h, w), 1)
    slot = jnp.where(lax.broadcasted_iota(jnp.int32, (h, w), 0) < half, lane, lane - 1)
    pair = slot >> 1
    eastern = (slot & 1) == 0

    def both(cells):
        return jnp.concatenate([cells, cells], axis=0)

    def moved(cells, by):
        return both(pltpu.roll(cells, by % w, 1))

    def columns(cells, at):
        return jnp.concatenate(
            [jnp.broadcast_to(cells[:, i : i + 1], (half, w)) for i in (at, at + 1)], axis=0
        )

    near = jnp.where(eastern, mine, moved(west, 1))
    far = jnp.where(eastern, moved(east, -1), mine)
    west_speed = jnp.where(pair < nk, moved(west, 1 - 4 * nk), moved(west, 1 - 2 * nk))
    far_depth = jnp.where(eastern, columns(east, 6 * nk + 1), columns(west, 6 * nk))
    near_weight, far_weight = face_weights(
        jnp.where(eastern, own_speed, west_speed),
        far_depth > (pair & (nk - 1)).astype(jnp.float32),
    )
    edge = edge_gain * (near_weight * near + far_weight * far)

    total_area, total_fresh, salt_fresh, salt_only = (
        jnp.broadcast_to(totals[:, i : i + 1], (1, w)) for i in range(4)
    )
    mean_fresh = total_fresh / total_area
    lift = (salt_fresh - mean_fresh * salt_only) / total_area
    virtual = surface_wet * lift + surface * mean_fresh

    at_edge = (lane[:half] == 0) | (lane[:half] == w - 1)
    step = nk // store_cuts
    copies = []
    for i, (ref, out, hbm) in enumerate(((t_ref, t_v, t_hbm), (s_ref, s_v, s_hbm))):
        for cut in reversed(range(store_cuts)):
            for k in range(cut * step, (cut + 1) * step):
                j = i * nk + k
                for part, shift in ((0, w - 1 - 2 * j), (1, w - 2 - 2 * j)):
                    rows = slice(part * half, (part + 1) * half)
                    change = jnp.where(at_edge, pltpu.roll(edge[rows], shift % w, 1), 0.0)
                    if j == nk:
                        change = change + virtual[rows]
                    at = pl.ds(k * h + part * half, half)
                    out[at, :] = ref[at, :] + change
            at = pl.ds(cut * step * h, step * h)
            copy = pltpu.make_async_copy(out.at[at], hbm.at[at], sems.at[len(copies)])
            copy.start()
            copies.append(copy)
    for copy in copies:
        copy.wait()


def shards(nx, ny, t, s, uv, sea, layers, area, rain, seam):
    nk, h, w = t.shape
    assert w == 128 and h % 16 == 0 and nk & (nk - 1) == 0 and nk % 8 == 0 and 6 * nk + 3 <= w and nx > 3 and hubs == 2
    f32 = jnp.float32
    peers = nx * ny - 1
    half_plane = pltpu.VMEM((h // 2, w), f32)
    vmem = 67043328 - 4 * w * (2 * nk * h + 6 * h + 8)
    any_space = pl.BlockSpec(memory_space=pl.ANY)
    dma = pltpu.SemaphoreType.DMA
    plane = pltpu.VMEM((h, w), f32)
    t_next, s_next, side = pl.pallas_call(
        functools.partial(kernel, nx, ny, nk, h, w),
        out_shape=[pltpu.VMEM((nk * h, w), f32)] * 2 + [pltpu.VMEM((6 * h + 8, w), f32)],
        in_specs=[any_space] * 8,
        out_specs=[pl.BlockSpec(memory_space=pltpu.VMEM)] * 3,
        scratch_shapes=[
            pltpu.VMEM((nk * h + 8, w), f32),
            pltpu.VMEM((nk * h + 8, w), f32),
            pltpu.VMEM((2 * nk * h, w), f32),
            pltpu.VMEM((h, w), jnp.int32),
            pltpu.VMEM((h, w), jnp.int32),
            plane, plane, plane, plane, plane,
            plane, half_plane, half_plane, half_plane, half_plane,
            pltpu.VMEM((3 * nk + 8, w), f32),
            pltpu.VMEM((2 * nk + 8, w), f32),
            pltpu.VMEM((3 * nk + 8, w), f32),
            pltpu.VMEM((2 * nk + 8, w), f32),
            pltpu.VMEM((nx, 3 * nk + 8, w), f32),
            pltpu.VMEM((1, w), f32),
            pltpu.VMEM((nx * ny, 1, w), f32),
            pltpu.VMEM((1, w), f32),
            pltpu.SMEM((w,), jnp.int32),
            plane, plane,
            pltpu.VMEM((2 * nk * (h + 8), w), f32),
            dma((10,)), dma((4,)), dma((4,)), dma((2,)), dma((2,)),
            dma((nx - 1,)), dma((nx - 1,)), dma, dma, dma, dma,
        ],
        compiler_params=pltpu.CompilerParams(
            collective_id=0, has_side_effects=True, vmem_limit_bytes=vmem
        ),
        name="tracer_step",
    )(
        t.reshape(nk * h, w), s.reshape(nk * h, w), uv.reshape(2 * nk * h, w),
        sea, layers, area, rain, seam,
    )
    t_next, s_next = pl.pallas_call(
        functools.partial(store_kernel, nk, h, w),
        out_shape=[jax.ShapeDtypeStruct((nk * h, w), f32)] * 2,
        in_specs=[pl.BlockSpec(memory_space=pltpu.VMEM)] * 3,
        out_specs=[any_space] * 2,
        scratch_shapes=[pltpu.VMEM((nk * h, w), f32)] * 2 + [dma((2 * store_cuts,))],
        compiler_params=pltpu.CompilerParams(vmem_limit_bytes=8 << 20),
        name="store",
    )(t_next, s_next, side)
    return t_next.reshape(t.shape), s_next.reshape(s.shape)


def solution(mesh):
    in_specs = (
        P("groups", "gy", "gx"),
        P("groups", "gy", "gx"),
        P("groups", None, "gy", "gx"),
        P("gy", "gx"),
        P("gy", "gx"),
        P("gy", "gx"),
        P("gy", "gx"),
        P("gx"),
    )
    out_specs = (P("groups", "gy", "gx"), P("groups", "gy", "gx"))
    return jax.shard_map(
        functools.partial(shards, mesh.shape["gx"], mesh.shape["gy"]),
        mesh=mesh, in_specs=in_specs, out_specs=out_specs, check_vma=False,
    )
```

```python
import functools

import jax
import jax.numpy as jnp
from jax import lax
from jax.experimental import pallas as pl
from jax.experimental.pallas import tpu as pltpu
from jax.sharding import PartitionSpec as P

time_step = 0.25
diffusivity = 0.5
vertical_mixing = 0.3
top_thickness = 0.5

block_rows = 16
hub_column = 1

MESH = pl.DeviceIdType.MESH


def repeat(count, body):
    if count <= 16:
        for i in range(count):
            body(i)
    else:
        pl.loop(0, count)(body)


def face_weights(speed, open_face):
    near_weight = jnp.maximum(speed, 0.0) + diffusivity
    far_weight = speed - near_weight
    return jnp.where(open_face, near_weight, 0.0), jnp.where(open_face, far_weight, 0.0)


def kernel(
    nx, ny, nk, h, w,
    t_hbm, s_hbm, uv_hbm, sea_hbm, lay_hbm, area_hbm, rain_hbm, seam_hbm,
    t_out, s_out, side_out,
    t_v, s_v, uv_v, sea_v, lay_v, area_v, rain_v, s0_v, g_v, depth_v,
    pack_v, last_v, first_v, east_v, west_v, up_v, down_v, south_v, north_v, fold_v,
    part_v, parts_v, total_v, seam_smem, depth_east_v, depth_north_v, flux_v,
    load_sems, pack_send, pack_recv, row_send, row_recv, fold_send, fold_recv,
    part_send, part_recv, total_send, total_recv, ready,
):
    mx, my = lax.axis_index("gx"), lax.axis_index("gy")
    is_top = my == ny - 1
    peers = nx * ny - 1

    barrier = pltpu.get_barrier_semaphore()

    east, west = lax.rem(mx + 1, nx), lax.rem(mx + nx - 1, nx)
    near = ny // 2
    hubs = near + ny

    def hub(gx, gy):
        return (gx == hub_column) | ((gx == 0) & (gy < near))

    is_hub = hub(mx, my)
    plain = jnp.logical_not(is_hub)
    seam_west = mx == 0
    seam_east = mx == nx - 1
    has_north, has_south = my < ny - 1, my > 0

    def count(flag):
        return jnp.where(flag, 1, 0)

    row_partners = jnp.where(
        is_top,
        nx - 1 - count(mx != hub_column),
        count(jnp.logical_not(hub(east, my)))
        + count(jnp.logical_not(hub(west, my) | seam_west)),
    )
    partners = (
        hubs - count(is_hub) + row_partners
        + count(has_north & jnp.logical_not(hub(mx, my + 1)))
        + count(has_south & jnp.logical_not(hub(mx, my - 1)))
    )

    def signal(gx, gy):
        pl.semaphore_signal(
            barrier, inc=1, device_id={"gx": gx, "gy": gy}, device_id_type=MESH
        )

    def greet():
        @pl.when(is_hub)
        def _():
            def one(r):
                r = r + 1
                signal(lax.rem(mx + r // ny, nx), lax.rem(my + r % ny, ny))

            repeat(peers, one)

        @pl.when(plain & is_top)
        def _():
            repeat(nx - 1, lambda d: signal(lax.rem(mx + 1 + d, nx), my))

        @pl.when(plain & has_north)
        def _():
            signal(west, my)
            pl.when(jnp.logical_not(seam_east))(lambda: signal(east, my))
            signal(mx, my + 1)

        @pl.when(plain & has_south)
        def _():
            signal(mx, my - 1)

    loads = [
        pltpu.make_async_copy(src, dst, load_sems.at[i])
        for i, (src, dst) in enumerate(
            [
                (area_hbm, area_v),
                (sea_hbm, sea_v),
                (rain_hbm, rain_v),
                (s_hbm.at[pl.ds(0, h)], s0_v),
                (lay_hbm, lay_v),
                (t_hbm, t_v.at[pl.ds(0, nk * h)]),
                (s_hbm, s_v.at[pl.ds(0, nk * h)]),
                (uv_hbm.at[pl.ds(0, nk * h)], uv_v.at[pl.ds(0, nk * h)]),
                (uv_hbm.at[pl.ds(nk * h, nk * h)], uv_v.at[pl.ds(nk * h, nk * h)]),
                (seam_hbm, seam_smem),
            ]
        )
    ]
    for load in loads[:8]:
        load.start()
    greet()
    for load in loads[8:]:
        load.start()
    zeros = jnp.zeros((8, w), jnp.float32)
    for ref in (t_v, s_v):
        ref[pl.ds(nk * h, 8), :] = zeros
    for i in range(2 * nk):
        flux_v[pl.ds(i * (h + 8), 8), :] = zeros

    for load in loads[:4]:
        load.wait()
    area = area_v[...]
    sea = sea_v[...]
    wet_area = area * sea.astype(jnp.float32)
    surface = s0_v[...]
    fresh = wet_area * rain_v[...]
    lane1 = lax.broadcasted_iota(jnp.int32, (1, w), 1)
    part = jnp.zeros((1, w), jnp.float32)
    for i, term in enumerate((wet_area, fresh, fresh * surface, wet_area * surface)):
        rows8 = jnp.sum(term.reshape(h // 8, 8, w), axis=0)
        part = jnp.where(
            lane1 == i, jnp.sum(jnp.sum(rows8, axis=1, keepdims=True), axis=0, keepdims=True), part
        )
    part_v[...] = part
    gain = time_step / area
    g_v[...] = gain

    me = mx * ny + my
    parts_v[me] = part

    def send_part(gx, gy):
        @pl.when(gx * ny + gy != me)
        def _():
            pltpu.make_async_remote_copy(
                src_ref=part_v, dst_ref=parts_v.at[me], send_sem=part_send, recv_sem=part_recv,
                device_id={"gx": gx, "gy": gy}, device_id_type=MESH,
            ).start()

    def several(ref, n, sends, arrivals):
        block = ref.at[pl.ds(0, n)]
        return pltpu.make_async_remote_copy(
            src_ref=block, dst_ref=block, send_sem=sends, recv_sem=arrivals,
            device_id={"gx": east}, device_id_type=MESH,
        )

    def hand_on(gx, gy):
        return pltpu.make_async_remote_copy(
            src_ref=total_v, dst_ref=total_v, send_sem=total_send, recv_sem=total_recv,
            device_id={"gx": gx, "gy": gy}, device_id_type=MESH,
        )

    def meet():
        pl.semaphore_wait(barrier, partners)
        repeat(near, lambda gy: send_part(0, gy))
        repeat(ny, lambda gy: send_part(hub_column, gy))
        pl.when(seam_east)(
            lambda: pl.semaphore_signal(ready, inc=1, device_id={"gx": east}, device_id_type=MESH)
        )

    early = seam_west & (my < near)
    pack_first = (mx > 0) & (my < near)
    pl.when(my >= near)(meet)

    loads[4].wait()
    depth = (sea * lay_v[...]).astype(jnp.float32)
    depth_v[...] = depth

    half = h // 2
    depth_at = 6 * nk
    lane = lax.broadcasted_iota(jnp.int32, (h, w), 1)
    row = lax.broadcasted_iota(jnp.int32, (h, w), 0)
    slot = jnp.where(row < half, lane, lane - 1)
    pair = slot >> 1
    eastern = (slot & 1) == 0
    even_half = (lane[:half] & 1) == 0

    quarter = h // 4

    def cells(ref, k, b):
        return [
            ref[pl.ds(k * h + side * half + b * quarter, quarter), :] for side in (0, 1)
        ]

    def pack(packed, b, ref, first, count):
        for k in range(count):
            j = first + k
            packed = [
                jnp.where(
                    pair[side * half : side * half + quarter] == j,
                    pltpu.roll(plane, 2 * j + 1 + side, 1),
                    old,
                )
                for side, (plane, old) in enumerate(zip(cells(ref, k, b), packed))
            ]
        return packed

    empty = [jnp.zeros((quarter, w), jnp.float32)] * 2
    packed = [pack(empty, b, depth_v, 3 * nk, 1) for b in (0, 1)]
    for i, ref in enumerate((t_v, s_v)):
        loads[5 + i].wait()
        packed = [pack(packed[b], b, ref, i * nk, nk) for b in (0, 1)]
    loads[7].wait()

    def finish(b):
        upper, lower = pack(packed[b], b, uv_v, 2 * nk, nk)
        pack_v[pl.ds(b * quarter, quarter), :] = upper
        pack_v[pl.ds(half + b * quarter, quarter), :] = lower
        at = pl.ds(b * quarter, quarter)
        last_v[at, :] = jnp.where(even_half[:quarter], upper, lower)
        first_v[at, :] = jnp.where(even_half[:quarter], lower, upper)

    def strip(b, src, dst, n, step):
        at = pl.ds(b * quarter, quarter)
        return pltpu.make_async_remote_copy(
            src_ref=src.at[at], dst_ref=dst.at[at],
            send_sem=pack_send.at[2 * b + n], recv_sem=pack_recv.at[2 * b + n],
            device_id={"gx": lax.rem(mx + step, nx)}, device_id_type=MESH,
        )

    to_east = [strip(b, last_v, west_v, 0, 1) for b in (0, 1)]
    to_west = [strip(b, first_v, east_v, 1, nx - 1) for b in (0, 1)]

    for b in (0, 1):
        finish(b)
    pl.when(pack_first)(meet)

    @pl.when(jnp.logical_not(early))
    def _():
        for b in (0, 1):
            to_east[b].start()

    depth_east_v[...] = jnp.where(
        lane == w - 1, 0.0, jnp.minimum(depth, pltpu.roll(depth, w - 1, 1))
    )
    depth_north_v[...] = jnp.where(
        row == h - 1, 0.0, jnp.minimum(depth, pltpu.roll(depth, h - 1, 0))
    )

    def interior(block, carry):
        start = pl.multiple_of(block * block_rows, block_rows)
        here = pl.ds(start, block_rows)
        deep_east, deep_north = depth_east_v[here, :], depth_north_v[here, :]
        deep, gain = depth_v[here, :], g_v[here, :]
        came = [0.0, 0.0]
        for k in range(nk):
            at = pl.ds(start + k * h, block_rows)
            east_near, east_far = face_weights(uv_v[at, :], deep_east > k)
            north_near, north_far = face_weights(
                uv_v[pl.ds(start + (nk + k) * h, block_rows), :], deep_north > k
            )
            mix = jnp.where(deep > k + 1, time_step * vertical_mixing, 0.0)
            for n, (ref, out) in enumerate(((t_v, t_out), (s_v, s_out))):
                c = ref[at, :]
                east = east_near * c + east_far * pltpu.roll(c, w - 1, 1)
                north = north_near * c + north_far * ref[pl.ds(start + k * h + 1, block_rows), :]
                strip_at = (n * nk + k) * (h + 8) + 8
                flux_v[pl.ds(start + strip_at, block_rows), :] = north
                south = flux_v[pl.ds(start + strip_at - 1, block_rows), :]
                flow = (pltpu.roll(east, 1, 1) - east) + (south - north)
                fall = 0.0
                if k < nk - 1:
                    fall = mix * (c - ref[pl.ds(start + (k + 1) * h, block_rows), :])
                out[at, :] = c + (gain * flow + (came[n] - fall))
                came[n] = fall
        return carry

    split = jnp.where(early, h // block_rows, 0)

    @pl.when(early)
    def _():
        for load in loads[8:]:
            load.wait()

    lax.fori_loop(0, split, interior, 0)
    pl.when(early)(meet)

    @pl.when(early)
    def _():
        for b in (0, 1):
            to_east[b].start()

    @pl.when(jnp.logical_not(seam_west))
    def _():
        for b in (0, 1):
            to_west[b].start()

    @pl.when(jnp.logical_not(early))
    def _():
        for load in loads[8:]:
            load.wait()


    def rows(ref, row, base=0):
        return ref[pl.ds(base + row, nk, stride=h), :]

    up_v[pl.ds(0, nk), :] = rows(t_v, h - 1)
    up_v[pl.ds(nk, nk), :] = rows(s_v, h - 1)
    up_v[pl.ds(2 * nk, nk), :] = rows(uv_v, h - 1, nk * h)
    up_v[pl.ds(3 * nk, 8), :] = jnp.broadcast_to(depth[h - 1 : h, :], (8, w))
    down_v[pl.ds(0, nk), :] = rows(t_v, 0)
    down_v[pl.ds(nk, nk), :] = rows(s_v, 0)
    down_v[pl.ds(2 * nk, 8), :] = jnp.broadcast_to(depth[0:1, :], (8, w))

    @pl.when(is_top)
    def _():
        up = up_v[...]
        flip = (w - 1) - lax.broadcasted_iota(jnp.int32, up.shape, 1)
        fold_v[mx] = jnp.take_along_axis(up, flip, axis=1)

    to_north = pltpu.make_async_remote_copy(
        src_ref=up_v, dst_ref=south_v, send_sem=row_send.at[0], recv_sem=row_recv.at[0],
        device_id={"gy": lax.rem(my + 1, ny)}, device_id_type=MESH,
    )
    to_south = pltpu.make_async_remote_copy(
        src_ref=down_v, dst_ref=north_v, send_sem=row_send.at[1], recv_sem=row_recv.at[1],
        device_id={"gy": lax.rem(my + ny - 1, ny)}, device_id_type=MESH,
    )

    def fold_copy(d):
        return pltpu.make_async_remote_copy(
            src_ref=fold_v.at[mx], dst_ref=fold_v.at[mx],
            send_sem=fold_send.at[d], recv_sem=fold_recv.at[d],
            device_id={"gx": lax.rem(mx + d + 1, nx)}, device_id_type=MESH,
        )


    @pl.when(jnp.logical_not(is_top))
    def _():
        to_north.start()

    @pl.when(my > 0)
    def _():
        to_south.start()

    @pl.when(is_top)
    def _():
        repeat(nx - 1, lambda d: fold_copy(d).start())

    lax.fori_loop(split, h // block_rows, interior, 0)

    level_row = lax.broadcasted_iota(jnp.int32, (nk, w), 0).astype(jnp.float32)

    def north_edge(far_t, far_s, speed, far_depth):
        near_weight, far_weight = face_weights(
            speed, jnp.minimum(up_v[3 * nk : 3 * nk + 1, :], far_depth) > level_row
        )
        for near, far, out in (
            (up_v[pl.ds(0, nk), :], far_t, t_out),
            (up_v[pl.ds(nk, nk), :], far_s, s_out),
        ):
            at = pl.ds(h - 1, nk, stride=h)
            out[at, :] -= g_v[h - 1 : h, :] * (near_weight * near + far_weight * far)

    @pl.when(seam_west)
    def _():
        pl.semaphore_wait(ready, 1)
        for b in (0, 1):
            to_west[b].start()

    @pl.when(jnp.logical_not(is_top))
    def _():
        to_north.wait_send()
        to_south.wait_recv()
        north_edge(
            north_v[pl.ds(0, nk), :],
            north_v[pl.ds(nk, nk), :],
            up_v[pl.ds(2 * nk, nk), :],
            north_v[2 * nk : 2 * nk + 1, :],
        )

    @pl.when(my > 0)
    def _():
        to_south.wait_send()
        to_north.wait_recv()
        near_weight, far_weight = face_weights(
            south_v[pl.ds(2 * nk, nk), :],
            jnp.minimum(down_v[2 * nk : 2 * nk + 1, :], south_v[3 * nk : 3 * nk + 1, :]) > level_row,
        )
        for i, out in enumerate((t_out, s_out)):
            at = pl.ds(0, nk, stride=h)
            out[at, :] += g_v[0:1, :] * (
                near_weight * south_v[pl.ds(i * nk, nk), :]
                + far_weight * down_v[pl.ds(i * nk, nk), :]
            )

    @pl.when(is_hub)
    def _():
        several(parts_v, peers, part_send, part_recv).wait_recv()
        total_v[...] = jnp.sum(parts_v[...], axis=0)

    in_column = mx == hub_column
    seam_giver = seam_west & (my == near - 1)

    @pl.when(in_column)
    def _():
        repeat(nx - 2, lambda d: hand_on(hub_column + 1 + d, my).start())

    @pl.when(seam_giver)
    def _():
        repeat(ny - near, lambda d: hand_on(0, near + d).start())

    @pl.when(is_top)
    def _():
        repeat(nx - 1, lambda d: fold_copy(d).wait())
        partner = fold_v[seam_smem[0] // w]
        north_edge(
            partner[:nk],
            partner[nk : 2 * nk],
            0.5 * (up_v[pl.ds(2 * nk, nk), :] - partner[2 * nk : 3 * nk]),
            partner[3 * nk : 3 * nk + 1],
        )

    def column(plane, at):
        return jnp.broadcast_to(plane[:, at : at + 1], (h, w))

    mine = pack_v[...]
    depth = depth_v[...]
    gain = g_v[...]
    level_of = (pair & (nk - 1)).astype(jnp.float32)
    open_cell = jnp.where(eastern, column(depth, w - 1), column(depth, 0)) > level_of
    edge_gain = jnp.where(eastern, -column(gain, w - 1), column(gain, 0))
    surface_wet = jnp.where(depth > 0.0, time_step / top_thickness, 0.0)
    surface = s0_v[...]
    s_out[pl.ds(0, h), :] -= surface_wet * surface * rain_v[...]
    for i, plane in enumerate(
        (
            mine,
            jnp.where(pair < nk, pltpu.roll(mine, w - 4 * nk, 1), pltpu.roll(mine, w - 2 * nk, 1)),
            jnp.where(open_cell, edge_gain, 0.0),
            surface_wet * surface,
            surface_wet,
        )
    ):
        side_out[pl.ds(i * h, h), :] = plane

    @pl.when(is_hub)
    def _():
        several(parts_v, hubs - 1, part_send, part_recv).wait_send()

    @pl.when(plain)
    def _():
        several(parts_v, hubs, part_send, part_recv).wait_send()
        hand_on(0, 0).wait_recv()

    @pl.when(in_column)
    def _():
        several(parts_v, nx - 2, total_send, total_recv).wait_send()

    @pl.when(seam_giver)
    def _():
        several(parts_v, ny - near, total_send, total_recv).wait_send()

    side_out[pl.ds(6 * h, 8), :] = jnp.broadcast_to(total_v[...], (8, w))
    for b in (0, 1):
        to_east[b].wait()
        to_west[b].wait()
    side_out[pl.ds(5 * h, half), :] = west_v[...]
    side_out[pl.ds(5 * h + half, half), :] = east_v[...]


store_cuts = 4


def store_kernel(nk, h, w, t_ref, s_ref, side_ref, t_hbm, s_hbm, t_v, s_v, sems):
    half = h // 2
    mine, own_speed, edge_gain, surface, surface_wet = (
        side_ref[pl.ds(i * h, h), :] for i in range(5)
    )
    west = side_ref[pl.ds(5 * h, half), :]
    east = side_ref[pl.ds(5 * h + half, half), :]
    totals = side_ref[pl.ds(6 * h, 1), :]

    lane = lax.broadcasted_iota(jnp.int32, (h, w), 1)
    slot = jnp.where(lax.broadcasted_iota(jnp.int32, (h, w), 0) < half, lane, lane - 1)
    pair = slot >> 1
    eastern = (slot & 1) == 0

    def both(cells):
        return jnp.concatenate([cells, cells], axis=0)

    def moved(cells, by):
        return both(pltpu.roll(cells, by % w, 1))

    def columns(cells, at):
        return jnp.concatenate(
            [jnp.broadcast_to(cells[:, i : i + 1], (half, w)) for i in (at, at + 1)], axis=0
        )

    near = jnp.where(eastern, mine, moved(west, 1))
    far = jnp.where(eastern, moved(east, -1), mine)
    west_speed = jnp.where(pair < nk, moved(west, 1 - 4 * nk), moved(west, 1 - 2 * nk))
    far_depth = jnp.where(eastern, columns(east, 6 * nk + 1), columns(west, 6 * nk))
    near_weight, far_weight = face_weights(
        jnp.where(eastern, own_speed, west_speed),
        far_depth > (pair & (nk - 1)).astype(jnp.float32),
    )
    edge = edge_gain * (near_weight * near + far_weight * far)

    total_area, total_fresh, salt_fresh, salt_only = (
        jnp.broadcast_to(totals[:, i : i + 1], (1, w)) for i in range(4)
    )
    mean_fresh = total_fresh / total_area
    lift = (salt_fresh - mean_fresh * salt_only) / total_area
    virtual = surface_wet * lift + surface * mean_fresh

    at_edge = (lane[:half] == 0) | (lane[:half] == w - 1)
    step = nk // store_cuts
    copies = []
    for i, (ref, out, hbm) in enumerate(((t_ref, t_v, t_hbm), (s_ref, s_v, s_hbm))):
        for cut in reversed(range(store_cuts)):
            for k in range(cut * step, (cut + 1) * step):
                j = i * nk + k
                for part, shift in ((0, w - 1 - 2 * j), (1, w - 2 - 2 * j)):
                    rows = slice(part * half, (part + 1) * half)
                    change = jnp.where(at_edge, pltpu.roll(edge[rows], shift % w, 1), 0.0)
                    if j == nk:
                        change = change + virtual[rows]
                    at = pl.ds(k * h + part * half, half)
                    out[at, :] = ref[at, :] + change
            at = pl.ds(cut * step * h, step * h)
            copy = pltpu.make_async_copy(out.at[at], hbm.at[at], sems.at[len(copies)])
            copy.start()
            copies.append(copy)
    for copy in copies:
        copy.wait()


def shards(nx, ny, t, s, uv, sea, layers, area, rain, seam):
    nk, h, w = t.shape
    assert w == 128 and h % 16 == 0 and nk & (nk - 1) == 0 and nk % 8 == 0 and 6 * nk + 3 <= w and nx > 3
    f32 = jnp.float32
    peers = nx * ny - 1
    half_plane = pltpu.VMEM((h // 2, w), f32)
    vmem = 67043328 - 4 * w * (2 * nk * h + 6 * h + 8)
    any_space = pl.BlockSpec(memory_space=pl.ANY)
    dma = pltpu.SemaphoreType.DMA
    plane = pltpu.VMEM((h, w), f32)
    t_next, s_next, side = pl.pallas_call(
        functools.partial(kernel, nx, ny, nk, h, w),
        out_shape=[pltpu.VMEM((nk * h, w), f32)] * 2 + [pltpu.VMEM((6 * h + 8, w), f32)],
        in_specs=[any_space] * 8,
        out_specs=[pl.BlockSpec(memory_space=pltpu.VMEM)] * 3,
        scratch_shapes=[
            pltpu.VMEM((nk * h + 8, w), f32),
            pltpu.VMEM((nk * h + 8, w), f32),
            pltpu.VMEM((2 * nk * h, w), f32),
            pltpu.VMEM((h, w), jnp.int32),
            pltpu.VMEM((h, w), jnp.int32),
            plane, plane, plane, plane, plane,
            plane, half_plane, half_plane, half_plane, half_plane,
            pltpu.VMEM((3 * nk + 8, w), f32),
            pltpu.VMEM((2 * nk + 8, w), f32),
            pltpu.VMEM((3 * nk + 8, w), f32),
            pltpu.VMEM((2 * nk + 8, w), f32),
            pltpu.VMEM((nx, 3 * nk + 8, w), f32),
            pltpu.VMEM((1, w), f32),
            pltpu.VMEM((nx * ny, 1, w), f32),
            pltpu.VMEM((1, w), f32),
            pltpu.SMEM((w,), jnp.int32),
            plane, plane,
            pltpu.VMEM((2 * nk * (h + 8), w), f32),
            dma((10,)), dma((4,)), dma((4,)), dma((2,)), dma((2,)),
            dma((nx - 1,)), dma((nx - 1,)), dma, dma, dma, dma, pltpu.SemaphoreType.REGULAR,
        ],
        compiler_params=pltpu.CompilerParams(
            collective_id=0, has_side_effects=True, vmem_limit_bytes=vmem
        ),
        name="tracer_step",
    )(
        t.reshape(nk * h, w), s.reshape(nk * h, w), uv.reshape(2 * nk * h, w),
        sea, layers, area, rain, seam,
    )
    t_next, s_next = pl.pallas_call(
        functools.partial(store_kernel, nk, h, w),
        out_shape=[jax.ShapeDtypeStruct((nk * h, w), f32)] * 2,
        in_specs=[pl.BlockSpec(memory_space=pltpu.VMEM)] * 3,
        out_specs=[any_space] * 2,
        scratch_shapes=[pltpu.VMEM((nk * h, w), f32)] * 2 + [dma((2 * store_cuts,))],
        compiler_params=pltpu.CompilerParams(vmem_limit_bytes=8 << 20),
        name="store",
    )(t_next, s_next, side)
    return t_next.reshape(t.shape), s_next.reshape(s.shape)


def solution(mesh):
    in_specs = (
        P("groups", "gy", "gx"),
        P("groups", "gy", "gx"),
        P("groups", None, "gy", "gx"),
        P("gy", "gx"),
        P("gy", "gx"),
        P("gy", "gx"),
        P("gy", "gx"),
        P("gx"),
    )
    out_specs = (P("groups", "gy", "gx"), P("groups", "gy", "gx"))
    return jax.shard_map(
        functools.partial(shards, mesh.shape["gx"], mesh.shape["gy"]),
        mesh=mesh, in_specs=in_specs, out_specs=out_specs, check_vma=False,
    )
```

```python
import functools

import jax
import jax.numpy as jnp
from jax import lax
from jax.experimental import pallas as pl
from jax.experimental.pallas import tpu as pltpu
from jax.sharding import PartitionSpec as P

time_step = 0.25
diffusivity = 0.5
vertical_mixing = 0.3
top_thickness = 0.5

block_rows = 16
hub_column = 1

MESH = pl.DeviceIdType.MESH


def repeat(count, body):
    if count <= 16:
        for i in range(count):
            body(i)
    else:
        pl.loop(0, count)(body)


def face_weights(speed, open_face):
    near_weight = jnp.maximum(speed, 0.0) + diffusivity
    far_weight = speed - near_weight
    return jnp.where(open_face, near_weight, 0.0), jnp.where(open_face, far_weight, 0.0)


def kernel(
    nx, ny, nk, h, w,
    t_hbm, s_hbm, uv_hbm, sea_hbm, lay_hbm, area_hbm, rain_hbm, seam_hbm,
    t_out, s_out, side_out,
    t_v, s_v, uv_v, sea_v, lay_v, area_v, rain_v, s0_v, g_v, depth_v,
    pack_v, last_v, first_v, east_v, west_v, up_v, down_v, south_v, north_v, fold_v,
    part_v, parts_v, total_v, seam_smem, depth_east_v, depth_north_v, flux_v,
    load_sems, pack_send, pack_recv, row_send, row_recv, fold_send, fold_recv,
    part_send, part_recv, total_send, total_recv, ready,
):
    mx, my = lax.axis_index("gx"), lax.axis_index("gy")
    is_top = my == ny - 1
    peers = nx * ny - 1

    barrier = pltpu.get_barrier_semaphore()

    east, west = lax.rem(mx + 1, nx), lax.rem(mx + nx - 1, nx)
    near = ny // 2
    hubs = near + 1 + ny

    def hub(gx, gy):
        return (gx == hub_column) | ((gx == 0) & ((gy < near) | (gy == ny - 1)))

    is_hub = hub(mx, my)
    plain = jnp.logical_not(is_hub)
    seam_west = mx == 0
    seam_east = mx == nx - 1
    has_north, has_south = my < ny - 1, my > 0

    def count(flag):
        return jnp.where(flag, 1, 0)

    row_partners = jnp.where(
        is_top,
        nx - 2 - count(mx > hub_column),
        count(jnp.logical_not(hub(east, my)))
        + count(jnp.logical_not(hub(west, my) | seam_west)),
    )
    partners = (
        hubs - count(is_hub) + row_partners
        + count(has_north & jnp.logical_not(hub(mx, my + 1)))
        + count(has_south & jnp.logical_not(hub(mx, my - 1)))
    )

    def signal(gx, gy):
        pl.semaphore_signal(
            barrier, inc=1, device_id={"gx": gx, "gy": gy}, device_id_type=MESH
        )

    def greet():
        @pl.when(is_hub)
        def _():
            def one(r):
                r = r + 1
                signal(lax.rem(mx + r // ny, nx), lax.rem(my + r % ny, ny))

            repeat(peers, one)

        @pl.when(plain & is_top)
        def _():
            repeat(nx - 1, lambda d: signal(lax.rem(mx + 1 + d, nx), my))

        @pl.when(plain & has_north)
        def _():
            signal(west, my)
            pl.when(jnp.logical_not(seam_east))(lambda: signal(east, my))
            signal(mx, my + 1)

        @pl.when(plain & has_south)
        def _():
            signal(mx, my - 1)

    loads = [
        pltpu.make_async_copy(src, dst, load_sems.at[max(i - 4, 0)])
        for i, (src, dst) in enumerate(
            [
                (area_hbm, area_v),
                (sea_hbm, sea_v),
                (rain_hbm, rain_v),
                (s_hbm.at[pl.ds(0, h)], s0_v),
                (lay_hbm, lay_v),
                (t_hbm, t_v.at[pl.ds(0, nk * h)]),
                (s_hbm, s_v.at[pl.ds(0, nk * h)]),
                (uv_hbm.at[pl.ds(0, nk * h)], uv_v.at[pl.ds(0, nk * h)]),
                (uv_hbm.at[pl.ds(nk * h, nk * h)], uv_v.at[pl.ds(nk * h, nk * h)]),
                (seam_hbm, seam_smem),
            ]
        )
    ]
    for load in loads[:8]:
        load.start()
    greet()
    for load in loads[8:]:
        load.start()
    zeros = jnp.zeros((8, w), jnp.float32)
    for ref in (t_v, s_v):
        ref[pl.ds(nk * h, 8), :] = zeros
    for i in range(2 * nk):
        flux_v[pl.ds(i * (h + 8), 8), :] = zeros

    small = pl.ds(0, 5 * h)
    pltpu.make_async_copy(t_hbm.at[small], t_v.at[small], load_sems.at[0]).wait()
    area = area_v[...]
    sea = sea_v[...]
    wet_area = area * sea.astype(jnp.float32)
    surface = s0_v[...]
    fresh = wet_area * rain_v[...]
    lane1 = lax.broadcasted_iota(jnp.int32, (1, w), 1)
    part = jnp.zeros((1, w), jnp.float32)
    for i, term in enumerate((wet_area, fresh, fresh * surface, wet_area * surface)):
        rows8 = jnp.sum(term.reshape(h // 8, 8, w), axis=0)
        part = jnp.where(
            lane1 == i, jnp.sum(jnp.sum(rows8, axis=1, keepdims=True), axis=0, keepdims=True), part
        )
    part_v[...] = part
    gain = time_step / area
    g_v[...] = gain

    me = mx * ny + my
    parts_v[me] = part

    def send_part(gx, gy):
        @pl.when(gx * ny + gy != me)
        def _():
            pltpu.make_async_remote_copy(
                src_ref=part_v, dst_ref=parts_v.at[me], send_sem=part_send, recv_sem=part_recv,
                device_id={"gx": gx, "gy": gy}, device_id_type=MESH,
            ).start()

    def several(ref, n, sends, arrivals):
        block = ref.at[pl.ds(0, n)]
        return pltpu.make_async_remote_copy(
            src_ref=block, dst_ref=block, send_sem=sends, recv_sem=arrivals,
            device_id={"gx": east}, device_id_type=MESH,
        )

    def hand_on(gx, gy):
        return pltpu.make_async_remote_copy(
            src_ref=total_v, dst_ref=total_v, send_sem=total_send, recv_sem=total_recv,
            device_id={"gx": gx, "gy": gy}, device_id_type=MESH,
        )

    def meet():
        pl.semaphore_wait(barrier, partners)
        repeat(near, lambda gy: send_part(0, gy))
        send_part(0, ny - 1)
        repeat(ny, lambda gy: send_part(hub_column, gy))
        pl.when(seam_east)(
            lambda: pl.semaphore_signal(ready, inc=1, device_id={"gx": east}, device_id_type=MESH)
        )

    early = seam_west & (my < near)
    pack_first = (mx > 0) & (my < near)
    pl.when(my >= near)(meet)

    depth = (sea * lay_v[...]).astype(jnp.float32)
    depth_v[...] = depth

    half = h // 2
    depth_at = 6 * nk
    lane = lax.broadcasted_iota(jnp.int32, (h, w), 1)
    row = lax.broadcasted_iota(jnp.int32, (h, w), 0)
    slot = jnp.where(row < half, lane, lane - 1)
    pair = slot >> 1
    eastern = (slot & 1) == 0
    even_half = (lane[:half] & 1) == 0

    quarter = h // 4

    def cells(ref, k, b):
        return [
            ref[pl.ds(k * h + side * half + b * quarter, quarter), :] for side in (0, 1)
        ]

    def pack(packed, b, ref, first, count):
        for k in range(count):
            j = first + k
            packed = [
                jnp.where(
                    pair[side * half : side * half + quarter] == j,
                    pltpu.roll(plane, 2 * j + 1 + side, 1),
                    old,
                )
                for side, (plane, old) in enumerate(zip(cells(ref, k, b), packed))
            ]
        return packed

    empty = [jnp.zeros((quarter, w), jnp.float32)] * 2
    packed = [pack(empty, b, depth_v, 3 * nk, 1) for b in (0, 1)]
    for i, ref in enumerate((t_v, s_v)):
        loads[5 + i].wait()
        packed = [pack(packed[b], b, ref, i * nk, nk) for b in (0, 1)]
    loads[7].wait()

    def finish(b):
        upper, lower = pack(packed[b], b, uv_v, 2 * nk, nk)
        pack_v[pl.ds(b * quarter, quarter), :] = upper
        pack_v[pl.ds(half + b * quarter, quarter), :] = lower
        at = pl.ds(b * quarter, quarter)
        last_v[at, :] = jnp.where(even_half[:quarter], upper, lower)
        first_v[at, :] = jnp.where(even_half[:quarter], lower, upper)

    def strip(b, src, dst, step):
        at = pl.ds(b * quarter, quarter)
        return pltpu.make_async_remote_copy(
            src_ref=src.at[at], dst_ref=dst.at[at],
            send_sem=pack_send, recv_sem=pack_recv,
            device_id={"gx": lax.rem(mx + step, nx)}, device_id_type=MESH,
        )

    to_east = [strip(b, last_v, west_v, 1) for b in (0, 1)]
    to_west = [strip(b, first_v, east_v, nx - 1) for b in (0, 1)]

    for b in (0, 1):
        finish(b)
    pl.when(pack_first)(meet)

    @pl.when(jnp.logical_not(early))
    def _():
        for b in (0, 1):
            to_east[b].start()

    depth_east_v[...] = jnp.where(
        lane == w - 1, 0.0, jnp.minimum(depth, pltpu.roll(depth, w - 1, 1))
    )
    depth_north_v[...] = jnp.where(
        row == h - 1, 0.0, jnp.minimum(depth, pltpu.roll(depth, h - 1, 0))
    )

    def interior(block, carry):
        start = pl.multiple_of(block * block_rows, block_rows)
        here = pl.ds(start, block_rows)
        deep_east, deep_north = depth_east_v[here, :], depth_north_v[here, :]
        deep, gain = depth_v[here, :], g_v[here, :]
        came = [0.0, 0.0]
        for k in range(nk):
            at = pl.ds(start + k * h, block_rows)
            east_near, east_far = face_weights(uv_v[at, :], deep_east > k)
            north_near, north_far = face_weights(
                uv_v[pl.ds(start + (nk + k) * h, block_rows), :], deep_north > k
            )
            mix = jnp.where(deep > k + 1, time_step * vertical_mixing, 0.0)
            for n, (ref, out) in enumerate(((t_v, t_out), (s_v, s_out))):
                c = ref[at, :]
                east = east_near * c + east_far * pltpu.roll(c, w - 1, 1)
                north = north_near * c + north_far * ref[pl.ds(start + k * h + 1, block_rows), :]
                strip_at = (n * nk + k) * (h + 8) + 8
                flux_v[pl.ds(start + strip_at, block_rows), :] = north
                south = flux_v[pl.ds(start + strip_at - 1, block_rows), :]
                flow = (pltpu.roll(east, 1, 1) - east) + (south - north)
                fall = 0.0
                if k < nk - 1:
                    fall = mix * (c - ref[pl.ds(start + (k + 1) * h, block_rows), :])
                out[at, :] = c + (gain * flow + (came[n] - fall))
                came[n] = fall
        return carry

    split = jnp.where(early, h // block_rows, 0)

    @pl.when(early)
    def _():
        for load in loads[8:]:
            load.wait()

    lax.fori_loop(0, split, interior, 0)
    pl.when(early)(meet)

    @pl.when(early)
    def _():
        for b in (0, 1):
            to_east[b].start()

    @pl.when(jnp.logical_not(seam_west))
    def _():
        for b in (0, 1):
            to_west[b].start()

    @pl.when(jnp.logical_not(early))
    def _():
        for load in loads[8:]:
            load.wait()


    def rows(ref, row, base=0):
        return ref[pl.ds(base + row, nk, stride=h), :]

    up_v[pl.ds(0, nk), :] = rows(t_v, h - 1)
    up_v[pl.ds(nk, nk), :] = rows(s_v, h - 1)
    up_v[pl.ds(2 * nk, nk), :] = rows(uv_v, h - 1, nk * h)
    up_v[pl.ds(3 * nk, 8), :] = jnp.broadcast_to(depth[h - 1 : h, :], (8, w))
    down_v[pl.ds(0, nk), :] = rows(t_v, 0)
    down_v[pl.ds(nk, nk), :] = rows(s_v, 0)
    down_v[pl.ds(2 * nk, 8), :] = jnp.broadcast_to(depth[0:1, :], (8, w))

    @pl.when(is_top)
    def _():
        up = up_v[...]
        flip = (w - 1) - lax.broadcasted_iota(jnp.int32, up.shape, 1)
        fold_v[mx] = jnp.take_along_axis(up, flip, axis=1)

    to_north = pltpu.make_async_remote_copy(
        src_ref=up_v, dst_ref=south_v, send_sem=row_send.at[0], recv_sem=row_recv.at[0],
        device_id={"gy": lax.rem(my + 1, ny)}, device_id_type=MESH,
    )
    to_south = pltpu.make_async_remote_copy(
        src_ref=down_v, dst_ref=north_v, send_sem=row_send.at[1], recv_sem=row_recv.at[1],
        device_id={"gy": lax.rem(my + ny - 1, ny)}, device_id_type=MESH,
    )

    def fold_copy(d):
        return pltpu.make_async_remote_copy(
            src_ref=fold_v.at[mx], dst_ref=fold_v.at[mx],
            send_sem=fold_send, recv_sem=fold_recv,
            device_id={"gx": lax.rem(mx + d + 1, nx)}, device_id_type=MESH,
        )


    @pl.when(jnp.logical_not(is_top))
    def _():
        to_north.start()

    @pl.when(my > 0)
    def _():
        to_south.start()

    @pl.when(is_top)
    def _():
        repeat(nx - 1, lambda d: fold_copy(d).start())

    lax.fori_loop(split, h // block_rows, interior, 0)

    level_row = lax.broadcasted_iota(jnp.int32, (nk, w), 0).astype(jnp.float32)

    def north_edge(far_t, far_s, speed, far_depth):
        near_weight, far_weight = face_weights(
            speed, jnp.minimum(up_v[3 * nk : 3 * nk + 1, :], far_depth) > level_row
        )
        for near, far, out in (
            (up_v[pl.ds(0, nk), :], far_t, t_out),
            (up_v[pl.ds(nk, nk), :], far_s, s_out),
        ):
            at = pl.ds(h - 1, nk, stride=h)
            out[at, :] -= g_v[h - 1 : h, :] * (near_weight * near + far_weight * far)

    @pl.when(seam_west)
    def _():
        pl.semaphore_wait(ready, 1)
        for b in (0, 1):
            to_west[b].start()

    @pl.when(jnp.logical_not(is_top))
    def _():
        to_north.wait_send()
        to_south.wait_recv()
        north_edge(
            north_v[pl.ds(0, nk), :],
            north_v[pl.ds(nk, nk), :],
            up_v[pl.ds(2 * nk, nk), :],
            north_v[2 * nk : 2 * nk + 1, :],
        )

    @pl.when(my > 0)
    def _():
        to_south.wait_send()
        to_north.wait_recv()
        near_weight, far_weight = face_weights(
            south_v[pl.ds(2 * nk, nk), :],
            jnp.minimum(down_v[2 * nk : 2 * nk + 1, :], south_v[3 * nk : 3 * nk + 1, :]) > level_row,
        )
        for i, out in enumerate((t_out, s_out)):
            at = pl.ds(0, nk, stride=h)
            out[at, :] += g_v[0:1, :] * (
                near_weight * south_v[pl.ds(i * nk, nk), :]
                + far_weight * down_v[pl.ds(i * nk, nk), :]
            )

    def column(plane, at):
        return jnp.broadcast_to(plane[:, at : at + 1], (h, w))

    mine = pack_v[...]
    depth = depth_v[...]
    gain = g_v[...]
    level_of = (pair & (nk - 1)).astype(jnp.float32)
    open_cell = jnp.where(eastern, column(depth, w - 1), column(depth, 0)) > level_of
    edge_gain = jnp.where(eastern, -column(gain, w - 1), column(gain, 0))
    surface_wet = jnp.where(depth > 0.0, time_step / top_thickness, 0.0)
    surface = s0_v[...]
    s_out[pl.ds(0, h), :] -= surface_wet * surface * rain_v[...]
    for i, plane in enumerate(
        (
            mine,
            jnp.where(pair < nk, pltpu.roll(mine, w - 4 * nk, 1), pltpu.roll(mine, w - 2 * nk, 1)),
            jnp.where(open_cell, edge_gain, 0.0),
            surface_wet * surface,
            surface_wet,
        )
    ):
        side_out[pl.ds(i * h, h), :] = plane

    @pl.when(is_hub)
    def _():
        several(parts_v, peers, part_send, part_recv).wait_recv()
        total_v[...] = jnp.sum(parts_v[...], axis=0)

    in_column = mx == hub_column
    seam_giver = seam_west & is_top

    @pl.when(in_column)
    def _():
        repeat(nx - 2, lambda d: hand_on(hub_column + 1 + d, my).start())

    @pl.when(seam_giver)
    def _():
        repeat(ny - 1 - near, lambda d: hand_on(0, near + d).start())

    @pl.when(is_top)
    def _():
        several(fold_v, nx - 1, fold_send, fold_recv).wait()
        partner = fold_v[seam_smem[0] // w]
        north_edge(
            partner[:nk],
            partner[nk : 2 * nk],
            0.5 * (up_v[pl.ds(2 * nk, nk), :] - partner[2 * nk : 3 * nk]),
            partner[3 * nk : 3 * nk + 1],
        )

    @pl.when(is_hub)
    def _():
        several(parts_v, hubs - 1, part_send, part_recv).wait_send()

    @pl.when(plain)
    def _():
        several(parts_v, hubs, part_send, part_recv).wait_send()
        hand_on(0, 0).wait_recv()

    @pl.when(in_column)
    def _():
        several(parts_v, nx - 2, total_send, total_recv).wait_send()

    @pl.when(seam_giver)
    def _():
        several(parts_v, ny - 1 - near, total_send, total_recv).wait_send()

    side_out[pl.ds(6 * h, 8), :] = jnp.broadcast_to(total_v[...], (8, w))
    several(pack_v, h, pack_send, pack_recv).wait()
    side_out[pl.ds(5 * h, half), :] = west_v[...]
    side_out[pl.ds(5 * h + half, half), :] = east_v[...]


store_cuts = 4


def store_kernel(nk, h, w, t_ref, s_ref, side_ref, t_hbm, s_hbm, t_v, s_v, sem):
    half = h // 2
    mine, own_speed, edge_gain, surface, surface_wet = (
        side_ref[pl.ds(i * h, h), :] for i in range(5)
    )
    west = side_ref[pl.ds(5 * h, half), :]
    east = side_ref[pl.ds(5 * h + half, half), :]
    totals = side_ref[pl.ds(6 * h, 1), :]

    lane = lax.broadcasted_iota(jnp.int32, (h, w), 1)
    slot = jnp.where(lax.broadcasted_iota(jnp.int32, (h, w), 0) < half, lane, lane - 1)
    pair = slot >> 1
    eastern = (slot & 1) == 0

    def both(cells):
        return jnp.concatenate([cells, cells], axis=0)

    def moved(cells, by):
        return both(pltpu.roll(cells, by % w, 1))

    def columns(cells, at):
        return jnp.concatenate(
            [jnp.broadcast_to(cells[:, i : i + 1], (half, w)) for i in (at, at + 1)], axis=0
        )

    near = jnp.where(eastern, mine, moved(west, 1))
    far = jnp.where(eastern, moved(east, -1), mine)
    west_speed = jnp.where(pair < nk, moved(west, 1 - 4 * nk), moved(west, 1 - 2 * nk))
    far_depth = jnp.where(eastern, columns(east, 6 * nk + 1), columns(west, 6 * nk))
    near_weight, far_weight = face_weights(
        jnp.where(eastern, own_speed, west_speed),
        far_depth > (pair & (nk - 1)).astype(jnp.float32),
    )
    edge = edge_gain * (near_weight * near + far_weight * far)

    total_area, total_fresh, salt_fresh, salt_only = (
        jnp.broadcast_to(totals[:, i : i + 1], (1, w)) for i in range(4)
    )
    mean_fresh = total_fresh / total_area
    lift = (salt_fresh - mean_fresh * salt_only) / total_area
    virtual = surface_wet * lift + surface * mean_fresh

    at_edge = (lane[:half] == 0) | (lane[:half] == w - 1)
    step = nk // store_cuts
    for i, (ref, out, hbm) in enumerate(((t_ref, t_v, t_hbm), (s_ref, s_v, s_hbm))):
        for cut in reversed(range(store_cuts)):
            for k in range(cut * step, (cut + 1) * step):
                j = i * nk + k
                for part, shift in ((0, w - 1 - 2 * j), (1, w - 2 - 2 * j)):
                    rows = slice(part * half, (part + 1) * half)
                    change = jnp.where(at_edge, pltpu.roll(edge[rows], shift % w, 1), 0.0)
                    if j == nk:
                        change = change + virtual[rows]
                    at = pl.ds(k * h + part * half, half)
                    out[at, :] = ref[at, :] + change
            at = pl.ds(cut * step * h, step * h)
            pltpu.make_async_copy(out.at[at], hbm.at[at], sem).start()
    for out, hbm in ((t_v, t_hbm), (s_v, s_hbm)):
        pltpu.make_async_copy(out, hbm, sem).wait()


def shards(nx, ny, t, s, uv, sea, layers, area, rain, seam):
    nk, h, w = t.shape
    assert w == 128 and h % 16 == 0 and nk & (nk - 1) == 0 and nk % 8 == 0 and 6 * nk + 3 <= w and nx > 3 and ny > 3
    f32 = jnp.float32
    peers = nx * ny - 1
    half_plane = pltpu.VMEM((h // 2, w), f32)
    vmem = 67043328 - 4 * w * (2 * nk * h + 6 * h + 8)
    any_space = pl.BlockSpec(memory_space=pl.ANY)
    dma = pltpu.SemaphoreType.DMA
    plane = pltpu.VMEM((h, w), f32)
    t_next, s_next, side = pl.pallas_call(
        functools.partial(kernel, nx, ny, nk, h, w),
        out_shape=[pltpu.VMEM((nk * h, w), f32)] * 2 + [pltpu.VMEM((6 * h + 8, w), f32)],
        in_specs=[any_space] * 8,
        out_specs=[pl.BlockSpec(memory_space=pltpu.VMEM)] * 3,
        scratch_shapes=[
            pltpu.VMEM((nk * h + 8, w), f32),
            pltpu.VMEM((nk * h + 8, w), f32),
            pltpu.VMEM((2 * nk * h, w), f32),
            pltpu.VMEM((h, w), jnp.int32),
            pltpu.VMEM((h, w), jnp.int32),
            plane, plane, plane, plane, plane,
            plane, half_plane, half_plane, half_plane, half_plane,
            pltpu.VMEM((3 * nk + 8, w), f32),
            pltpu.VMEM((2 * nk + 8, w), f32),
            pltpu.VMEM((3 * nk + 8, w), f32),
            pltpu.VMEM((2 * nk + 8, w), f32),
            pltpu.VMEM((nx, 3 * nk + 8, w), f32),
            pltpu.VMEM((1, w), f32),
            pltpu.VMEM((nx * ny, 1, w), f32),
            pltpu.VMEM((1, w), f32),
            pltpu.SMEM((w,), jnp.int32),
            plane, plane,
            pltpu.VMEM((2 * nk * (h + 8), w), f32),
            dma((6,)), dma, dma, dma((2,)), dma((2,)),
            dma, dma, dma, dma, dma, dma, pltpu.SemaphoreType.REGULAR,
        ],
        compiler_params=pltpu.CompilerParams(
            collective_id=0, has_side_effects=True, vmem_limit_bytes=vmem
        ),
        name="tracer_step",
    )(
        t.reshape(nk * h, w), s.reshape(nk * h, w), uv.reshape(2 * nk * h, w),
        sea, layers, area, rain, seam,
    )
    t_next, s_next = pl.pallas_call(
        functools.partial(store_kernel, nk, h, w),
        out_shape=[jax.ShapeDtypeStruct((nk * h, w), f32)] * 2,
        in_specs=[pl.BlockSpec(memory_space=pltpu.VMEM)] * 3,
        out_specs=[any_space] * 2,
        scratch_shapes=[pltpu.VMEM((nk * h, w), f32)] * 2 + [dma],
        compiler_params=pltpu.CompilerParams(vmem_limit_bytes=8 << 20),
        name="store",
    )(t_next, s_next, side)
    return t_next.reshape(t.shape), s_next.reshape(s.shape)


def solution(mesh):
    in_specs = (
        P("groups", "gy", "gx"),
        P("groups", "gy", "gx"),
        P("groups", None, "gy", "gx"),
        P("gy", "gx"),
        P("gy", "gx"),
        P("gy", "gx"),
        P("gy", "gx"),
        P("gx"),
    )
    out_specs = (P("groups", "gy", "gx"), P("groups", "gy", "gx"))
    return jax.shard_map(
        functools.partial(shards, mesh.shape["gx"], mesh.shape["gy"]),
        mesh=mesh, in_specs=in_specs, out_specs=out_specs, check_vma=False,
    )
```

```python
import functools

import jax
import jax.numpy as jnp
from jax import lax
from jax.experimental import pallas as pl
from jax.experimental.pallas import tpu as pltpu
from jax.sharding import PartitionSpec as P

time_step = 0.25
diffusivity = 0.5
vertical_mixing = 0.3
top_thickness = 0.5

block_rows = 16
hub_column = 1

MESH = pl.DeviceIdType.MESH


def repeat(count, body):
    if count <= 16:
        for i in range(count):
            body(i)
    else:
        pl.loop(0, count)(body)


def face_weights(speed, open_face):
    near_weight = jnp.maximum(speed, 0.0) + diffusivity
    far_weight = speed - near_weight
    return jnp.where(open_face, near_weight, 0.0), jnp.where(open_face, far_weight, 0.0)


def kernel(
    nx, ny, nk, h, w,
    t_hbm, s_hbm, uv_hbm, sea_hbm, lay_hbm, area_hbm, rain_hbm, seam_hbm,
    t_out, s_out, side_out,
    t_v, s_v, uv_v, sea_v, lay_v, area_v, rain_v, s0_v, g_v, depth_v,
    pack_v, last_v, first_v, east_v, west_v, up_v, down_v, south_v, north_v, fold_v,
    part_v, parts_v, total_v, seam_smem, depth_east_v, depth_north_v, flux_v,
    load_sems, pack_send, pack_recv, row_send, row_recv, fold_send, fold_recv,
    part_send, part_recv, total_send, total_recv, ready,
):
    mx, my = lax.axis_index("gx"), lax.axis_index("gy")
    is_top = my == ny - 1
    peers = nx * ny - 1

    barrier = pltpu.get_barrier_semaphore()

    east, west = lax.rem(mx + 1, nx), lax.rem(mx + nx - 1, nx)
    near = ny // 2
    hubs = near + 1 + ny

    def hub(gx, gy):
        return (gx == hub_column) | ((gx == 0) & ((gy < near) | (gy == ny - 1)))

    is_hub = hub(mx, my)
    plain = jnp.logical_not(is_hub)
    seam_west = mx == 0
    seam_east = mx == nx - 1
    has_north, has_south = my < ny - 1, my > 0

    def count(flag):
        return jnp.where(flag, 1, 0)

    row_partners = jnp.where(
        is_top,
        nx - 2 - count(mx > hub_column),
        count(jnp.logical_not(hub(east, my)))
        + count(jnp.logical_not(hub(west, my) | seam_west)),
    )
    partners = (
        hubs - count(is_hub) + row_partners
        + count(has_north & jnp.logical_not(hub(mx, my + 1)))
        + count(has_south & jnp.logical_not(hub(mx, my - 1)))
    )

    def signal(gx, gy):
        pl.semaphore_signal(
            barrier, inc=1, device_id={"gx": gx, "gy": gy}, device_id_type=MESH
        )

    def greet():
        @pl.when(is_hub)
        def _():
            def one(r):
                r = r + 1
                signal(lax.rem(mx + r // ny, nx), lax.rem(my + r % ny, ny))

            repeat(peers, one)

        @pl.when(plain & is_top)
        def _():
            repeat(nx - 1, lambda d: signal(lax.rem(mx + 1 + d, nx), my))

        @pl.when(plain & has_north)
        def _():
            signal(west, my)
            pl.when(jnp.logical_not(seam_east))(lambda: signal(east, my))
            signal(mx, my + 1)

        @pl.when(plain & has_south)
        def _():
            signal(mx, my - 1)

    loads = [
        pltpu.make_async_copy(src, dst, load_sems.at[max(i - 4, 0)])
        for i, (src, dst) in enumerate(
            [
                (area_hbm, area_v),
                (sea_hbm, sea_v),
                (rain_hbm, rain_v),
                (s_hbm.at[pl.ds(0, h)], s0_v),
                (lay_hbm, lay_v),
                (t_hbm, t_v.at[pl.ds(0, nk * h)]),
                (s_hbm, s_v.at[pl.ds(0, nk * h)]),
                (uv_hbm.at[pl.ds(0, nk * h)], uv_v.at[pl.ds(0, nk * h)]),
                (uv_hbm.at[pl.ds(nk * h, nk * h)], uv_v.at[pl.ds(nk * h, nk * h)]),
                (seam_hbm, seam_smem),
            ]
        )
    ]
    for load in loads[:8]:
        load.start()
    greet()
    for load in loads[8:]:
        load.start()
    zeros = jnp.zeros((8, w), jnp.float32)
    for ref in (t_v, s_v):
        ref[pl.ds(nk * h, 8), :] = zeros
    for i in range(2 * nk):
        flux_v[pl.ds(i * (h + 8), 8), :] = zeros

    small = pl.ds(0, 5 * h)
    pltpu.make_async_copy(t_hbm.at[small], t_v.at[small], load_sems.at[0]).wait()
    area = area_v[...]
    sea = sea_v[...]
    wet_area = area * sea.astype(jnp.float32)
    surface = s0_v[...]
    fresh = wet_area * rain_v[...]
    lane1 = lax.broadcasted_iota(jnp.int32, (1, w), 1)
    part = jnp.zeros((1, w), jnp.float32)
    for i, term in enumerate((wet_area, fresh, fresh * surface, wet_area * surface)):
        rows8 = jnp.sum(term.reshape(h // 8, 8, w), axis=0)
        part = jnp.where(
            lane1 == i, jnp.sum(jnp.sum(rows8, axis=1, keepdims=True), axis=0, keepdims=True), part
        )
    part_v[...] = part
    gain = time_step / area
    g_v[...] = gain

    me = mx * ny + my
    parts_v[me] = part

    def send_part(gx, gy):
        @pl.when(gx * ny + gy != me)
        def _():
            pltpu.make_async_remote_copy(
                src_ref=part_v, dst_ref=parts_v.at[me], send_sem=part_send, recv_sem=part_recv,
                device_id={"gx": gx, "gy": gy}, device_id_type=MESH,
            ).start()

    def several(ref, n, sends, arrivals):
        block = ref.at[pl.ds(0, n)]
        return pltpu.make_async_remote_copy(
            src_ref=block, dst_ref=block, send_sem=sends, recv_sem=arrivals,
            device_id={"gx": east}, device_id_type=MESH,
        )

    def hand_on(gx, gy):
        return pltpu.make_async_remote_copy(
            src_ref=total_v, dst_ref=total_v, send_sem=total_send, recv_sem=total_recv,
            device_id={"gx": gx, "gy": gy}, device_id_type=MESH,
        )

    def meet():
        pl.semaphore_wait(barrier, partners)
        repeat(near, lambda gy: send_part(0, gy))
        send_part(0, ny - 1)
        repeat(ny, lambda gy: send_part(hub_column, gy))
        pl.when(seam_east)(
            lambda: pl.semaphore_signal(ready, inc=1, device_id={"gx": east}, device_id_type=MESH)
        )

    early = seam_west & (my < near)
    pack_first = (mx > 0) & (my < near)
    pl.when(my >= near)(meet)

    depth = (sea * lay_v[...]).astype(jnp.float32)
    depth_v[...] = depth

    half = h // 2
    depth_at = 6 * nk
    lane = lax.broadcasted_iota(jnp.int32, (h, w), 1)
    row = lax.broadcasted_iota(jnp.int32, (h, w), 0)
    slot = jnp.where(row < half, lane, lane - 1)
    pair = slot >> 1
    eastern = (slot & 1) == 0
    even_half = (lane[:half] & 1) == 0

    quarter = h // 4

    def cells(ref, k, b):
        return [
            ref[pl.ds(k * h + side * half + b * quarter, quarter), :] for side in (0, 1)
        ]

    def pack(packed, b, ref, first, count):
        for k in range(count):
            j = first + k
            packed = [
                jnp.where(
                    pair[side * half : side * half + quarter] == j,
                    pltpu.roll(plane, 2 * j + 1 + side, 1),
                    old,
                )
                for side, (plane, old) in enumerate(zip(cells(ref, k, b), packed))
            ]
        return packed

    empty = [jnp.zeros((quarter, w), jnp.float32)] * 2
    packed = [pack(empty, b, depth_v, 3 * nk, 1) for b in (0, 1)]
    for i, ref in enumerate((t_v, s_v)):
        loads[5 + i].wait()
        packed = [pack(packed[b], b, ref, i * nk, nk) for b in (0, 1)]
    loads[7].wait()

    def finish(b):
        upper, lower = pack(packed[b], b, uv_v, 2 * nk, nk)
        pack_v[pl.ds(b * quarter, quarter), :] = upper
        pack_v[pl.ds(half + b * quarter, quarter), :] = lower
        at = pl.ds(b * quarter, quarter)
        last_v[at, :] = jnp.where(even_half[:quarter], upper, lower)
        first_v[at, :] = jnp.where(even_half[:quarter], lower, upper)

    def strip(b, src, dst, step):
        at = pl.ds(b * quarter, quarter)
        return pltpu.make_async_remote_copy(
            src_ref=src.at[at], dst_ref=dst.at[at],
            send_sem=pack_send, recv_sem=pack_recv,
            device_id={"gx": lax.rem(mx + step, nx)}, device_id_type=MESH,
        )

    to_east = [strip(b, last_v, west_v, 1) for b in (0, 1)]
    to_west = [strip(b, first_v, east_v, nx - 1) for b in (0, 1)]

    for b in (0, 1):
        finish(b)
    pl.when(pack_first)(meet)

    @pl.when(jnp.logical_not(early))
    def _():
        for b in (0, 1):
            to_east[b].start()

    depth_east_v[...] = jnp.where(
        lane == w - 1, 0.0, jnp.minimum(depth, pltpu.roll(depth, w - 1, 1))
    )
    depth_north_v[...] = jnp.where(
        row == h - 1, 0.0, jnp.minimum(depth, pltpu.roll(depth, h - 1, 0))
    )

    def interior(block, carry):
        start = pl.multiple_of(block * block_rows, block_rows)
        here = pl.ds(start, block_rows)
        deep_east, deep_north = depth_east_v[here, :], depth_north_v[here, :]
        deep, gain = depth_v[here, :], g_v[here, :]
        came = [0.0, 0.0]
        for k in range(nk):
            at = pl.ds(start + k * h, block_rows)
            east_near, east_far = face_weights(uv_v[at, :], deep_east > k)
            north_near, north_far = face_weights(
                uv_v[pl.ds(start + (nk + k) * h, block_rows), :], deep_north > k
            )
            mix = jnp.where(deep > k + 1, time_step * vertical_mixing, 0.0)
            for n, (ref, out) in enumerate(((t_v, t_out), (s_v, s_out))):
                c = ref[at, :]
                east = east_near * c + east_far * pltpu.roll(c, w - 1, 1)
                north = north_near * c + north_far * ref[pl.ds(start + k * h + 1, block_rows), :]
                strip_at = (n * nk + k) * (h + 8) + 8
                flux_v[pl.ds(start + strip_at, block_rows), :] = north
                south = flux_v[pl.ds(start + strip_at - 1, block_rows), :]
                flow = (pltpu.roll(east, 1, 1) - east) + (south - north)
                fall = 0.0
                if k < nk - 1:
                    fall = mix * (c - ref[pl.ds(start + (k + 1) * h, block_rows), :])
                out[at, :] = c + (gain * flow + (came[n] - fall))
                came[n] = fall
        return carry

    split = jnp.where(early, h // block_rows, 0)

    @pl.when(early)
    def _():
        for load in loads[8:]:
            load.wait()

    lax.fori_loop(0, split, interior, 0)
    pl.when(early)(meet)

    @pl.when(early)
    def _():
        for b in (0, 1):
            to_east[b].start()

    @pl.when(jnp.logical_not(seam_west))
    def _():
        for b in (0, 1):
            to_west[b].start()

    @pl.when(jnp.logical_not(early))
    def _():
        for load in loads[8:]:
            load.wait()


    def rows(ref, row, base=0):
        return ref[pl.ds(base + row, nk, stride=h), :]

    up_v[pl.ds(0, nk), :] = rows(t_v, h - 1)
    up_v[pl.ds(nk, nk), :] = rows(s_v, h - 1)
    up_v[pl.ds(2 * nk, nk), :] = rows(uv_v, h - 1, nk * h)
    up_v[pl.ds(3 * nk, 8), :] = jnp.broadcast_to(depth[h - 1 : h, :], (8, w))
    down_v[pl.ds(0, nk), :] = rows(t_v, 0)
    down_v[pl.ds(nk, nk), :] = rows(s_v, 0)
    down_v[pl.ds(2 * nk, 8), :] = jnp.broadcast_to(depth[0:1, :], (8, w))

    @pl.when(is_top)
    def _():
        up = up_v[...]
        flip = (w - 1) - lax.broadcasted_iota(jnp.int32, up.shape, 1)
        fold_v[mx] = jnp.take_along_axis(up, flip, axis=1)

    to_north = pltpu.make_async_remote_copy(
        src_ref=up_v, dst_ref=south_v, send_sem=row_send.at[0], recv_sem=row_recv.at[0],
        device_id={"gy": lax.rem(my + 1, ny)}, device_id_type=MESH,
    )
    to_south = pltpu.make_async_remote_copy(
        src_ref=down_v, dst_ref=north_v, send_sem=row_send.at[1], recv_sem=row_recv.at[1],
        device_id={"gy": lax.rem(my + ny - 1, ny)}, device_id_type=MESH,
    )

    def fold_copy(d):
        return pltpu.make_async_remote_copy(
            src_ref=fold_v.at[mx], dst_ref=fold_v.at[mx],
            send_sem=fold_send, recv_sem=fold_recv,
            device_id={"gx": lax.rem(mx + d + 1, nx)}, device_id_type=MESH,
        )


    @pl.when(jnp.logical_not(is_top))
    def _():
        to_north.start()

    @pl.when(my > 0)
    def _():
        to_south.start()

    @pl.when(is_top)
    def _():
        repeat(nx - 1, lambda d: fold_copy(d).start())

    lax.fori_loop(split, h // block_rows, interior, 0)

    level_row = lax.broadcasted_iota(jnp.int32, (nk, w), 0).astype(jnp.float32)

    def north_edge(far_t, far_s, speed, far_depth):
        near_weight, far_weight = face_weights(
            speed, jnp.minimum(up_v[3 * nk : 3 * nk + 1, :], far_depth) > level_row
        )
        for near, far, out in (
            (up_v[pl.ds(0, nk), :], far_t, t_out),
            (up_v[pl.ds(nk, nk), :], far_s, s_out),
        ):
            at = pl.ds(h - 1, nk, stride=h)
            out[at, :] -= g_v[h - 1 : h, :] * (near_weight * near + far_weight * far)

    @pl.when(seam_west)
    def _():
        pl.semaphore_wait(ready, 1)
        for b in (0, 1):
            to_west[b].start()

    @pl.when(jnp.logical_not(is_top))
    def _():
        to_north.wait_send()
        to_south.wait_recv()
        north_edge(
            north_v[pl.ds(0, nk), :],
            north_v[pl.ds(nk, nk), :],
            up_v[pl.ds(2 * nk, nk), :],
            north_v[2 * nk : 2 * nk + 1, :],
        )

    @pl.when(my > 0)
    def _():
        to_south.wait_send()
        to_north.wait_recv()
        near_weight, far_weight = face_weights(
            south_v[pl.ds(2 * nk, nk), :],
            jnp.minimum(down_v[2 * nk : 2 * nk + 1, :], south_v[3 * nk : 3 * nk + 1, :]) > level_row,
        )
        for i, out in enumerate((t_out, s_out)):
            at = pl.ds(0, nk, stride=h)
            out[at, :] += g_v[0:1, :] * (
                near_weight * south_v[pl.ds(i * nk, nk), :]
                + far_weight * down_v[pl.ds(i * nk, nk), :]
            )

    def column(plane, at):
        return jnp.broadcast_to(plane[:, at : at + 1], (h, w))

    mine = pack_v[...]
    depth = depth_v[...]
    gain = g_v[...]
    level_of = (pair & (nk - 1)).astype(jnp.float32)
    open_cell = jnp.where(eastern, column(depth, w - 1), column(depth, 0)) > level_of
    edge_gain = jnp.where(eastern, -column(gain, w - 1), column(gain, 0))
    surface_wet = jnp.where(depth > 0.0, time_step / top_thickness, 0.0)
    surface = s0_v[...]
    s_out[pl.ds(0, h), :] -= surface_wet * surface * rain_v[...]
    for i, plane in enumerate(
        (
            mine,
            jnp.where(pair < nk, pltpu.roll(mine, w - 4 * nk, 1), pltpu.roll(mine, w - 2 * nk, 1)),
            jnp.where(open_cell, edge_gain, 0.0),
            surface_wet * surface,
            surface_wet,
        )
    ):
        side_out[pl.ds(i * h, h), :] = plane

    @pl.when(is_hub)
    def _():
        several(parts_v, peers, part_send, part_recv).wait_recv()
        total_v[...] = jnp.sum(parts_v[...], axis=0)

    in_column = mx == hub_column
    seam_giver = seam_west & is_top

    @pl.when(in_column)
    def _():
        repeat(nx - 2, lambda d: hand_on(hub_column + 1 + d, my).start())

    @pl.when(seam_giver)
    def _():
        repeat(ny - 1 - near, lambda d: hand_on(0, near + d).start())

    @pl.when(is_top)
    def _():
        several(fold_v, nx - 1, fold_send, fold_recv).wait()
        partner = fold_v[seam_smem[0] // w]
        north_edge(
            partner[:nk],
            partner[nk : 2 * nk],
            0.5 * (up_v[pl.ds(2 * nk, nk), :] - partner[2 * nk : 3 * nk]),
            partner[3 * nk : 3 * nk + 1],
        )

    @pl.when(is_hub)
    def _():
        several(parts_v, hubs - 1, part_send, part_recv).wait_send()

    @pl.when(plain)
    def _():
        several(parts_v, hubs, part_send, part_recv).wait_send()
        hand_on(0, 0).wait_recv()

    @pl.when(in_column)
    def _():
        several(parts_v, nx - 2, total_send, total_recv).wait_send()

    @pl.when(seam_giver)
    def _():
        several(parts_v, ny - 1 - near, total_send, total_recv).wait_send()

    side_out[pl.ds(6 * h, 8), :] = jnp.broadcast_to(total_v[...], (8, w))
    several(pack_v, h, pack_send, pack_recv).wait()
    side_out[pl.ds(5 * h, half), :] = west_v[...]
    side_out[pl.ds(5 * h + half, half), :] = east_v[...]


store_cuts = 16


def store_kernel(nk, h, w, t_ref, s_ref, side_ref, t_hbm, s_hbm, t_v, s_v, sem):
    half = h // 2
    mine, own_speed, edge_gain, surface, surface_wet = (
        side_ref[pl.ds(i * h, h), :] for i in range(5)
    )
    west = side_ref[pl.ds(5 * h, half), :]
    east = side_ref[pl.ds(5 * h + half, half), :]
    totals = side_ref[pl.ds(6 * h, 1), :]

    lane = lax.broadcasted_iota(jnp.int32, (h, w), 1)
    slot = jnp.where(lax.broadcasted_iota(jnp.int32, (h, w), 0) < half, lane, lane - 1)
    pair = slot >> 1
    eastern = (slot & 1) == 0

    def both(cells):
        return jnp.concatenate([cells, cells], axis=0)

    def moved(cells, by):
        return both(pltpu.roll(cells, by % w, 1))

    def columns(cells, at):
        return jnp.concatenate(
            [jnp.broadcast_to(cells[:, i : i + 1], (half, w)) for i in (at, at + 1)], axis=0
        )

    near = jnp.where(eastern, mine, moved(west, 1))
    far = jnp.where(eastern, moved(east, -1), mine)
    west_speed = jnp.where(pair < nk, moved(west, 1 - 4 * nk), moved(west, 1 - 2 * nk))
    far_depth = jnp.where(eastern, columns(east, 6 * nk + 1), columns(west, 6 * nk))
    near_weight, far_weight = face_weights(
        jnp.where(eastern, own_speed, west_speed),
        far_depth > (pair & (nk - 1)).astype(jnp.float32),
    )
    edge = edge_gain * (near_weight * near + far_weight * far)

    total_area, total_fresh, salt_fresh, salt_only = (
        jnp.broadcast_to(totals[:, i : i + 1], (1, w)) for i in range(4)
    )
    mean_fresh = total_fresh / total_area
    lift = (salt_fresh - mean_fresh * salt_only) / total_area
    virtual = surface_wet * lift + surface * mean_fresh

    at_edge = (lane[:half] == 0) | (lane[:half] == w - 1)
    step = nk // store_cuts
    for i, (ref, out, hbm) in enumerate(((t_ref, t_v, t_hbm), (s_ref, s_v, s_hbm))):
        for cut in reversed(range(store_cuts)):
            for k in range(cut * step, (cut + 1) * step):
                j = i * nk + k
                for part, shift in ((0, w - 1 - 2 * j), (1, w - 2 - 2 * j)):
                    rows = slice(part * half, (part + 1) * half)
                    change = jnp.where(at_edge, pltpu.roll(edge[rows], shift % w, 1), 0.0)
                    if j == nk:
                        change = change + virtual[rows]
                    at = pl.ds(k * h + part * half, half)
                    out[at, :] = ref[at, :] + change
            at = pl.ds(cut * step * h, step * h)
            pltpu.make_async_copy(out.at[at], hbm.at[at], sem).start()
    for out, hbm in ((t_v, t_hbm), (s_v, s_hbm)):
        pltpu.make_async_copy(out, hbm, sem).wait()


def shards(nx, ny, t, s, uv, sea, layers, area, rain, seam):
    nk, h, w = t.shape
    assert w == 128 and h % 16 == 0 and nk & (nk - 1) == 0 and nk % 8 == 0 and 6 * nk + 3 <= w and nx > 3 and ny > 3
    f32 = jnp.float32
    peers = nx * ny - 1
    half_plane = pltpu.VMEM((h // 2, w), f32)
    vmem = 67043328 - 4 * w * (2 * nk * h + 6 * h + 8)
    any_space = pl.BlockSpec(memory_space=pl.ANY)
    dma = pltpu.SemaphoreType.DMA
    plane = pltpu.VMEM((h, w), f32)
    t_next, s_next, side = pl.pallas_call(
        functools.partial(kernel, nx, ny, nk, h, w),
        out_shape=[pltpu.VMEM((nk * h, w), f32)] * 2 + [pltpu.VMEM((6 * h + 8, w), f32)],
        in_specs=[any_space] * 8,
        out_specs=[pl.BlockSpec(memory_space=pltpu.VMEM)] * 3,
        scratch_shapes=[
            pltpu.VMEM((nk * h + 8, w), f32),
            pltpu.VMEM((nk * h + 8, w), f32),
            pltpu.VMEM((2 * nk * h, w), f32),
            pltpu.VMEM((h, w), jnp.int32),
            pltpu.VMEM((h, w), jnp.int32),
            plane, plane, plane, plane, plane,
            plane, half_plane, half_plane, half_plane, half_plane,
            pltpu.VMEM((3 * nk + 8, w), f32),
            pltpu.VMEM((2 * nk + 8, w), f32),
            pltpu.VMEM((3 * nk + 8, w), f32),
            pltpu.VMEM((2 * nk + 8, w), f32),
            pltpu.VMEM((nx, 3 * nk + 8, w), f32),
            pltpu.VMEM((1, w), f32),
            pltpu.VMEM((nx * ny, 1, w), f32),
            pltpu.VMEM((1, w), f32),
            pltpu.SMEM((w,), jnp.int32),
            plane, plane,
            pltpu.VMEM((2 * nk * (h + 8), w), f32),
            dma((6,)), dma, dma, dma((2,)), dma((2,)),
            dma, dma, dma, dma, dma, dma, pltpu.SemaphoreType.REGULAR,
        ],
        compiler_params=pltpu.CompilerParams(
            collective_id=0, has_side_effects=True, vmem_limit_bytes=vmem
        ),
        name="tracer_step",
    )(
        t.reshape(nk * h, w), s.reshape(nk * h, w), uv.reshape(2 * nk * h, w),
        sea, layers, area, rain, seam,
    )
    t_next, s_next = pl.pallas_call(
        functools.partial(store_kernel, nk, h, w),
        out_shape=[jax.ShapeDtypeStruct((nk * h, w), f32)] * 2,
        in_specs=[pl.BlockSpec(memory_space=pltpu.VMEM)] * 3,
        out_specs=[any_space] * 2,
        scratch_shapes=[pltpu.VMEM((nk * h, w), f32)] * 2 + [dma],
        compiler_params=pltpu.CompilerParams(vmem_limit_bytes=8 << 20),
        name="store",
    )(t_next, s_next, side)
    return t_next.reshape(t.shape), s_next.reshape(s.shape)


def solution(mesh):
    in_specs = (
        P("groups", "gy", "gx"),
        P("groups", "gy", "gx"),
        P("groups", None, "gy", "gx"),
        P("gy", "gx"),
        P("gy", "gx"),
        P("gy", "gx"),
        P("gy", "gx"),
        P("gx"),
    )
    out_specs = (P("groups", "gy", "gx"), P("groups", "gy", "gx"))
    return jax.shard_map(
        functools.partial(shards, mesh.shape["gx"], mesh.shape["gy"]),
        mesh=mesh, in_specs=in_specs, out_specs=out_specs, check_vma=False,
    )
```

```python
import functools

import jax
import jax.numpy as jnp
from jax import lax
from jax.experimental import pallas as pl
from jax.experimental.pallas import tpu as pltpu
from jax.sharding import PartitionSpec as P

time_step = 0.25
diffusivity = 0.5
vertical_mixing = 0.3
top_thickness = 0.5

block_rows = 16
hub_column = 1

MESH = pl.DeviceIdType.MESH


def repeat(count, body):
    if count <= 16:
        for i in range(count):
            body(i)
    else:
        pl.loop(0, count)(body)


def face_weights(speed, open_face):
    near_weight = jnp.maximum(speed, 0.0) + diffusivity
    far_weight = speed - near_weight
    return jnp.where(open_face, near_weight, 0.0), jnp.where(open_face, far_weight, 0.0)


def kernel(
    nx, ny, nk, h, w,
    t_hbm, s_hbm, uv_hbm, sea_hbm, lay_hbm, area_hbm, rain_hbm, seam_hbm,
    t_out, s_out, side_out,
    t_v, s_v, uv_v, sea_v, lay_v, area_v, rain_v, s0_v, g_v, depth_v,
    pack_v, last_v, first_v, east_v, west_v, up_v, down_v, south_v, north_v, fold_v,
    part_v, parts_v, total_v, seam_smem, depth_east_v, depth_north_v, flux_v,
    load_sems, side_send, pack_recv, row_recv, part_send, part_recv, ready,
):
    mx, my = lax.axis_index("gx"), lax.axis_index("gy")
    is_top = my == ny - 1
    peers = nx * ny - 1

    barrier = pltpu.get_barrier_semaphore()

    east, west = lax.rem(mx + 1, nx), lax.rem(mx + nx - 1, nx)
    near = ny // 2
    hubs = near + 1 + ny

    def hub(gx, gy):
        return (gx == hub_column) | ((gx == 0) & ((gy < near) | (gy == ny - 1)))

    is_hub = hub(mx, my)
    plain = jnp.logical_not(is_hub)
    seam_west = mx == 0
    seam_east = mx == nx - 1
    has_north, has_south = my < ny - 1, my > 0

    def count(flag):
        return jnp.where(flag, 1, 0)

    row_partners = jnp.where(
        is_top,
        nx - 2 - count(mx > hub_column),
        count(jnp.logical_not(hub(east, my)))
        + count(jnp.logical_not(hub(west, my) | seam_west)),
    )
    partners = (
        hubs - count(is_hub) + row_partners
        + count(has_north & jnp.logical_not(hub(mx, my + 1)))
        + count(has_south & jnp.logical_not(hub(mx, my - 1)))
    )

    def signal(gx, gy):
        pl.semaphore_signal(
            barrier, inc=1, device_id={"gx": gx, "gy": gy}, device_id_type=MESH
        )

    def greet():
        @pl.when(is_hub)
        def _():
            def one(r):
                r = r + 1
                signal(lax.rem(mx + r // ny, nx), lax.rem(my + r % ny, ny))

            repeat(peers, one)

        @pl.when(plain & is_top)
        def _():
            repeat(nx - 1, lambda d: signal(lax.rem(mx + 1 + d, nx), my))

        @pl.when(plain & has_north)
        def _():
            signal(west, my)
            pl.when(jnp.logical_not(seam_east))(lambda: signal(east, my))
            signal(mx, my + 1)

        @pl.when(plain & has_south)
        def _():
            signal(mx, my - 1)

    loads = [
        pltpu.make_async_copy(src, dst, load_sems.at[min(max(i - 4, 0), 4)])
        for i, (src, dst) in enumerate(
            [
                (area_hbm, area_v),
                (sea_hbm, sea_v),
                (rain_hbm, rain_v),
                (s_hbm.at[pl.ds(0, h)], s0_v),
                (lay_hbm, lay_v),
                (t_hbm, t_v.at[pl.ds(0, nk * h)]),
                (s_hbm, s_v.at[pl.ds(0, nk * h)]),
                (uv_hbm.at[pl.ds(0, nk * h)], uv_v.at[pl.ds(0, nk * h)]),
                (uv_hbm.at[pl.ds(nk * h, nk * h)], uv_v.at[pl.ds(nk * h, nk * h)]),
                (seam_hbm, seam_smem),
            ]
        )
    ]
    for load in loads[:8]:
        load.start()
    greet()
    for load in loads[8:]:
        load.start()
    zeros = jnp.zeros((8, w), jnp.float32)
    for ref in (t_v, s_v):
        ref[pl.ds(nk * h, 8), :] = zeros
    for i in range(2 * nk):
        flux_v[pl.ds(i * (h + 8), 8), :] = zeros

    rest = pl.ds(0, nk * h + 1)
    late_loads = pltpu.make_async_copy(uv_hbm.at[rest], t_v.at[rest], load_sems.at[4])
    small = pl.ds(0, 5 * h)
    pltpu.make_async_copy(t_hbm.at[small], t_v.at[small], load_sems.at[0]).wait()
    area = area_v[...]
    sea = sea_v[...]
    wet_area = area * sea.astype(jnp.float32)
    surface = s0_v[...]
    fresh = wet_area * rain_v[...]
    lane1 = lax.broadcasted_iota(jnp.int32, (1, w), 1)
    part = jnp.zeros((1, w), jnp.float32)
    for i, term in enumerate((wet_area, fresh, fresh * surface, wet_area * surface)):
        rows8 = jnp.sum(term.reshape(h // 8, 8, w), axis=0)
        part = jnp.where(
            lane1 == i, jnp.sum(jnp.sum(rows8, axis=1, keepdims=True), axis=0, keepdims=True), part
        )
    part_v[...] = part
    gain = time_step / area
    g_v[...] = gain

    me = mx * ny + my
    parts_v[me] = part

    def send_part(gx, gy):
        @pl.when(gx * ny + gy != me)
        def _():
            pltpu.make_async_remote_copy(
                src_ref=part_v, dst_ref=parts_v.at[me], send_sem=part_send, recv_sem=part_recv,
                device_id={"gx": gx, "gy": gy}, device_id_type=MESH,
            ).start()

    edge_rows = 3 * nk + 8
    down_rows = 2 * nk + 8

    def bytes_of(n, sends, arrivals):
        block = flux_v.at[pl.ds(0, n)]
        return pltpu.make_async_remote_copy(
            src_ref=block, dst_ref=block, send_sem=sends, recv_sem=arrivals,
            device_id={"gx": east}, device_id_type=MESH,
        )

    def sent(flag, n, sends):
        pl.when(flag)(lambda: bytes_of(n, sends, pack_recv).wait_send())

    def came(flag, n, arrivals):
        pl.when(flag)(lambda: bytes_of(n, side_send, arrivals).wait_recv())

    def hand_on(gx, gy):
        return pltpu.make_async_remote_copy(
            src_ref=total_v, dst_ref=total_v, send_sem=part_send, recv_sem=part_recv,
            device_id={"gx": gx, "gy": gy}, device_id_type=MESH,
        )

    def meet():
        pl.semaphore_wait(barrier, partners)
        repeat(near, lambda gy: send_part(0, gy))
        send_part(0, ny - 1)
        repeat(ny, lambda gy: send_part(hub_column, gy))
        pl.when(seam_east)(
            lambda: pl.semaphore_signal(ready, inc=1, device_id={"gx": east}, device_id_type=MESH)
        )

    early = seam_west & (my < near)
    pack_first = (mx > 0) & (my < near)
    pl.when(my >= near)(meet)

    depth = (sea * lay_v[...]).astype(jnp.float32)
    depth_v[...] = depth

    half = h // 2
    depth_at = 6 * nk
    lane = lax.broadcasted_iota(jnp.int32, (h, w), 1)
    row = lax.broadcasted_iota(jnp.int32, (h, w), 0)
    slot = jnp.where(row < half, lane, lane - 1)
    pair = slot >> 1
    eastern = (slot & 1) == 0
    even_half = (lane[:half] & 1) == 0

    quarter = h // 4

    def cells(ref, k, b):
        return [
            ref[pl.ds(k * h + side * half + b * quarter, quarter), :] for side in (0, 1)
        ]

    def pack(packed, b, ref, first, count):
        for k in range(count):
            j = first + k
            packed = [
                jnp.where(
                    pair[side * half : side * half + quarter] == j,
                    pltpu.roll(plane, 2 * j + 1 + side, 1),
                    old,
                )
                for side, (plane, old) in enumerate(zip(cells(ref, k, b), packed))
            ]
        return packed

    empty = [jnp.zeros((quarter, w), jnp.float32)] * 2
    packed = [pack(empty, b, depth_v, 3 * nk, 1) for b in (0, 1)]
    for i, ref in enumerate((t_v, s_v)):
        loads[5 + i].wait()
        packed = [pack(packed[b], b, ref, i * nk, nk) for b in (0, 1)]
    loads[7].wait()

    def finish(b):
        upper, lower = pack(packed[b], b, uv_v, 2 * nk, nk)
        pack_v[pl.ds(b * quarter, quarter), :] = upper
        pack_v[pl.ds(half + b * quarter, quarter), :] = lower
        at = pl.ds(b * quarter, quarter)
        last_v[at, :] = jnp.where(even_half[:quarter], upper, lower)
        first_v[at, :] = jnp.where(even_half[:quarter], lower, upper)

    def strip(b, src, dst, step):
        at = pl.ds(b * quarter, quarter)
        return pltpu.make_async_remote_copy(
            src_ref=src.at[at], dst_ref=dst.at[at],
            send_sem=side_send, recv_sem=pack_recv,
            device_id={"gx": lax.rem(mx + step, nx)}, device_id_type=MESH,
        )

    to_east = [strip(b, last_v, west_v, 1) for b in (0, 1)]
    to_west = [strip(b, first_v, east_v, nx - 1) for b in (0, 1)]

    for b in (0, 1):
        finish(b)
    pl.when(pack_first)(meet)

    @pl.when(jnp.logical_not(early))
    def _():
        for b in (0, 1):
            to_east[b].start()

    depth_east_v[...] = jnp.where(
        lane == w - 1, 0.0, jnp.minimum(depth, pltpu.roll(depth, w - 1, 1))
    )
    depth_north_v[...] = jnp.where(
        row == h - 1, 0.0, jnp.minimum(depth, pltpu.roll(depth, h - 1, 0))
    )

    def interior(block, carry):
        start = pl.multiple_of(block * block_rows, block_rows)
        here = pl.ds(start, block_rows)
        deep_east, deep_north = depth_east_v[here, :], depth_north_v[here, :]
        deep, gain = depth_v[here, :], g_v[here, :]
        came = [0.0, 0.0]
        for k in range(nk):
            at = pl.ds(start + k * h, block_rows)
            east_near, east_far = face_weights(uv_v[at, :], deep_east > k)
            north_near, north_far = face_weights(
                uv_v[pl.ds(start + (nk + k) * h, block_rows), :], deep_north > k
            )
            mix = jnp.where(deep > k + 1, time_step * vertical_mixing, 0.0)
            for n, (ref, out) in enumerate(((t_v, t_out), (s_v, s_out))):
                c = ref[at, :]
                east = east_near * c + east_far * pltpu.roll(c, w - 1, 1)
                north = north_near * c + north_far * ref[pl.ds(start + k * h + 1, block_rows), :]
                strip_at = (n * nk + k) * (h + 8) + 8
                flux_v[pl.ds(start + strip_at, block_rows), :] = north
                south = flux_v[pl.ds(start + strip_at - 1, block_rows), :]
                flow = (pltpu.roll(east, 1, 1) - east) + (south - north)
                fall = 0.0
                if k < nk - 1:
                    fall = mix * (c - ref[pl.ds(start + (k + 1) * h, block_rows), :])
                out[at, :] = c + (gain * flow + (came[n] - fall))
                came[n] = fall
        return carry

    split = jnp.where(early, h // block_rows, 0)

    @pl.when(early)
    def _():
        late_loads.wait()

    lax.fori_loop(0, split, interior, 0)
    pl.when(early)(meet)

    @pl.when(early)
    def _():
        for b in (0, 1):
            to_east[b].start()

    @pl.when(jnp.logical_not(seam_west))
    def _():
        for b in (0, 1):
            to_west[b].start()

    @pl.when(jnp.logical_not(early))
    def _():
        late_loads.wait()


    def rows(ref, row, base=0):
        return ref[pl.ds(base + row, nk, stride=h), :]

    up_v[pl.ds(0, nk), :] = rows(t_v, h - 1)
    up_v[pl.ds(nk, nk), :] = rows(s_v, h - 1)
    up_v[pl.ds(2 * nk, nk), :] = rows(uv_v, h - 1, nk * h)
    up_v[pl.ds(3 * nk, 8), :] = jnp.broadcast_to(depth[h - 1 : h, :], (8, w))
    down_v[pl.ds(0, nk), :] = rows(t_v, 0)
    down_v[pl.ds(nk, nk), :] = rows(s_v, 0)
    down_v[pl.ds(2 * nk, 8), :] = jnp.broadcast_to(depth[0:1, :], (8, w))

    @pl.when(is_top)
    def _():
        up = up_v[...]
        flip = (w - 1) - lax.broadcasted_iota(jnp.int32, up.shape, 1)
        fold_v[mx] = jnp.take_along_axis(up, flip, axis=1)

    to_north = pltpu.make_async_remote_copy(
        src_ref=up_v, dst_ref=south_v, send_sem=side_send, recv_sem=row_recv,
        device_id={"gy": lax.rem(my + 1, ny)}, device_id_type=MESH,
    )
    to_south = pltpu.make_async_remote_copy(
        src_ref=down_v, dst_ref=north_v, send_sem=side_send, recv_sem=row_recv,
        device_id={"gy": lax.rem(my + ny - 1, ny)}, device_id_type=MESH,
    )

    def fold_copy(d):
        return pltpu.make_async_remote_copy(
            src_ref=fold_v.at[mx], dst_ref=fold_v.at[mx],
            send_sem=part_send, recv_sem=row_recv,
            device_id={"gx": lax.rem(mx + d + 1, nx)}, device_id_type=MESH,
        )


    @pl.when(jnp.logical_not(is_top))
    def _():
        to_north.start()

    @pl.when(my > 0)
    def _():
        to_south.start()

    @pl.when(is_top)
    def _():
        repeat(nx - 1, lambda d: fold_copy(d).start())

    lax.fori_loop(split, h // block_rows, interior, 0)

    level_row = lax.broadcasted_iota(jnp.int32, (nk, w), 0).astype(jnp.float32)

    def north_edge(far_t, far_s, speed, far_depth):
        near_weight, far_weight = face_weights(
            speed, jnp.minimum(up_v[3 * nk : 3 * nk + 1, :], far_depth) > level_row
        )
        for near, far, out in (
            (up_v[pl.ds(0, nk), :], far_t, t_out),
            (up_v[pl.ds(nk, nk), :], far_s, s_out),
        ):
            at = pl.ds(h - 1, nk, stride=h)
            out[at, :] -= g_v[h - 1 : h, :] * (near_weight * near + far_weight * far)

    @pl.when(seam_west)
    def _():
        pl.semaphore_wait(ready, 1)
        for b in (0, 1):
            to_west[b].start()

    def south_edge():
        near_weight, far_weight = face_weights(
            south_v[pl.ds(2 * nk, nk), :],
            jnp.minimum(down_v[2 * nk : 2 * nk + 1, :], south_v[3 * nk : 3 * nk + 1, :]) > level_row,
        )
        for i, out in enumerate((t_out, s_out)):
            at = pl.ds(0, nk, stride=h)
            out[at, :] += g_v[0:1, :] * (
                near_weight * south_v[pl.ds(i * nk, nk), :]
                + far_weight * down_v[pl.ds(i * nk, nk), :]
            )

    came(has_north & has_south, edge_rows + down_rows, row_recv)
    came(has_north & jnp.logical_not(has_south), down_rows, row_recv)

    @pl.when(has_north)
    def _():
        north_edge(
            north_v[pl.ds(0, nk), :],
            north_v[pl.ds(nk, nk), :],
            up_v[pl.ds(2 * nk, nk), :],
            north_v[2 * nk : 2 * nk + 1, :],
        )

    pl.when(has_north & has_south)(south_edge)

    def column(plane, at):
        return jnp.broadcast_to(plane[:, at : at + 1], (h, w))

    mine = pack_v[...]
    depth = depth_v[...]
    gain = g_v[...]
    level_of = (pair & (nk - 1)).astype(jnp.float32)
    open_cell = jnp.where(eastern, column(depth, w - 1), column(depth, 0)) > level_of
    edge_gain = jnp.where(eastern, -column(gain, w - 1), column(gain, 0))
    surface_wet = jnp.where(depth > 0.0, time_step / top_thickness, 0.0)
    surface = s0_v[...]
    s_out[pl.ds(0, h), :] -= surface_wet * surface * rain_v[...]
    for i, plane in enumerate(
        (
            mine,
            jnp.where(pair < nk, pltpu.roll(mine, w - 4 * nk, 1), pltpu.roll(mine, w - 2 * nk, 1)),
            jnp.where(open_cell, edge_gain, 0.0),
            surface_wet * surface,
            surface_wet,
        )
    ):
        side_out[pl.ds(i * h, h), :] = plane

    @pl.when(is_hub)
    def _():
        bytes_of(peers, side_send, part_recv).wait_recv()
        total_v[...] = jnp.sum(parts_v[...], axis=0)

    in_column = mx == hub_column
    seam_giver = seam_west & is_top

    @pl.when(in_column)
    def _():
        repeat(nx - 2, lambda d: hand_on(hub_column + 1 + d, my).start())

    @pl.when(seam_giver)
    def _():
        repeat(ny - 1 - near, lambda d: hand_on(0, near + d).start())

    @pl.when(is_top)
    def _():
        bytes_of(nx * edge_rows, side_send, row_recv).wait_recv()
        south_edge()
        partner = fold_v[seam_smem[0] // w]
        north_edge(
            partner[:nk],
            partner[nk : 2 * nk],
            0.5 * (up_v[pl.ds(2 * nk, nk), :] - partner[2 * nk : 3 * nk]),
            partner[3 * nk : 3 * nk + 1],
        )

    own_row = jnp.logical_not(is_top)
    fold_rows = (nx - 1) * edge_rows
    sent(plain & own_row, hubs, part_send)
    sent(plain & is_top, hubs + fold_rows, part_send)
    sent(in_column & own_row, hubs - 1 + nx - 2, part_send)
    sent(in_column & is_top, hubs - 1 + nx - 2 + fold_rows, part_send)
    sent(seam_west & (my < near), hubs - 1, part_send)
    sent(seam_giver, hubs - 1 + ny - 1 - near + fold_rows, part_send)
    sent(has_north & has_south, h + edge_rows + down_rows, side_send)
    sent(jnp.logical_not(has_south), h + edge_rows, side_send)
    sent(is_top, h + down_rows, side_send)
    pl.when(plain)(lambda: hand_on(0, 0).wait_recv())
    side_out[pl.ds(6 * h, 8), :] = jnp.broadcast_to(total_v[...], (8, w))
    bytes_of(h, side_send, pack_recv).wait_recv()
    side_out[pl.ds(5 * h, half), :] = west_v[...]
    side_out[pl.ds(5 * h + half, half), :] = east_v[...]


store_cuts = 16


def store_kernel(nk, h, w, t_ref, s_ref, side_ref, t_hbm, s_hbm, t_v, s_v, sem):
    half = h // 2
    mine, own_speed, edge_gain, surface, surface_wet = (
        side_ref[pl.ds(i * h, h), :] for i in range(5)
    )
    west = side_ref[pl.ds(5 * h, half), :]
    east = side_ref[pl.ds(5 * h + half, half), :]
    totals = side_ref[pl.ds(6 * h, 1), :]

    lane = lax.broadcasted_iota(jnp.int32, (h, w), 1)
    slot = jnp.where(lax.broadcasted_iota(jnp.int32, (h, w), 0) < half, lane, lane - 1)
    pair = slot >> 1
    eastern = (slot & 1) == 0

    def both(cells):
        return jnp.concatenate([cells, cells], axis=0)

    def moved(cells, by):
        return both(pltpu.roll(cells, by % w, 1))

    def columns(cells, at):
        return jnp.concatenate(
            [jnp.broadcast_to(cells[:, i : i + 1], (half, w)) for i in (at, at + 1)], axis=0
        )

    near = jnp.where(eastern, mine, moved(west, 1))
    far = jnp.where(eastern, moved(east, -1), mine)
    west_speed = jnp.where(pair < nk, moved(west, 1 - 4 * nk), moved(west, 1 - 2 * nk))
    far_depth = jnp.where(eastern, columns(east, 6 * nk + 1), columns(west, 6 * nk))
    near_weight, far_weight = face_weights(
        jnp.where(eastern, own_speed, west_speed),
        far_depth > (pair & (nk - 1)).astype(jnp.float32),
    )
    edge = edge_gain * (near_weight * near + far_weight * far)

    total_area, total_fresh, salt_fresh, salt_only = (
        jnp.broadcast_to(totals[:, i : i + 1], (1, w)) for i in range(4)
    )
    mean_fresh = total_fresh / total_area
    lift = (salt_fresh - mean_fresh * salt_only) / total_area
    virtual = surface_wet * lift + surface * mean_fresh

    at_edge = (lane[:half] == 0) | (lane[:half] == w - 1)
    step = nk // store_cuts
    for i, (ref, out, hbm) in enumerate(((t_ref, t_v, t_hbm), (s_ref, s_v, s_hbm))):
        for cut in reversed(range(store_cuts)):
            for k in range(cut * step, (cut + 1) * step):
                j = i * nk + k
                for part, shift in ((0, w - 1 - 2 * j), (1, w - 2 - 2 * j)):
                    rows = slice(part * half, (part + 1) * half)
                    change = jnp.where(at_edge, pltpu.roll(edge[rows], shift % w, 1), 0.0)
                    if j == nk:
                        change = change + virtual[rows]
                    at = pl.ds(k * h + part * half, half)
                    out[at, :] = ref[at, :] + change
            at = pl.ds(cut * step * h, step * h)
            pltpu.make_async_copy(out.at[at], hbm.at[at], sem).start()
    for out, hbm in ((t_v, t_hbm), (s_v, s_hbm)):
        pltpu.make_async_copy(out, hbm, sem).wait()


def shards(nx, ny, t, s, uv, sea, layers, area, rain, seam):
    nk, h, w = t.shape
    assert w == 128 and h % 16 == 0 and nk & (nk - 1) == 0 and nk % 8 == 0 and 6 * nk + 3 <= w and nx > 3 and ny > 3
    f32 = jnp.float32
    peers = nx * ny - 1
    half_plane = pltpu.VMEM((h // 2, w), f32)
    vmem = 67043328 - 4 * w * (2 * nk * h + 6 * h + 8)
    any_space = pl.BlockSpec(memory_space=pl.ANY)
    dma = pltpu.SemaphoreType.DMA
    plane = pltpu.VMEM((h, w), f32)
    t_next, s_next, side = pl.pallas_call(
        functools.partial(kernel, nx, ny, nk, h, w),
        out_shape=[pltpu.VMEM((nk * h, w), f32)] * 2 + [pltpu.VMEM((6 * h + 8, w), f32)],
        in_specs=[any_space] * 8,
        out_specs=[pl.BlockSpec(memory_space=pltpu.VMEM)] * 3,
        scratch_shapes=[
            pltpu.VMEM((nk * h + 8, w), f32),
            pltpu.VMEM((nk * h + 8, w), f32),
            pltpu.VMEM((2 * nk * h, w), f32),
            pltpu.VMEM((h, w), jnp.int32),
            pltpu.VMEM((h, w), jnp.int32),
            plane, plane, plane, plane, plane,
            plane, half_plane, half_plane, half_plane, half_plane,
            pltpu.VMEM((3 * nk + 8, w), f32),
            pltpu.VMEM((2 * nk + 8, w), f32),
            pltpu.VMEM((3 * nk + 8, w), f32),
            pltpu.VMEM((2 * nk + 8, w), f32),
            pltpu.VMEM((nx, 3 * nk + 8, w), f32),
            pltpu.VMEM((1, w), f32),
            pltpu.VMEM((nx * ny, 1, w), f32),
            pltpu.VMEM((1, w), f32),
            pltpu.SMEM((w,), jnp.int32),
            plane, plane,
            pltpu.VMEM((max(2 * nk * (h + 8), (nx + 2) * (3 * nk + 8)), w), f32),
            dma((5,)), dma, dma, dma, dma, dma, pltpu.SemaphoreType.REGULAR,
        ],
        compiler_params=pltpu.CompilerParams(
            collective_id=0, has_side_effects=True, vmem_limit_bytes=vmem
        ),
        name="tracer_step",
    )(
        t.reshape(nk * h, w), s.reshape(nk * h, w), uv.reshape(2 * nk * h, w),
        sea, layers, area, rain, seam,
    )
    t_next, s_next = pl.pallas_call(
        functools.partial(store_kernel, nk, h, w),
        out_shape=[jax.ShapeDtypeStruct((nk * h, w), f32)] * 2,
        in_specs=[pl.BlockSpec(memory_space=pltpu.VMEM)] * 3,
        out_specs=[any_space] * 2,
        scratch_shapes=[pltpu.VMEM((nk * h, w), f32)] * 2 + [dma],
        compiler_params=pltpu.CompilerParams(vmem_limit_bytes=8 << 20),
        name="store",
    )(t_next, s_next, side)
    return t_next.reshape(t.shape), s_next.reshape(s.shape)


def solution(mesh):
    in_specs = (
        P("groups", "gy", "gx"),
        P("groups", "gy", "gx"),
        P("groups", None, "gy", "gx"),
        P("gy", "gx"),
        P("gy", "gx"),
        P("gy", "gx"),
        P("gy", "gx"),
        P("gx"),
    )
    out_specs = (P("groups", "gy", "gx"), P("groups", "gy", "gx"))
    return jax.shard_map(
        functools.partial(shards, mesh.shape["gx"], mesh.shape["gy"]),
        mesh=mesh, in_specs=in_specs, out_specs=out_specs, check_vma=False,
    )
```

```python
import functools

import jax
import jax.numpy as jnp
from jax import lax
from jax.experimental import pallas as pl
from jax.experimental.pallas import tpu as pltpu
from jax.sharding import PartitionSpec as P

time_step = 0.25
diffusivity = 0.5
vertical_mixing = 0.3
top_thickness = 0.5

block_rows = 16
hub_column = 1

MESH = pl.DeviceIdType.MESH


def repeat(count, body):
    if count <= 16:
        for i in range(count):
            body(i)
    else:
        pl.loop(0, count)(body)


def face_weights(speed, open_face):
    near_weight = jnp.maximum(speed, 0.0) + diffusivity
    far_weight = speed - near_weight
    return jnp.where(open_face, near_weight, 0.0), jnp.where(open_face, far_weight, 0.0)


def kernel(
    nx, ny, nk, h, w,
    t_hbm, s_hbm, uv_hbm, sea_hbm, lay_hbm, area_hbm, rain_hbm, seam_hbm,
    t_out, s_out, side_out,
    t_v, s_v, uv_v, sea_v, lay_v, area_v, rain_v, s0_v, g_v, depth_v,
    pack_v, last_v, first_v, east_v, west_v, up_v, down_v, south_v, north_v, fold_v,
    part_v, parts_v, total_v, seam_smem, depth_east_v, depth_north_v, flux_v,
    load_sems, side_send, pack_recv, row_recv, part_send, part_recv, ready,
):
    mx, my = lax.axis_index("gx"), lax.axis_index("gy")
    is_top = my == ny - 1
    me = mx * ny + my
    peers = nx * ny - 1

    barrier = pltpu.get_barrier_semaphore()

    east, west = lax.rem(mx + 1, nx), lax.rem(mx + nx - 1, nx)
    near = ny // 2
    hubs = near + 1 + ny

    def hub(gx, gy):
        return (gx == hub_column) | ((gx == 0) & ((gy < near) | (gy == ny - 1)))

    is_hub = hub(mx, my)
    plain = jnp.logical_not(is_hub)
    seam_west = mx == 0
    seam_east = mx == nx - 1
    has_north, has_south = my < ny - 1, my > 0

    def count(flag):
        return jnp.where(flag, 1, 0)

    row_partners = jnp.where(
        is_top,
        nx - 2 - count(mx > hub_column),
        count(jnp.logical_not(hub(east, my)))
        + count(jnp.logical_not(hub(west, my) | seam_west)),
    )
    partners = (
        hubs - count(is_hub) + row_partners
        + count(has_north & jnp.logical_not(hub(mx, my + 1)))
        + count(has_south & jnp.logical_not(hub(mx, my - 1)))
    )

    def signal(gx, gy):
        pl.semaphore_signal(
            barrier, inc=1, device_id={"gx": gx, "gy": gy}, device_id_type=MESH
        )

    def greet():
        @pl.when(is_hub)
        def _():
            def one(r):
                gx, gy = nx - 1 - r // ny, r % ny
                pl.when(gx * ny + gy != me)(lambda: signal(gx, gy))

            repeat(nx * ny, one)

        @pl.when(plain & is_top)
        def _():
            repeat(nx - 1, lambda d: signal(lax.rem(mx + 1 + d, nx), my))

        @pl.when(plain & has_north)
        def _():
            signal(west, my)
            pl.when(jnp.logical_not(seam_east))(lambda: signal(east, my))
            signal(mx, my + 1)

        @pl.when(plain & has_south)
        def _():
            signal(mx, my - 1)

    loads = [
        pltpu.make_async_copy(src, dst, load_sems.at[min(max(i - 4, 0), 4)])
        for i, (src, dst) in enumerate(
            [
                (area_hbm, area_v),
                (sea_hbm, sea_v),
                (rain_hbm, rain_v),
                (s_hbm.at[pl.ds(0, h)], s0_v),
                (lay_hbm, lay_v),
                (t_hbm, t_v.at[pl.ds(0, nk * h)]),
                (s_hbm, s_v.at[pl.ds(0, nk * h)]),
                (uv_hbm.at[pl.ds(0, nk * h)], uv_v.at[pl.ds(0, nk * h)]),
                (uv_hbm.at[pl.ds(nk * h, nk * h)], uv_v.at[pl.ds(nk * h, nk * h)]),
                (seam_hbm, seam_smem),
            ]
        )
    ]
    for load in loads[:8]:
        load.start()
    greet()
    for load in loads[8:]:
        load.start()
    zeros = jnp.zeros((8, w), jnp.float32)
    for ref in (t_v, s_v):
        ref[pl.ds(nk * h, 8), :] = zeros
    for i in range(2 * nk):
        flux_v[pl.ds(i * (h + 8), 8), :] = zeros

    rest = pl.ds(0, nk * h + 1)
    late_loads = pltpu.make_async_copy(uv_hbm.at[rest], t_v.at[rest], load_sems.at[4])
    small = pl.ds(0, 5 * h)
    pltpu.make_async_copy(t_hbm.at[small], t_v.at[small], load_sems.at[0]).wait()
    area = area_v[...]
    sea = sea_v[...]
    wet_area = area * sea.astype(jnp.float32)
    surface = s0_v[...]
    fresh = wet_area * rain_v[...]
    lane1 = lax.broadcasted_iota(jnp.int32, (1, w), 1)
    part = jnp.zeros((1, w), jnp.float32)
    for i, term in enumerate((wet_area, fresh, fresh * surface, wet_area * surface)):
        rows8 = jnp.sum(term.reshape(h // 8, 8, w), axis=0)
        part = jnp.where(
            lane1 == i, jnp.sum(jnp.sum(rows8, axis=1, keepdims=True), axis=0, keepdims=True), part
        )
    part_v[...] = part
    gain = time_step / area
    g_v[...] = gain

    parts_v[me] = part

    def send_part(gx, gy):
        @pl.when(gx * ny + gy != me)
        def _():
            pltpu.make_async_remote_copy(
                src_ref=part_v, dst_ref=parts_v.at[me], send_sem=part_send, recv_sem=part_recv,
                device_id={"gx": gx, "gy": gy}, device_id_type=MESH,
            ).start()

    edge_rows = 3 * nk + 8
    down_rows = 2 * nk + 8

    def bytes_of(n, sends, arrivals):
        block = flux_v.at[pl.ds(0, n)]
        return pltpu.make_async_remote_copy(
            src_ref=block, dst_ref=block, send_sem=sends, recv_sem=arrivals,
            device_id={"gx": east}, device_id_type=MESH,
        )

    def sent(flag, n, sends):
        pl.when(flag)(lambda: bytes_of(n, sends, pack_recv).wait_send())

    def came(flag, n, arrivals):
        pl.when(flag)(lambda: bytes_of(n, side_send, arrivals).wait_recv())

    def hand_on(gx, gy):
        return pltpu.make_async_remote_copy(
            src_ref=total_v, dst_ref=total_v, send_sem=part_send, recv_sem=part_recv,
            device_id={"gx": gx, "gy": gy}, device_id_type=MESH,
        )

    def meet():
        pl.semaphore_wait(barrier, partners)
        repeat(near, lambda gy: send_part(0, gy))
        send_part(0, ny - 1)
        repeat(ny, lambda gy: send_part(hub_column, gy))
        pl.when(seam_east)(
            lambda: pl.semaphore_signal(ready, inc=1, device_id={"gx": east}, device_id_type=MESH)
        )

    early = seam_west & (my < near)
    pack_first = (mx > 0) & (my < near)
    pl.when(my >= near)(meet)

    depth = (sea * lay_v[...]).astype(jnp.float32)
    depth_v[...] = depth

    half = h // 2
    depth_at = 6 * nk
    lane = lax.broadcasted_iota(jnp.int32, (h, w), 1)
    row = lax.broadcasted_iota(jnp.int32, (h, w), 0)
    slot = jnp.where(row < half, lane, lane - 1)
    pair = slot >> 1
    eastern = (slot & 1) == 0
    even_half = (lane[:half] & 1) == 0

    quarter = h // 4

    def cells(ref, k, b):
        return [
            ref[pl.ds(k * h + side * half + b * quarter, quarter), :] for side in (0, 1)
        ]

    def pack(packed, b, ref, first, count):
        for k in range(count):
            j = first + k
            packed = [
                jnp.where(
                    pair[side * half : side * half + quarter] == j,
                    pltpu.roll(plane, 2 * j + 1 + side, 1),
                    old,
                )
                for side, (plane, old) in enumerate(zip(cells(ref, k, b), packed))
            ]
        return packed

    empty = [jnp.zeros((quarter, w), jnp.float32)] * 2
    packed = [pack(empty, b, depth_v, 3 * nk, 1) for b in (0, 1)]
    for i, ref in enumerate((t_v, s_v)):
        loads[5 + i].wait()
        packed = [pack(packed[b], b, ref, i * nk, nk) for b in (0, 1)]
    loads[7].wait()

    def finish(b):
        upper, lower = pack(packed[b], b, uv_v, 2 * nk, nk)
        pack_v[pl.ds(b * quarter, quarter), :] = upper
        pack_v[pl.ds(half + b * quarter, quarter), :] = lower
        at = pl.ds(b * quarter, quarter)
        last_v[at, :] = jnp.where(even_half[:quarter], upper, lower)
        first_v[at, :] = jnp.where(even_half[:quarter], lower, upper)

    def strip(b, src, dst, step):
        at = pl.ds(b * quarter, quarter)
        return pltpu.make_async_remote_copy(
            src_ref=src.at[at], dst_ref=dst.at[at],
            send_sem=side_send, recv_sem=pack_recv,
            device_id={"gx": lax.rem(mx + step, nx)}, device_id_type=MESH,
        )

    to_east = [strip(b, last_v, west_v, 1) for b in (0, 1)]
    to_west = [strip(b, first_v, east_v, nx - 1) for b in (0, 1)]

    for b in (0, 1):
        finish(b)
    pl.when(pack_first)(meet)

    @pl.when(jnp.logical_not(early))
    def _():
        for b in (0, 1):
            to_east[b].start()

    depth_east_v[...] = jnp.where(
        lane == w - 1, 0.0, jnp.minimum(depth, pltpu.roll(depth, w - 1, 1))
    )
    depth_north_v[...] = jnp.where(
        row == h - 1, 0.0, jnp.minimum(depth, pltpu.roll(depth, h - 1, 0))
    )

    def interior(block, carry):
        start = pl.multiple_of(block * block_rows, block_rows)
        here = pl.ds(start, block_rows)
        deep_east, deep_north = depth_east_v[here, :], depth_north_v[here, :]
        deep, gain = depth_v[here, :], g_v[here, :]
        came = [0.0, 0.0]
        for k in range(nk):
            at = pl.ds(start + k * h, block_rows)
            east_near, east_far = face_weights(uv_v[at, :], deep_east > k)
            north_near, north_far = face_weights(
                uv_v[pl.ds(start + (nk + k) * h, block_rows), :], deep_north > k
            )
            mix = jnp.where(deep > k + 1, time_step * vertical_mixing, 0.0)
            for n, (ref, out) in enumerate(((t_v, t_out), (s_v, s_out))):
                c = ref[at, :]
                east = east_near * c + east_far * pltpu.roll(c, w - 1, 1)
                north = north_near * c + north_far * ref[pl.ds(start + k * h + 1, block_rows), :]
                strip_at = (n * nk + k) * (h + 8) + 8
                flux_v[pl.ds(start + strip_at, block_rows), :] = north
                south = flux_v[pl.ds(start + strip_at - 1, block_rows), :]
                flow = (pltpu.roll(east, 1, 1) - east) + (south - north)
                fall = 0.0
                if k < nk - 1:
                    fall = mix * (c - ref[pl.ds(start + (k + 1) * h, block_rows), :])
                out[at, :] = c + (gain * flow + (came[n] - fall))
                came[n] = fall
        return carry

    split = jnp.where(early, h // block_rows, 0)

    @pl.when(early)
    def _():
        late_loads.wait()

    lax.fori_loop(0, split, interior, 0)
    pl.when(early)(meet)

    @pl.when(early)
    def _():
        for b in (0, 1):
            to_east[b].start()

    @pl.when(jnp.logical_not(seam_west))
    def _():
        for b in (0, 1):
            to_west[b].start()

    @pl.when(jnp.logical_not(early))
    def _():
        late_loads.wait()


    def rows(ref, row, base=0):
        return ref[pl.ds(base + row, nk, stride=h), :]

    up_v[pl.ds(0, nk), :] = rows(t_v, h - 1)
    up_v[pl.ds(nk, nk), :] = rows(s_v, h - 1)
    up_v[pl.ds(2 * nk, nk), :] = rows(uv_v, h - 1, nk * h)
    up_v[pl.ds(3 * nk, 8), :] = jnp.broadcast_to(depth[h - 1 : h, :], (8, w))
    down_v[pl.ds(0, nk), :] = rows(t_v, 0)
    down_v[pl.ds(nk, nk), :] = rows(s_v, 0)
    down_v[pl.ds(2 * nk, 8), :] = jnp.broadcast_to(depth[0:1, :], (8, w))

    @pl.when(is_top)
    def _():
        up = up_v[...]
        flip = (w - 1) - lax.broadcasted_iota(jnp.int32, up.shape, 1)
        fold_v[mx] = jnp.take_along_axis(up, flip, axis=1)

    to_north = pltpu.make_async_remote_copy(
        src_ref=up_v, dst_ref=south_v, send_sem=side_send, recv_sem=row_recv,
        device_id={"gy": lax.rem(my + 1, ny)}, device_id_type=MESH,
    )
    to_south = pltpu.make_async_remote_copy(
        src_ref=down_v, dst_ref=north_v, send_sem=side_send, recv_sem=row_recv,
        device_id={"gy": lax.rem(my + ny - 1, ny)}, device_id_type=MESH,
    )

    def fold_copy(d):
        return pltpu.make_async_remote_copy(
            src_ref=fold_v.at[mx], dst_ref=fold_v.at[mx],
            send_sem=part_send, recv_sem=row_recv,
            device_id={"gx": lax.rem(mx + d + 1, nx)}, device_id_type=MESH,
        )


    @pl.when(jnp.logical_not(is_top))
    def _():
        to_north.start()

    @pl.when(my > 0)
    def _():
        to_south.start()

    @pl.when(is_top)
    def _():
        repeat(nx - 1, lambda d: fold_copy(d).start())

    lax.fori_loop(split, h // block_rows, interior, 0)

    level_row = lax.broadcasted_iota(jnp.int32, (nk, w), 0).astype(jnp.float32)

    def north_edge(far_t, far_s, speed, far_depth):
        near_weight, far_weight = face_weights(
            speed, jnp.minimum(up_v[3 * nk : 3 * nk + 1, :], far_depth) > level_row
        )
        for near, far, out in (
            (up_v[pl.ds(0, nk), :], far_t, t_out),
            (up_v[pl.ds(nk, nk), :], far_s, s_out),
        ):
            at = pl.ds(h - 1, nk, stride=h)
            out[at, :] -= g_v[h - 1 : h, :] * (near_weight * near + far_weight * far)

    @pl.when(seam_west)
    def _():
        pl.semaphore_wait(ready, 1)
        for b in (0, 1):
            to_west[b].start()

    def south_edge():
        near_weight, far_weight = face_weights(
            south_v[pl.ds(2 * nk, nk), :],
            jnp.minimum(down_v[2 * nk : 2 * nk + 1, :], south_v[3 * nk : 3 * nk + 1, :]) > level_row,
        )
        for i, out in enumerate((t_out, s_out)):
            at = pl.ds(0, nk, stride=h)
            out[at, :] += g_v[0:1, :] * (
                near_weight * south_v[pl.ds(i * nk, nk), :]
                + far_weight * down_v[pl.ds(i * nk, nk), :]
            )

    came(has_north & has_south, edge_rows + down_rows, row_recv)
    came(has_north & jnp.logical_not(has_south), down_rows, row_recv)

    @pl.when(has_north)
    def _():
        north_edge(
            north_v[pl.ds(0, nk), :],
            north_v[pl.ds(nk, nk), :],
            up_v[pl.ds(2 * nk, nk), :],
            north_v[2 * nk : 2 * nk + 1, :],
        )

    pl.when(has_north & has_south)(south_edge)

    def column(plane, at):
        return jnp.broadcast_to(plane[:, at : at + 1], (h, w))

    mine = pack_v[...]
    depth = depth_v[...]
    gain = g_v[...]
    level_of = (pair & (nk - 1)).astype(jnp.float32)
    open_cell = jnp.where(eastern, column(depth, w - 1), column(depth, 0)) > level_of
    edge_gain = jnp.where(eastern, -column(gain, w - 1), column(gain, 0))
    surface_wet = jnp.where(depth > 0.0, time_step / top_thickness, 0.0)
    surface = s0_v[...]
    s_out[pl.ds(0, h), :] -= surface_wet * surface * rain_v[...]
    for i, plane in enumerate(
        (
            mine,
            jnp.where(pair < nk, pltpu.roll(mine, w - 4 * nk, 1), pltpu.roll(mine, w - 2 * nk, 1)),
            jnp.where(open_cell, edge_gain, 0.0),
            surface_wet * surface,
            surface_wet,
        )
    ):
        side_out[pl.ds(i * h, h), :] = plane

    @pl.when(is_hub)
    def _():
        bytes_of(peers, side_send, part_recv).wait_recv()
        total_v[...] = jnp.sum(parts_v[...], axis=0)

    in_column = mx == hub_column
    seam_giver = seam_west & is_top

    @pl.when(in_column)
    def _():
        repeat(nx - 2, lambda d: hand_on(hub_column + 1 + d, my).start())

    @pl.when(seam_giver)
    def _():
        repeat(ny - 1 - near, lambda d: hand_on(0, near + d).start())

    @pl.when(is_top)
    def _():
        bytes_of(nx * edge_rows, side_send, row_recv).wait_recv()
        south_edge()
        partner = fold_v[seam_smem[0] // w]
        north_edge(
            partner[:nk],
            partner[nk : 2 * nk],
            0.5 * (up_v[pl.ds(2 * nk, nk), :] - partner[2 * nk : 3 * nk]),
            partner[3 * nk : 3 * nk + 1],
        )

    own_row = jnp.logical_not(is_top)
    fold_rows = (nx - 1) * edge_rows
    sent(plain & own_row, hubs, part_send)
    sent(plain & is_top, hubs + fold_rows, part_send)
    sent(in_column & own_row, hubs - 1 + nx - 2, part_send)
    sent(in_column & is_top, hubs - 1 + nx - 2 + fold_rows, part_send)
    sent(seam_west & (my < near), hubs - 1, part_send)
    sent(seam_giver, hubs - 1 + ny - 1 - near + fold_rows, part_send)
    sent(has_north & has_south, h + edge_rows + down_rows, side_send)
    sent(jnp.logical_not(has_south), h + edge_rows, side_send)
    sent(is_top, h + down_rows, side_send)
    pl.when(plain)(lambda: hand_on(0, 0).wait_recv())
    side_out[pl.ds(6 * h, 8), :] = jnp.broadcast_to(total_v[...], (8, w))
    bytes_of(h, side_send, pack_recv).wait_recv()
    side_out[pl.ds(5 * h, half), :] = west_v[...]
    side_out[pl.ds(5 * h + half, half), :] = east_v[...]


store_cuts = 16


def store_kernel(nk, h, w, t_ref, s_ref, side_ref, t_hbm, s_hbm, t_v, s_v, sem):
    half = h // 2
    mine, own_speed, edge_gain, surface, surface_wet = (
        side_ref[pl.ds(i * h, h), :] for i in range(5)
    )
    west = side_ref[pl.ds(5 * h, half), :]
    east = side_ref[pl.ds(5 * h + half, half), :]
    totals = side_ref[pl.ds(6 * h, 1), :]

    lane = lax.broadcasted_iota(jnp.int32, (h, w), 1)
    slot = jnp.where(lax.broadcasted_iota(jnp.int32, (h, w), 0) < half, lane, lane - 1)
    pair = slot >> 1
    eastern = (slot & 1) == 0

    def both(cells):
        return jnp.concatenate([cells, cells], axis=0)

    def moved(cells, by):
        return both(pltpu.roll(cells, by % w, 1))

    def columns(cells, at):
        return jnp.concatenate(
            [jnp.broadcast_to(cells[:, i : i + 1], (half, w)) for i in (at, at + 1)], axis=0
        )

    near = jnp.where(eastern, mine, moved(west, 1))
    far = jnp.where(eastern, moved(east, -1), mine)
    west_speed = jnp.where(pair < nk, moved(west, 1 - 4 * nk), moved(west, 1 - 2 * nk))
    far_depth = jnp.where(eastern, columns(east, 6 * nk + 1), columns(west, 6 * nk))
    near_weight, far_weight = face_weights(
        jnp.where(eastern, own_speed, west_speed),
        far_depth > (pair & (nk - 1)).astype(jnp.float32),
    )
    edge = edge_gain * (near_weight * near + far_weight * far)

    total_area, total_fresh, salt_fresh, salt_only = (
        jnp.broadcast_to(totals[:, i : i + 1], (1, w)) for i in range(4)
    )
    mean_fresh = total_fresh / total_area
    lift = (salt_fresh - mean_fresh * salt_only) / total_area
    virtual = surface_wet * lift + surface * mean_fresh

    at_edge = (lane[:half] == 0) | (lane[:half] == w - 1)
    step = nk // store_cuts
    for i, (ref, out, hbm) in enumerate(((t_ref, t_v, t_hbm), (s_ref, s_v, s_hbm))):
        for cut in reversed(range(store_cuts)):
            for k in range(cut * step, (cut + 1) * step):
                j = i * nk + k
                for part, shift in ((0, w - 1 - 2 * j), (1, w - 2 - 2 * j)):
                    rows = slice(part * half, (part + 1) * half)
                    change = jnp.where(at_edge, pltpu.roll(edge[rows], shift % w, 1), 0.0)
                    if j == nk:
                        change = change + virtual[rows]
                    at = pl.ds(k * h + part * half, half)
                    out[at, :] = ref[at, :] + change
            at = pl.ds(cut * step * h, step * h)
            pltpu.make_async_copy(out.at[at], hbm.at[at], sem).start()
    for out, hbm in ((t_v, t_hbm), (s_v, s_hbm)):
        pltpu.make_async_copy(out, hbm, sem).wait()


def shards(nx, ny, t, s, uv, sea, layers, area, rain, seam):
    nk, h, w = t.shape
    assert w == 128 and h % 16 == 0 and nk & (nk - 1) == 0 and nk % 8 == 0 and 6 * nk + 3 <= w and nx > 3 and ny > 3
    f32 = jnp.float32
    peers = nx * ny - 1
    half_plane = pltpu.VMEM((h // 2, w), f32)
    vmem = 67043328 - 4 * w * (2 * nk * h + 6 * h + 8)
    any_space = pl.BlockSpec(memory_space=pl.ANY)
    dma = pltpu.SemaphoreType.DMA
    plane = pltpu.VMEM((h, w), f32)
    t_next, s_next, side = pl.pallas_call(
        functools.partial(kernel, nx, ny, nk, h, w),
        out_shape=[pltpu.VMEM((nk * h, w), f32)] * 2 + [pltpu.VMEM((6 * h + 8, w), f32)],
        in_specs=[any_space] * 8,
        out_specs=[pl.BlockSpec(memory_space=pltpu.VMEM)] * 3,
        scratch_shapes=[
            pltpu.VMEM((nk * h + 8, w), f32),
            pltpu.VMEM((nk * h + 8, w), f32),
            pltpu.VMEM((2 * nk * h, w), f32),
            pltpu.VMEM((h, w), jnp.int32),
            pltpu.VMEM((h, w), jnp.int32),
            plane, plane, plane, plane, plane,
            plane, half_plane, half_plane, half_plane, half_plane,
            pltpu.VMEM((3 * nk + 8, w), f32),
            pltpu.VMEM((2 * nk + 8, w), f32),
            pltpu.VMEM((3 * nk + 8, w), f32),
            pltpu.VMEM((2 * nk + 8, w), f32),
            pltpu.VMEM((nx, 3 * nk + 8, w), f32),
            pltpu.VMEM((1, w), f32),
            pltpu.VMEM((nx * ny, 1, w), f32),
            pltpu.VMEM((1, w), f32),
            pltpu.SMEM((w,), jnp.int32),
            plane, plane,
            pltpu.VMEM((max(2 * nk * (h + 8), (nx + 2) * (3 * nk + 8)), w), f32),
            dma((5,)), dma, dma, dma, dma, dma, pltpu.SemaphoreType.REGULAR,
        ],
        compiler_params=pltpu.CompilerParams(
            collective_id=0, has_side_effects=True, vmem_limit_bytes=vmem
        ),
        name="tracer_step",
    )(
        t.reshape(nk * h, w), s.reshape(nk * h, w), uv.reshape(2 * nk * h, w),
        sea, layers, area, rain, seam,
    )
    t_next, s_next = pl.pallas_call(
        functools.partial(store_kernel, nk, h, w),
        out_shape=[jax.ShapeDtypeStruct((nk * h, w), f32)] * 2,
        in_specs=[pl.BlockSpec(memory_space=pltpu.VMEM)] * 3,
        out_specs=[any_space] * 2,
        scratch_shapes=[pltpu.VMEM((nk * h, w), f32)] * 2 + [dma],
        compiler_params=pltpu.CompilerParams(vmem_limit_bytes=8 << 20),
        name="store",
    )(t_next, s_next, side)
    return t_next.reshape(t.shape), s_next.reshape(s.shape)


def solution(mesh):
    in_specs = (
        P("groups", "gy", "gx"),
        P("groups", "gy", "gx"),
        P("groups", None, "gy", "gx"),
        P("gy", "gx"),
        P("gy", "gx"),
        P("gy", "gx"),
        P("gy", "gx"),
        P("gx"),
    )
    out_specs = (P("groups", "gy", "gx"), P("groups", "gy", "gx"))
    return jax.shard_map(
        functools.partial(shards, mesh.shape["gx"], mesh.shape["gy"]),
        mesh=mesh, in_specs=in_specs, out_specs=out_specs, check_vma=False,
    )
```

```python
import functools

import jax
import jax.numpy as jnp
from jax import lax
from jax.experimental import pallas as pl
from jax.experimental.pallas import tpu as pltpu
from jax.sharding import PartitionSpec as P

time_step = 0.25
diffusivity = 0.5
vertical_mixing = 0.3
top_thickness = 0.5

block_rows = 16
hub_column = 1

MESH = pl.DeviceIdType.MESH


def repeat(count, body):
    if count <= 16:
        for i in range(count):
            body(i)
    else:
        pl.loop(0, count)(body)


def face_weights(speed, open_face):
    near_weight = jnp.maximum(speed, 0.0) + diffusivity
    far_weight = speed - near_weight
    return jnp.where(open_face, near_weight, 0.0), jnp.where(open_face, far_weight, 0.0)


def kernel(
    nx, ny, nk, h, w,
    t_hbm, s_hbm, uv_hbm, sea_hbm, lay_hbm, area_hbm, rain_hbm, seam_hbm,
    t_out, s_out, side_out,
    t_v, s_v, uv_v, sea_v, lay_v, area_v, rain_v, s0_v, g_v, depth_v,
    pack_v, last_v, first_v, east_v, west_v, up_v, down_v, south_v, north_v, fold_v,
    part_v, parts_v, total_v, seam_smem, depth_east_v, depth_north_v, flux_v,
    load_sems, side_send, pack_recv, row_recv, part_send, part_recv, ready,
):
    mx, my = lax.axis_index("gx"), lax.axis_index("gy")
    is_top = my == ny - 1
    me = mx * ny + my
    peers = nx * ny - 1

    barrier = pltpu.get_barrier_semaphore()

    east, west = lax.rem(mx + 1, nx), lax.rem(mx + nx - 1, nx)
    near = ny // 2
    hubs = near + 1 + ny

    def hub(gx, gy):
        return (gx == hub_column) | ((gx == 0) & ((gy < near) | (gy == ny - 1)))

    is_hub = hub(mx, my)
    plain = jnp.logical_not(is_hub)
    seam_west = mx == 0
    seam_east = mx == nx - 1
    has_north, has_south = my < ny - 1, my > 0

    def count(flag):
        return jnp.where(flag, 1, 0)

    row_partners = jnp.where(
        is_top,
        nx - 2 - count(mx > hub_column),
        count(jnp.logical_not(hub(east, my)))
        + count(jnp.logical_not(hub(west, my) | seam_west)),
    )
    partners = (
        hubs - count(is_hub) + row_partners
        + count(has_north & jnp.logical_not(hub(mx, my + 1)))
        + count(has_south & jnp.logical_not(hub(mx, my - 1)))
    )

    def signal(gx, gy):
        pl.semaphore_signal(
            barrier, inc=1, device_id={"gx": gx, "gy": gy}, device_id_type=MESH
        )

    def greet():
        @pl.when(is_hub)
        def _():
            def one(r):
                gx, gy = nx - 1 - r // ny, r % ny
                pl.when(gx * ny + gy != me)(lambda: signal(gx, gy))

            repeat(nx * ny, one)

        @pl.when(plain & is_top)
        def _():
            repeat(nx - 1, lambda d: signal(lax.rem(mx + 1 + d, nx), my))

        @pl.when(plain & has_north)
        def _():
            signal(west, my)
            pl.when(jnp.logical_not(seam_east))(lambda: signal(east, my))
            signal(mx, my + 1)

        @pl.when(plain & has_south)
        def _():
            signal(mx, my - 1)

    loads = [
        pltpu.make_async_copy(src, dst, load_sems.at[min(max(i - 4, 0), 4)])
        for i, (src, dst) in enumerate(
            [
                (area_hbm, area_v),
                (sea_hbm, sea_v),
                (rain_hbm, rain_v),
                (s_hbm.at[pl.ds(0, h)], s0_v),
                (lay_hbm, lay_v),
                (t_hbm, t_v.at[pl.ds(0, nk * h)]),
                (s_hbm, s_v.at[pl.ds(0, nk * h)]),
                (uv_hbm.at[pl.ds(0, nk * h)], uv_v.at[pl.ds(0, nk * h)]),
                (uv_hbm.at[pl.ds(nk * h, nk * h)], uv_v.at[pl.ds(nk * h, nk * h)]),
                (seam_hbm, seam_smem),
            ]
        )
    ]
    for load in loads[:8]:
        load.start()
    greet()
    for load in loads[8:]:
        load.start()
    zeros = jnp.zeros((8, w), jnp.float32)
    for ref in (t_v, s_v):
        ref[pl.ds(nk * h, 8), :] = zeros
    for i in range(2 * nk):
        flux_v[pl.ds(i * (h + 8), 8), :] = zeros

    rest = pl.ds(0, nk * h + 1)
    late_loads = pltpu.make_async_copy(uv_hbm.at[rest], t_v.at[rest], load_sems.at[4])
    small = pl.ds(0, 5 * h)
    pltpu.make_async_copy(t_hbm.at[small], t_v.at[small], load_sems.at[0]).wait()
    area = area_v[...]
    sea = sea_v[...]
    wet_area = area * sea.astype(jnp.float32)
    surface = s0_v[...]
    fresh = wet_area * rain_v[...]
    lane1 = lax.broadcasted_iota(jnp.int32, (1, w), 1)
    part = jnp.zeros((1, w), jnp.float32)
    for i, term in enumerate((wet_area, fresh, fresh * surface, wet_area * surface)):
        rows8 = jnp.sum(term.reshape(h // 8, 8, w), axis=0)
        part = jnp.where(
            lane1 == i, jnp.sum(jnp.sum(rows8, axis=1, keepdims=True), axis=0, keepdims=True), part
        )
    part_v[...] = part
    gain = time_step / area
    g_v[...] = gain

    parts_v[me] = part

    def send_part(gx, gy):
        @pl.when(gx * ny + gy != me)
        def _():
            pltpu.make_async_remote_copy(
                src_ref=part_v, dst_ref=parts_v.at[me], send_sem=part_send, recv_sem=part_recv,
                device_id={"gx": gx, "gy": gy}, device_id_type=MESH,
            ).start()

    edge_rows = 3 * nk + 8
    down_rows = 2 * nk + 8

    def bytes_of(n, sends, arrivals):
        block = flux_v.at[pl.ds(0, n)]
        return pltpu.make_async_remote_copy(
            src_ref=block, dst_ref=block, send_sem=sends, recv_sem=arrivals,
            device_id={"gx": east}, device_id_type=MESH,
        )

    def sent(flag, n, sends):
        pl.when(flag)(lambda: bytes_of(n, sends, pack_recv).wait_send())

    def came(flag, n, arrivals):
        pl.when(flag)(lambda: bytes_of(n, side_send, arrivals).wait_recv())

    def hand_on(gx, gy):
        return pltpu.make_async_remote_copy(
            src_ref=total_v, dst_ref=total_v, send_sem=part_send, recv_sem=part_recv,
            device_id={"gx": gx, "gy": gy}, device_id_type=MESH,
        )

    def meet():
        pl.semaphore_wait(barrier, partners)
        repeat(near, lambda gy: send_part(0, gy))
        send_part(0, ny - 1)
        repeat(ny, lambda gy: send_part(hub_column, gy))
        pl.when(seam_east)(
            lambda: pl.semaphore_signal(ready, inc=1, device_id={"gx": east}, device_id_type=MESH)
        )

    early = seam_west & (my < near)
    pack_first = (mx > 0) & (my < near)
    pl.when(my >= near)(meet)

    depth = (sea * lay_v[...]).astype(jnp.float32)
    depth_v[...] = depth

    half = h // 2
    depth_at = 6 * nk
    lane = lax.broadcasted_iota(jnp.int32, (h, w), 1)
    row = lax.broadcasted_iota(jnp.int32, (h, w), 0)
    slot = jnp.where(row < half, lane, lane - 1)
    pair = slot >> 1
    eastern = (slot & 1) == 0
    even_half = (lane[:half] & 1) == 0

    quarter = h // 4

    def cells(ref, k, b):
        return [
            ref[pl.ds(k * h + side * half + b * quarter, quarter), :] for side in (0, 1)
        ]

    def pack(packed, b, ref, first, count):
        for k in range(count):
            j = first + k
            packed = [
                jnp.where(
                    pair[side * half : side * half + quarter] == j,
                    pltpu.roll(plane, 2 * j + 1 + side, 1),
                    old,
                )
                for side, (plane, old) in enumerate(zip(cells(ref, k, b), packed))
            ]
        return packed

    empty = [jnp.zeros((quarter, w), jnp.float32)] * 2
    packed = [pack(empty, b, depth_v, 3 * nk, 1) for b in (0, 1)]
    for i, ref in enumerate((t_v, s_v)):
        loads[5 + i].wait()
        packed = [pack(packed[b], b, ref, i * nk, nk) for b in (0, 1)]
    loads[7].wait()

    def finish(b):
        upper, lower = pack(packed[b], b, uv_v, 2 * nk, nk)
        pack_v[pl.ds(b * quarter, quarter), :] = upper
        pack_v[pl.ds(half + b * quarter, quarter), :] = lower
        at = pl.ds(b * quarter, quarter)
        last_v[at, :] = jnp.where(even_half[:quarter], upper, lower)
        first_v[at, :] = jnp.where(even_half[:quarter], lower, upper)

    def strip(b, src, dst, step):
        at = pl.ds(b * quarter, quarter)
        return pltpu.make_async_remote_copy(
            src_ref=src.at[at], dst_ref=dst.at[at],
            send_sem=side_send, recv_sem=pack_recv,
            device_id={"gx": lax.rem(mx + step, nx)}, device_id_type=MESH,
        )

    to_east = [strip(b, last_v, west_v, 1) for b in (0, 1)]
    to_west = [strip(b, first_v, east_v, nx - 1) for b in (0, 1)]

    for b in (0, 1):
        finish(b)
    pl.when(pack_first)(meet)

    @pl.when(jnp.logical_not(early))
    def _():
        for b in (0, 1):
            to_east[b].start()

    depth_east_v[...] = jnp.where(
        lane == w - 1, 0.0, jnp.minimum(depth, pltpu.roll(depth, w - 1, 1))
    )
    depth_north_v[...] = jnp.where(
        row == h - 1, 0.0, jnp.minimum(depth, pltpu.roll(depth, h - 1, 0))
    )

    def interior(block, carry):
        start = pl.multiple_of(block * block_rows, block_rows)
        here = pl.ds(start, block_rows)
        deep_east, deep_north = depth_east_v[here, :], depth_north_v[here, :]
        deep, gain = depth_v[here, :], g_v[here, :]
        came = [0.0, 0.0]
        for k in range(nk):
            at = pl.ds(start + k * h, block_rows)
            east_near, east_far = face_weights(uv_v[at, :], deep_east > k)
            north_near, north_far = face_weights(
                uv_v[pl.ds(start + (nk + k) * h, block_rows), :], deep_north > k
            )
            mix = jnp.where(deep > k + 1, time_step * vertical_mixing, 0.0)
            for n, (ref, out) in enumerate(((t_v, t_out), (s_v, s_out))):
                c = ref[at, :]
                east = east_near * c + east_far * pltpu.roll(c, w - 1, 1)
                north = north_near * c + north_far * ref[pl.ds(start + k * h + 1, block_rows), :]
                strip_at = (n * nk + k) * (h + 8) + 8
                flux_v[pl.ds(start + strip_at, block_rows), :] = north
                south = flux_v[pl.ds(start + strip_at - 1, block_rows), :]
                flow = (pltpu.roll(east, 1, 1) - east) + (south - north)
                fall = 0.0
                if k < nk - 1:
                    fall = mix * (c - ref[pl.ds(start + (k + 1) * h, block_rows), :])
                out[at, :] = c + (gain * flow + (came[n] - fall))
                came[n] = fall
        return carry

    split = jnp.where(early, h // block_rows, 0)

    @pl.when(early)
    def _():
        late_loads.wait()

    lax.fori_loop(0, split, interior, 0)
    pl.when(early)(meet)

    @pl.when(early)
    def _():
        for b in (0, 1):
            to_east[b].start()

    @pl.when(jnp.logical_not(seam_west))
    def _():
        for b in (0, 1):
            to_west[b].start()

    @pl.when(jnp.logical_not(early))
    def _():
        late_loads.wait()


    def rows(ref, row, base=0):
        return ref[pl.ds(base + row, nk, stride=h), :]

    up_v[pl.ds(0, nk), :] = rows(t_v, h - 1)
    up_v[pl.ds(nk, nk), :] = rows(s_v, h - 1)
    up_v[pl.ds(2 * nk, nk), :] = rows(uv_v, h - 1, nk * h)
    up_v[pl.ds(3 * nk, 8), :] = jnp.broadcast_to(depth[h - 1 : h, :], (8, w))
    down_v[pl.ds(0, nk), :] = rows(t_v, 0)
    down_v[pl.ds(nk, nk), :] = rows(s_v, 0)
    down_v[pl.ds(2 * nk, 8), :] = jnp.broadcast_to(depth[0:1, :], (8, w))

    @pl.when(is_top)
    def _():
        up = up_v[...]
        flip = (w - 1) - lax.broadcasted_iota(jnp.int32, up.shape, 1)
        fold_v[mx] = jnp.take_along_axis(up, flip, axis=1)

    to_north = pltpu.make_async_remote_copy(
        src_ref=up_v, dst_ref=south_v, send_sem=side_send, recv_sem=row_recv,
        device_id={"gy": lax.rem(my + 1, ny)}, device_id_type=MESH,
    )
    to_south = pltpu.make_async_remote_copy(
        src_ref=down_v, dst_ref=north_v, send_sem=side_send, recv_sem=row_recv,
        device_id={"gy": lax.rem(my + ny - 1, ny)}, device_id_type=MESH,
    )

    def fold_copy(d):
        return pltpu.make_async_remote_copy(
            src_ref=fold_v.at[mx], dst_ref=fold_v.at[mx],
            send_sem=part_send, recv_sem=row_recv,
            device_id={"gx": lax.rem(mx + d + 1, nx)}, device_id_type=MESH,
        )


    @pl.when(jnp.logical_not(is_top))
    def _():
        to_north.start()

    @pl.when(my > 0)
    def _():
        to_south.start()

    @pl.when(is_top)
    def _():
        repeat(nx - 1, lambda d: fold_copy(d).start())

    lax.fori_loop(split, h // block_rows, interior, 0)

    level_row = lax.broadcasted_iota(jnp.int32, (nk, w), 0).astype(jnp.float32)

    def north_edge(far_t, far_s, speed, far_depth):
        near_weight, far_weight = face_weights(
            speed, jnp.minimum(up_v[3 * nk : 3 * nk + 1, :], far_depth) > level_row
        )
        for near, far, out in (
            (up_v[pl.ds(0, nk), :], far_t, t_out),
            (up_v[pl.ds(nk, nk), :], far_s, s_out),
        ):
            at = pl.ds(h - 1, nk, stride=h)
            out[at, :] -= g_v[h - 1 : h, :] * (near_weight * near + far_weight * far)

    @pl.when(seam_west)
    def _():
        pl.semaphore_wait(ready, 1)
        for b in (0, 1):
            to_west[b].start()

    def south_edge():
        near_weight, far_weight = face_weights(
            south_v[pl.ds(2 * nk, nk), :],
            jnp.minimum(down_v[2 * nk : 2 * nk + 1, :], south_v[3 * nk : 3 * nk + 1, :]) > level_row,
        )
        for i, out in enumerate((t_out, s_out)):
            at = pl.ds(0, nk, stride=h)
            out[at, :] += g_v[0:1, :] * (
                near_weight * south_v[pl.ds(i * nk, nk), :]
                + far_weight * down_v[pl.ds(i * nk, nk), :]
            )

    came(has_north & has_south, edge_rows + down_rows, row_recv)
    came(has_north & jnp.logical_not(has_south), down_rows, row_recv)

    @pl.when(has_north)
    def _():
        north_edge(
            north_v[pl.ds(0, nk), :],
            north_v[pl.ds(nk, nk), :],
            up_v[pl.ds(2 * nk, nk), :],
            north_v[2 * nk : 2 * nk + 1, :],
        )

    pl.when(has_north & has_south)(south_edge)

    def column(plane, at):
        return jnp.broadcast_to(plane[:, at : at + 1], (h, w))

    mine = pack_v[...]
    depth = depth_v[...]
    gain = g_v[...]
    level_of = (pair & (nk - 1)).astype(jnp.float32)
    open_cell = jnp.where(eastern, column(depth, w - 1), column(depth, 0)) > level_of
    edge_gain = jnp.where(eastern, -column(gain, w - 1), column(gain, 0))
    surface_wet = jnp.where(depth > 0.0, time_step / top_thickness, 0.0)
    surface = s0_v[...]
    s_out[pl.ds(0, h), :] -= surface_wet * surface * rain_v[...]
    for i, plane in enumerate(
        (
            mine,
            jnp.where(pair < nk, pltpu.roll(mine, w - 4 * nk, 1), pltpu.roll(mine, w - 2 * nk, 1)),
            jnp.where(open_cell, edge_gain, 0.0),
            surface_wet * surface,
            surface_wet,
        )
    ):
        side_out[pl.ds(i * h, h), :] = plane

    own_row = jnp.logical_not(is_top)
    fold_rows = (nx - 1) * edge_rows
    sent(plain & own_row, hubs, part_send)
    sent(plain & is_top, hubs + fold_rows, part_send)
    sent(seam_west & (my < near), hubs - 1, part_send)
    sent(has_north & has_south, h + edge_rows + down_rows, side_send)
    sent(jnp.logical_not(has_south), h + edge_rows, side_send)
    sent(is_top, h + down_rows, side_send)

    @pl.when(is_hub)
    def _():
        bytes_of(peers, side_send, part_recv).wait_recv()
        total_v[...] = jnp.sum(parts_v[...], axis=0)

    in_column = mx == hub_column
    seam_giver = seam_west & is_top

    @pl.when(in_column)
    def _():
        repeat(nx - 2, lambda d: hand_on(hub_column + 1 + d, my).start())

    @pl.when(seam_giver)
    def _():
        repeat(ny - 1 - near, lambda d: hand_on(0, near + d).start())

    @pl.when(is_top)
    def _():
        bytes_of(nx * edge_rows, side_send, row_recv).wait_recv()
        south_edge()
        partner = fold_v[seam_smem[0] // w]
        north_edge(
            partner[:nk],
            partner[nk : 2 * nk],
            0.5 * (up_v[pl.ds(2 * nk, nk), :] - partner[2 * nk : 3 * nk]),
            partner[3 * nk : 3 * nk + 1],
        )

    sent(in_column & own_row, hubs - 1 + nx - 2, part_send)
    sent(in_column & is_top, hubs - 1 + nx - 2 + fold_rows, part_send)
    sent(seam_giver, hubs - 1 + ny - 1 - near + fold_rows, part_send)
    pl.when(plain)(lambda: hand_on(0, 0).wait_recv())
    side_out[pl.ds(6 * h, 8), :] = jnp.broadcast_to(total_v[...], (8, w))
    bytes_of(h, side_send, pack_recv).wait_recv()
    side_out[pl.ds(5 * h, half), :] = west_v[...]
    side_out[pl.ds(5 * h + half, half), :] = east_v[...]


store_cuts = 16


def store_kernel(nk, h, w, t_ref, s_ref, side_ref, t_hbm, s_hbm, t_v, s_v, sem):
    half = h // 2
    mine, own_speed, edge_gain, surface, surface_wet = (
        side_ref[pl.ds(i * h, h), :] for i in range(5)
    )
    west = side_ref[pl.ds(5 * h, half), :]
    east = side_ref[pl.ds(5 * h + half, half), :]
    totals = side_ref[pl.ds(6 * h, 1), :]

    lane = lax.broadcasted_iota(jnp.int32, (h, w), 1)
    slot = jnp.where(lax.broadcasted_iota(jnp.int32, (h, w), 0) < half, lane, lane - 1)
    pair = slot >> 1
    eastern = (slot & 1) == 0

    def both(cells):
        return jnp.concatenate([cells, cells], axis=0)

    def moved(cells, by):
        return both(pltpu.roll(cells, by % w, 1))

    def columns(cells, at):
        return jnp.concatenate(
            [jnp.broadcast_to(cells[:, i : i + 1], (half, w)) for i in (at, at + 1)], axis=0
        )

    near = jnp.where(eastern, mine, moved(west, 1))
    far = jnp.where(eastern, moved(east, -1), mine)
    west_speed = jnp.where(pair < nk, moved(west, 1 - 4 * nk), moved(west, 1 - 2 * nk))
    far_depth = jnp.where(eastern, columns(east, 6 * nk + 1), columns(west, 6 * nk))
    near_weight, far_weight = face_weights(
        jnp.where(eastern, own_speed, west_speed),
        far_depth > (pair & (nk - 1)).astype(jnp.float32),
    )
    edge = edge_gain * (near_weight * near + far_weight * far)

    total_area, total_fresh, salt_fresh, salt_only = (
        jnp.broadcast_to(totals[:, i : i + 1], (1, w)) for i in range(4)
    )
    mean_fresh = total_fresh / total_area
    lift = (salt_fresh - mean_fresh * salt_only) / total_area
    virtual = surface_wet * lift + surface * mean_fresh

    at_edge = (lane[:half] == 0) | (lane[:half] == w - 1)
    step = nk // store_cuts
    for i, (ref, out, hbm) in enumerate(((t_ref, t_v, t_hbm), (s_ref, s_v, s_hbm))):
        for cut in reversed(range(store_cuts)):
            for k in range(cut * step, (cut + 1) * step):
                j = i * nk + k
                for part, shift in ((0, w - 1 - 2 * j), (1, w - 2 - 2 * j)):
                    rows = slice(part * half, (part + 1) * half)
                    change = jnp.where(at_edge, pltpu.roll(edge[rows], shift % w, 1), 0.0)
                    if j == nk:
                        change = change + virtual[rows]
                    at = pl.ds(k * h + part * half, half)
                    out[at, :] = ref[at, :] + change
            at = pl.ds(cut * step * h, step * h)
            pltpu.make_async_copy(out.at[at], hbm.at[at], sem).start()
    for out, hbm in ((t_v, t_hbm), (s_v, s_hbm)):
        pltpu.make_async_copy(out, hbm, sem).wait()


def shards(nx, ny, t, s, uv, sea, layers, area, rain, seam):
    nk, h, w = t.shape
    assert w == 128 and h % 16 == 0 and nk & (nk - 1) == 0 and nk % 8 == 0 and 6 * nk + 3 <= w and nx > 3 and ny > 3
    f32 = jnp.float32
    peers = nx * ny - 1
    half_plane = pltpu.VMEM((h // 2, w), f32)
    vmem = 67043328 - 4 * w * (2 * nk * h + 6 * h + 8)
    any_space = pl.BlockSpec(memory_space=pl.ANY)
    dma = pltpu.SemaphoreType.DMA
    plane = pltpu.VMEM((h, w), f32)
    t_next, s_next, side = pl.pallas_call(
        functools.partial(kernel, nx, ny, nk, h, w),
        out_shape=[pltpu.VMEM((nk * h, w), f32)] * 2 + [pltpu.VMEM((6 * h + 8, w), f32)],
        in_specs=[any_space] * 8,
        out_specs=[pl.BlockSpec(memory_space=pltpu.VMEM)] * 3,
        scratch_shapes=[
            pltpu.VMEM((nk * h + 8, w), f32),
            pltpu.VMEM((nk * h + 8, w), f32),
            pltpu.VMEM((2 * nk * h, w), f32),
            pltpu.VMEM((h, w), jnp.int32),
            pltpu.VMEM((h, w), jnp.int32),
            plane, plane, plane, plane, plane,
            plane, half_plane, half_plane, half_plane, half_plane,
            pltpu.VMEM((3 * nk + 8, w), f32),
            pltpu.VMEM((2 * nk + 8, w), f32),
            pltpu.VMEM((3 * nk + 8, w), f32),
            pltpu.VMEM((2 * nk + 8, w), f32),
            pltpu.VMEM((nx, 3 * nk + 8, w), f32),
            pltpu.VMEM((1, w), f32),
            pltpu.VMEM((nx * ny, 1, w), f32),
            pltpu.VMEM((1, w), f32),
            pltpu.SMEM((w,), jnp.int32),
            plane, plane,
            pltpu.VMEM((max(2 * nk * (h + 8), (nx + 2) * (3 * nk + 8)), w), f32),
            dma((5,)), dma, dma, dma, dma, dma, pltpu.SemaphoreType.REGULAR,
        ],
        compiler_params=pltpu.CompilerParams(
            collective_id=0, has_side_effects=True, vmem_limit_bytes=vmem
        ),
        name="tracer_step",
    )(
        t.reshape(nk * h, w), s.reshape(nk * h, w), uv.reshape(2 * nk * h, w),
        sea, layers, area, rain, seam,
    )
    t_next, s_next = pl.pallas_call(
        functools.partial(store_kernel, nk, h, w),
        out_shape=[jax.ShapeDtypeStruct((nk * h, w), f32)] * 2,
        in_specs=[pl.BlockSpec(memory_space=pltpu.VMEM)] * 3,
        out_specs=[any_space] * 2,
        scratch_shapes=[pltpu.VMEM((nk * h, w), f32)] * 2 + [dma],
        compiler_params=pltpu.CompilerParams(vmem_limit_bytes=8 << 20),
        name="store",
    )(t_next, s_next, side)
    return t_next.reshape(t.shape), s_next.reshape(s.shape)


def solution(mesh):
    in_specs = (
        P("groups", "gy", "gx"),
        P("groups", "gy", "gx"),
        P("groups", None, "gy", "gx"),
        P("gy", "gx"),
        P("gy", "gx"),
        P("gy", "gx"),
        P("gy", "gx"),
        P("gx"),
    )
    out_specs = (P("groups", "gy", "gx"), P("groups", "gy", "gx"))
    return jax.shard_map(
        functools.partial(shards, mesh.shape["gx"], mesh.shape["gy"]),
        mesh=mesh, in_specs=in_specs, out_specs=out_specs, check_vma=False,
    )
```
